8 devices in a mesh: rep: 1 (over z), col: 2 (over y), row: 4 (over x, core).
Axes of the slice: x: 2, y: 2, z: 1, core: 2. Of those that a mesh axis runs over, the one named last changes fastest.
Arguments:
- part_mass: float32 [131072], P(('rep', 'col', 'row'))
- cell_idx: int32 [131072, 3], P(('rep', 'col', 'row'))
- cic_wts: float32 [131072, 3, 2], P(('rep', 'col', 'row'))
- live_mask: int32 [131072], P(('rep', 'col', 'row'))
- gas_mesh: float32 [192, 192, 192], P('rep', 'row', 'col')
Outputs:
- output 1: float32 [131072, 3], P(('rep', 'col', 'row'))
- output 2: float32 [1], P('rep')
All inputs are finite; a program needn't handle non-finite values.
Results may differ from the reference program's by a relative error of at most 0.001.
Values are sent between devices in bfloat16 or wider.
A program may use at most 1 GiB of HBM per device.

```python
import math
import jax
import jax.numpy as jnp
from jax import lax

MESH_N = 192
ROW_DEVS = 4
COL_DEVS = 2
PART_DEV = 16384

Y_BLOCK = MESH_N // ROW_DEVS
Z_BLOCK = MESH_N // COL_DEVS
SLOT_COUNT = ROW_DEVS * COL_DEVS * PART_DEV
GRAV_CONST = 1.0
ENERGY_NORM = 0.5 / (float(MESH_N) ** 3 * float(SLOT_COUNT))


def setup_inputs(seed: int = 0, part: int = 0) -> dict:
    base_key = jax.random.fold_in(jax.random.key(seed), part)
    key_list = jax.random.split(base_key, 10)
    dev_shape = (COL_DEVS, ROW_DEVS, PART_DEV)
    pos_x = jax.random.randint(key_list[0], dev_shape, 0, MESH_N)
    pos_y = jax.random.randint(key_list[1], dev_shape, 0, Y_BLOCK)
    pos_z = jax.random.randint(key_list[2], dev_shape, 0, Z_BLOCK)
    edge_kind = jax.random.randint(key_list[3], dev_shape, 0, 4)
    pos_y = jnp.where((edge_kind == 0) | (edge_kind == 2), Y_BLOCK - 1, pos_y)
    pos_z = jnp.where((edge_kind == 1) | (edge_kind == 2), Z_BLOCK - 1, pos_z)
    live_count = jax.random.randint(key_list[4], (COL_DEVS, ROW_DEVS), PART_DEV // 4, PART_DEV + 1)
    live_count = live_count.at[0, 0].set(PART_DEV)
    live_mask = (jnp.arange(PART_DEV)[None, None, :] < live_count[:, :, None]).astype(jnp.int32)
    frac_off = jax.random.uniform(key_list[5], dev_shape + (3,), jnp.float32)
    cic_wts = jnp.stack([1.0 - frac_off, frac_off], axis=-1)
    row_ids = jnp.arange(ROW_DEVS)[None, :, None]
    col_ids = jnp.arange(COL_DEVS)[:, None, None]
    glob_x = pos_x + frac_off[..., 0]
    glob_y = row_ids * Y_BLOCK + pos_y + frac_off[..., 1]
    glob_z = col_ids * Z_BLOCK + pos_z + frac_off[..., 2]
    wave_unit = 2.0 * math.pi / MESH_N
    phases = jax.random.uniform(key_list[6], (5,), jnp.float32, 0.0, 2.0 * math.pi)
    modulation = (jnp.sin(wave_unit * glob_x + phases[0]) + jnp.sin(wave_unit * glob_y + phases[1])
                  + jnp.sin(wave_unit * glob_z + phases[2]))
    mass_scale = MESH_N / math.sqrt(SLOT_COUNT)
    mass_noise = jax.random.normal(key_list[7], dev_shape, jnp.float32)
    part_mass = mass_scale * jnp.exp(0.4 * modulation + 0.2 * mass_noise)
    mesh_x = jnp.arange(MESH_N, dtype=jnp.float32)[:, None, None]
    mesh_y = jnp.arange(MESH_N, dtype=jnp.float32)[None, :, None]
    mesh_z = jnp.arange(MESH_N, dtype=jnp.float32)[None, None, :]
    gas_amp = 0.5 * mass_scale * SLOT_COUNT / MESH_N ** 3
    gas_noise = jax.random.normal(key_list[8], (MESH_N, MESH_N, MESH_N), jnp.float32)
    gas_mesh = gas_amp * (1.0 + 0.8 * jnp.sin(wave_unit * mesh_x + phases[3]) * jnp.cos(wave_unit * (mesh_y - mesh_z) + phases[4]) + 0.5 * gas_noise)
    cell_idx = jnp.stack([pos_x, pos_y, pos_z], axis=-1).reshape(SLOT_COUNT, 3).astype(jnp.int32)
    return dict(part_mass=part_mass.reshape(SLOT_COUNT), cell_idx=cell_idx,
                cic_wts=cic_wts.reshape(SLOT_COUNT, 3, 2), live_mask=live_mask.reshape(SLOT_COUNT),
                gas_mesh=gas_mesh)


def signed_freq(n_points):
    mode_ids = jnp.arange(n_points)
    return ((mode_ids + n_points // 2) % n_points - n_points // 2).astype(jnp.float32)


def reference(part_mass, cell_idx, cic_wts, live_mask, gas_mesh):
    slot_ids = jnp.arange(SLOT_COUNT)
    row_off = ((slot_ids // PART_DEV) % ROW_DEVS) * Y_BLOCK
    col_off = (slot_ids // (ROW_DEVS * PART_DEV)) * Z_BLOCK
    corner_off = jnp.arange(2)
    x_pts = (cell_idx[:, 0:1] + corner_off) % MESH_N
    y_pts = (cell_idx[:, 1:2] + row_off[:, None] + corner_off) % MESH_N
    z_pts = (cell_idx[:, 2:3] + col_off[:, None] + corner_off) % MESH_N
    flat_pts = ((x_pts[:, :, None, None] * MESH_N + y_pts[:, None, :, None]) * MESH_N + z_pts[:, None, None, :]).reshape(-1)
    stencil = (cic_wts[:, 0, :, None, None] * cic_wts[:, 1, None, :, None] * cic_wts[:, 2, None, None, :]).reshape(SLOT_COUNT, 8)
    charge = part_mass * live_mask.astype(jnp.float32)
    density = jax.ops.segment_sum((charge[:, None] * stencil).reshape(-1), flat_pts, num_segments=MESH_N ** 3)
    density = density.reshape(MESH_N, MESH_N, MESH_N) + gas_mesh
    rho_hat = jnp.fft.fftn(density)
    freq_ids = signed_freq(MESH_N)
    norm_sq = freq_ids[:, None, None] ** 2 + freq_ids[None, :, None] ** 2 + freq_ids[None, None, :] ** 2
    k_unit = 2.0 * math.pi / MESH_N
    wave_vec = k_unit * freq_ids
    influence = jnp.where(norm_sq > 0, -4.0 * math.pi * GRAV_CONST / (k_unit * k_unit * jnp.maximum(norm_sq, 1.0)), 0.0)
    mode_power = jnp.real(rho_hat) ** 2 + jnp.imag(rho_hat) ** 2
    energy = jnp.sum(influence * mode_power) * ENERGY_NORM
    pot_hat = influence * rho_hat

    def grad_field(axis_sel):
        k_dot = (axis_sel[0] * wave_vec[:, None, None] + axis_sel[1] * wave_vec[None, :, None]
                 + axis_sel[2] * wave_vec[None, None, :])
        return jnp.real(jnp.fft.ifftn(1j * k_dot * pot_hat))

    fields = lax.map(grad_field, jnp.eye(3, dtype=jnp.float32))
    samples = fields.reshape(3, -1)[:, flat_pts].reshape(3, SLOT_COUNT, 8)
    grad_vals = jnp.sum(samples * stencil[None], axis=2)
    part_force = -(charge[:, None] * grad_vals.T)
    return part_force.astype(jnp.float32), energy.reshape(1).astype(jnp.float32)
```

```python
import functools
import math
import jax
import jax.numpy as jnp
from jax import lax
from jax.sharding import PartitionSpec as P
from jax.experimental import pallas as pl
from jax.experimental.pallas import tpu as pltpu

MATMUL_PREC = lax.Precision.HIGHEST
GRAV_CONST = 1.0
F32 = jnp.float32
BF16 = jnp.bfloat16
LANES = 128
X_TILE = 96
X_ROWS = 112
Y_SHIFT = 15
X_SHIFT = 7
VMEM_BIG = 60 * 1024 * 1024


def split3(val):
    hi = val.astype(BF16)
    rest = val - hi.astype(F32)
    mid = rest.astype(BF16)
    lo = (rest - mid.astype(F32)).astype(BF16)
    return hi, mid, lo


def bitonic(bufs):
    sub = lax.broadcasted_iota(jnp.int32, (8, LANES), 0)
    lane = lax.broadcasted_iota(jnp.int32, (8, LANES), 1)
    base = lane * 128 + sub * 16

    def bit(rank, pos):
        return lax.shift_right_logical(rank, jnp.full_like(rank, pos)) & 1

    def vreg_stage(k, j):
        for v in range(16):
            if v & (1 << j):
                continue
            low, high = pl.ds(8 * v, 8), pl.ds(8 * (v + (1 << j)), 8)
            sgn = 1.0 - 2.0 * bit(base + v, k).astype(F32)
            a = [b[low, :] for b in bufs]
            c = [b[high, :] for b in bufs]
            swap = a[0] * sgn > c[0] * sgn
            for b, p, q in zip(bufs, a, c):
                b[low, :] = jnp.where(swap, q, p)
                b[high, :] = jnp.where(swap, p, q)

    def roll_stage(k, j, dist, axis):
        size = (8, LANES)[axis]
        upper = bit(base, j)
        keep_low = upper == 0
        for v in range(16):
            rows = pl.ds(8 * v, 8)
            sgn = 1.0 - 2.0 * (bit(base + v, k) ^ upper).astype(F32)
            own = [b[rows, :] for b in bufs]
            other = [jnp.where(keep_low, pltpu.roll(o, size - dist, axis), pltpu.roll(o, dist, axis)) for o in own]
            take = other[0] * sgn < own[0] * sgn
            for b, o, p in zip(bufs, own, other):
                b[rows, :] = jnp.where(take, p, o)

    for k in range(1, 8):
        for j in range(k - 1, -1, -1):
            if j >= 4:
                roll_stage(k, j, 1 << (j - 4), 0)
            else:
                vreg_stage(k, j)

    def phase(k, carry):
        def lane_stage(step, c):
            j = k - 1 - step
            roll_stage(k, j, jnp.left_shift(1, j - 7), 1)
            return c
        lax.fori_loop(0, k - 7, lane_stage, 0)
        for j in (6, 5, 4):
            roll_stage(k, j, 1 << (j - 4), 0)
        for j in (3, 2, 1, 0):
            vreg_stage(k, j)
        return carry
    lax.fori_loop(8, 15, phase, 0)


def sort_kernel(n_arr, in_ref, out_ref, *bufs):
    for n in range(n_arr):
        bufs[n][...] = in_ref[n]
    bitonic(bufs)
    for n in range(n_arr):
        out_ref[n] = bufs[n][...].T


def sort_call(stacked):
    n_arr = stacked.shape[0]
    return pl.pallas_call(
        functools.partial(sort_kernel, n_arr),
        out_shape=jax.ShapeDtypeStruct(stacked.shape, F32),
        in_specs=[pl.BlockSpec(memory_space=pltpu.VMEM)],
        out_specs=pl.BlockSpec(memory_space=pltpu.VMEM),
        scratch_shapes=[pltpu.VMEM((128, LANES), F32)] * n_arr,
        name="slot_sort",
    )(stacked)


def pair_table(key, n_blk, n_xt):
    b_ids = jnp.arange(n_blk + 1)
    bounds = ((b_ids // n_xt) << Y_SHIFT) | (((b_ids % n_xt) * X_TILE) << X_SHIFT)
    starts = jnp.sum((key[None, :] < bounds[:, None].astype(F32)).astype(jnp.int32), axis=1)
    first, last = starts[:-1], starts[1:]
    lo = first // LANES
    count = jnp.where(last > first, (last + LANES - 1) // LANES - lo, 0)
    ids = jnp.arange(n_blk)
    ends = jnp.sum(jnp.where(ids[None, :] <= ids[:, None], count[None, :], 0), axis=1)
    t_max = n_blk + 128
    t_ids = jnp.arange(t_max)
    blk = jnp.sum((ends[None, :] <= t_ids[:, None]).astype(jnp.int32), axis=1)
    chunk = t_ids + jnp.sum(jnp.where(ids[None, :] == blk[:, None], (lo - ends + count)[None, :], 0), axis=1)
    live = t_ids < ends[-1]
    table = jnp.stack([jnp.where(live, blk, n_blk + 7), jnp.where(live, chunk, 0)])
    return table.astype(jnp.int32), ends[-1:].astype(jnp.int32)


def read_pair(t, table_ref, slot_ref, n_blk, n_xt):
    blk = table_ref[0, t]
    chunk = table_ref[1, t]
    blk_in = jnp.minimum(blk, n_blk - 1)
    y_pl = blk_in // n_xt
    x_beg = pl.multiple_of((blk_in % n_xt) * X_TILE, 16)
    code = slot_ref[0, pl.ds(chunk, 1), :].astype(jnp.int32)
    x_c = (code >> X_SHIFT) & 255
    b_c = (code >> Y_SHIFT) * n_xt
    for m in range(1, n_xt):
        b_c = b_c + (x_c >= m * X_TILE).astype(jnp.int32)
    mask = b_c == blk
    vals = [slot_ref[n, pl.ds(chunk, 1), :] for n in range(1, 5)]
    return chunk, y_pl, x_beg, x_c - x_beg, code & 127, mask, vals


def deposit_kernel(n_blk, n_xt, grid_size, table_ref, num_ref, slot_ref, rho_ref):
    n_planes = rho_ref.shape[0]

    def clear(y, c):
        rho_ref[y] = jnp.zeros(rho_ref.shape[1:], F32)
        return c
    lax.fori_loop(0, n_planes, clear, 0)
    row_x = lax.broadcasted_iota(jnp.int32, (X_ROWS, LANES), 0)
    row_z = lax.broadcasted_iota(jnp.int32, (LANES, LANES), 0)

    def one(t):
        chunk, y_pl, x_beg, x_l, z_c, mask, (q, wx, wy, wz) = read_pair(t, table_ref, slot_ref, n_blk, n_xt)
        q = jnp.where(mask, q, 0.0)
        pick_x = jnp.concatenate([(row_x == x_l).astype(F32), (row_x == x_l + 1).astype(F32)], axis=1).astype(BF16)
        on_z = jnp.where(row_z == z_c, 1.0 - wz, jnp.where(row_z == z_c + 1, wz, 0.0))
        rows = []
        for w_y in (1.0 - wy, wy):
            rows.append(jnp.concatenate([on_z * (q * (1.0 - wx) * w_y), on_z * (q * wx * w_y)], axis=1))
        parts = split3(jnp.concatenate(rows, axis=0))
        res = None
        for part in parts:
            term = lax.dot_general(pick_x, part, (((1,), (1,)), ((), ())), preferred_element_type=F32)
            res = term if res is None else res + term
        for b in range(2):
            rho_ref[y_pl + b, pl.ds(x_beg, X_ROWS), :] += res[:, b * LANES:(b + 1) * LANES]

    def body(t, c):
        one(2 * t)
        one(2 * t + 1)
        return c
    lax.fori_loop(0, (num_ref[0] + 1) // 2, body, 0)

    def wrap(y, c):
        rho_ref[y, 0:8, :] += rho_ref[y, grid_size:grid_size + 8, :]
        return c
    lax.fori_loop(0, n_planes, wrap, 0)


def interp_kernel(n_blk, n_xt, table_ref, num_ref, slot_ref, fhm_ref, flo_ref, out_ref):
    out_ref[...] = jnp.zeros(out_ref.shape, F32)
    row_x = lax.broadcasted_iota(jnp.int32, (X_ROWS, LANES), 0)
    row_z = lax.broadcasted_iota(jnp.int32, (LANES, LANES), 0)

    def one(t):
        chunk, y_pl, x_beg, x_l, z_c, mask, (q, wx, wy, wz) = read_pair(t, table_ref, slot_ref, n_blk, n_xt)
        pick_z = jnp.concatenate([(row_z == z_c).astype(F32), (row_z == z_c + 1).astype(F32)], axis=1).astype(BF16)
        pick_2 = jnp.concatenate([pick_z, pick_z], axis=0)
        on_x = jnp.where(row_x == x_l, 1.0 - wx, jnp.where(row_x == x_l + 1, wx, 0.0))
        rows = pl.ds(x_beg, X_ROWS)
        wt = [on_x * (1.0 - wy), on_x * wy]
        for comp in range(3):
            acc = None
            for b in range(2):
                got = jnp.dot(fhm_ref[y_pl + b, comp, rows, :], pick_2, preferred_element_type=F32)
                got = got + jnp.dot(flo_ref[y_pl + b, comp, rows, :], pick_z, preferred_element_type=F32)
                term = (got[:, :LANES] * (1.0 - wz) + got[:, LANES:] * wz) * wt[b]
                acc = term if acc is None else acc + term
            grad = jnp.sum(acc, axis=0, keepdims=True)
            here = pl.ds(chunk, 1)
            out_ref[comp, here, :] = jnp.where(mask, -q * grad, out_ref[comp, here, :])

    def body(t, c):
        one(2 * t)
        one(2 * t + 1)
        return c
    lax.fori_loop(0, (num_ref[0] + 1) // 2, body, 0)


SMEM_SPEC = pl.BlockSpec(memory_space=pltpu.SMEM)
VMEM_SPEC = pl.BlockSpec(memory_space=pltpu.VMEM)


def deposit_call(table, num, slots, y_ext, grid_size, n_blk, n_xt):
    return pl.pallas_call(
        functools.partial(deposit_kernel, n_blk, n_xt, grid_size),
        out_shape=jax.ShapeDtypeStruct((y_ext, grid_size + 16, LANES), F32),
        in_specs=[SMEM_SPEC, SMEM_SPEC, VMEM_SPEC], out_specs=VMEM_SPEC,
        compiler_params=pltpu.CompilerParams(vmem_limit_bytes=VMEM_BIG), name="deposit",
    )(table, num, slots)


def interp_call(table, num, slots, fhm, flo, n_blk, n_xt):
    return pl.pallas_call(
        functools.partial(interp_kernel, n_blk, n_xt),
        out_shape=jax.ShapeDtypeStruct((3, 128, LANES), F32),
        in_specs=[SMEM_SPEC, SMEM_SPEC, VMEM_SPEC, VMEM_SPEC, VMEM_SPEC], out_specs=VMEM_SPEC,
        compiler_params=pltpu.CompilerParams(vmem_limit_bytes=VMEM_BIG), name="interp",
    )(table, num, slots, fhm, flo)


def slot_arrays(part_mass, cell_idx, cic_wts, live_mask, y_blk):
    charge = part_mass * live_mask.astype(F32)
    code = (cell_idx[:, 1] << Y_SHIFT) | (cell_idx[:, 0] << X_SHIFT) | cell_idx[:, 2]
    code = jnp.where(live_mask > 0, code, y_blk << Y_SHIFT).astype(F32)
    upper = cic_wts[:, :, 1]
    return jnp.stack([code, charge, upper[:, 0], upper[:, 1], upper[:, 2]]).reshape(5, 128, LANES)


def home_ranks():
    a = lax.broadcasted_iota(jnp.int32, (128, LANES), 0)
    b = lax.broadcasted_iota(jnp.int32, (128, LANES), 1)
    return (a * 128 + (b & 7) * 16 + (b >> 3)).astype(F32)


def dft_table(out_ids, n_points, sign_val):
    in_ids = jnp.arange(n_points)
    phase_arg = ((out_ids[:, None] * in_ids[None, :]) % n_points).astype(jnp.float32) * (2.0 * math.pi / n_points)
    return jnp.cos(phase_arg), sign_val * jnp.sin(phase_arg)


def complex_matrix(out_ids, n_points, sign_val):
    cos_t, sin_t = dft_table(out_ids, n_points, sign_val)
    return jnp.stack([jnp.stack([cos_t, -sin_t]), jnp.stack([sin_t, cos_t])])


def wave_numbers(mode_ids, n_points):
    return ((mode_ids + n_points // 2) % n_points - n_points // 2).astype(jnp.float32)


def influence_of(norm_sq, n_points):
    k_unit = 2.0 * math.pi / n_points
    return jnp.where(norm_sq > 0, -4.0 * math.pi * GRAV_CONST / (k_unit * k_unit * jnp.maximum(norm_sq, 1.0)), 0.0)


def dft_apply(form, lhs_mat, rhs_arr):
    return jnp.einsum(form, lhs_mat, rhs_arr, precision=MATMUL_PREC, preferred_element_type=jnp.float32)


def solution(mesh):
    n_rows = mesh.shape["row"]
    n_cols = mesh.shape["col"]
    slot_axes = ("rep", "col", "row")
    to_next_row = [(k, (k + 1) % n_rows) for k in range(n_rows)]
    to_prev_row = [(k, (k - 1) % n_rows) for k in range(n_rows)]
    to_next_col = [(k, (k + 1) % n_cols) for k in range(n_cols)]
    to_prev_col = [(k, (k - 1) % n_cols) for k in range(n_cols)]

    def device_body(part_mass, cell_idx, cic_wts, live_mask, gas_block):
        grid_size, y_blk, z_blk = gas_block.shape
        per_dev = part_mass.shape[0]
        n_slots = per_dev * n_rows * n_cols
        row_id = lax.axis_index("row")
        col_id = lax.axis_index("col")
        n_xt = grid_size // X_TILE
        n_blk = y_blk * n_xt
        raw = slot_arrays(part_mass, cell_idx, cic_wts, live_mask, y_blk)
        table, num = pair_table(raw[0].reshape(-1), n_blk, n_xt)
        slots = sort_call(jnp.concatenate([raw, home_ranks()[None]]))
        rho = deposit_call(table, num, slots, y_blk + 1, grid_size, n_blk, n_xt)
        spread = jnp.transpose(rho[:, :grid_size, :z_blk + 1], (1, 0, 2))
        from_row = lax.ppermute(spread[:, y_blk, :], "row", to_next_row)
        body_y = jnp.concatenate([spread[:, 0:1, :] + from_row[:, None, :], spread[:, 1:y_blk, :]], axis=1)
        from_col = lax.ppermute(body_y[:, :, z_blk], "col", to_next_col)
        density = jnp.concatenate([body_y[:, :, 0:1] + from_col[:, :, None], body_y[:, :, 1:z_blk]], axis=2) + gas_block

        full_ids = jnp.arange(grid_size)
        fwd_mat = complex_matrix(full_ids, grid_size, -1.0)
        stage_x = dft_apply("pkx,xyz->pkyz", fwd_mat[:, 0], density)
        swap_a = lax.all_to_all(stage_x, "row", 1, 2, tiled=True)
        stage_y = dft_apply("pqly,qkyz->plkz", fwd_mat, swap_a)
        swap_b = lax.all_to_all(stage_y, "col", 1, 3, tiled=True)
        rho_hat = dft_apply("pqmz,qlkz->pmlk", fwd_mat, swap_b)

        k_unit = 2.0 * math.pi / grid_size
        kz_n = wave_numbers(full_ids, grid_size)
        ky_n = wave_numbers(col_id * (grid_size // n_cols) + jnp.arange(grid_size // n_cols), grid_size)
        kx_n = wave_numbers(row_id * (grid_size // n_rows) + jnp.arange(grid_size // n_rows), grid_size)
        norm_sq = kz_n[:, None, None] ** 2 + ky_n[None, :, None] ** 2 + kx_n[None, None, :] ** 2
        influence = influence_of(norm_sq, grid_size)
        local_sum = jnp.sum(influence * (rho_hat[0] * rho_hat[0] + rho_hat[1] * rho_hat[1]))
        energy = lax.psum(local_sum, ("row", "col")) * (0.5 / (grid_size ** 3 * n_slots))
        i_pot = jnp.stack([-influence * rho_hat[1], influence * rho_hat[0]])
        deriv_hat = jnp.stack([i_pot * (k_unit * kx_n)[None, None, None, :],
                               i_pot * (k_unit * ky_n)[None, None, :, None],
                               i_pot * (k_unit * kz_n)[None, :, None, None]], axis=2)

        inv_mat = complex_matrix(full_ids, grid_size, 1.0)
        back_z = dft_apply("pqnm,qmclk->pnclk", inv_mat, deriv_hat)
        swap_c = lax.all_to_all(back_z, "col", 1, 3, tiled=True)
        back_y = dft_apply("pqyl,qzclk->pyzck", inv_mat, swap_c)
        swap_d = lax.all_to_all(back_y, "row", 1, 4, tiled=True)
        cos_t, sin_t = dft_table(full_ids, grid_size, 1.0)
        real_mat = jnp.stack([cos_t, -sin_t]) * (1.0 / grid_size ** 3)
        fields = dft_apply("qxk,qyzck->ycxz", real_mat, swap_d)

        from_row_next = lax.ppermute(fields[0:1], "row", to_prev_row)
        ext_y = jnp.concatenate([fields, from_row_next], axis=0)
        from_col_next = lax.ppermute(ext_y[..., 0:1], "col", to_prev_col)
        ext = jnp.concatenate([ext_y, from_col_next, jnp.zeros(ext_y.shape[:3] + (LANES - z_blk - 1,), F32)], axis=3)
        ext = jnp.concatenate([ext, ext[:, :, :16]], axis=2)
        hi = lax.reduce_precision(ext, 8, 7)
        mid = lax.reduce_precision(ext - hi, 8, 7)
        low = ext - hi - mid
        fhm = jnp.concatenate([hi, mid], axis=3).astype(BF16)
        forces = interp_call(table, num, slots, fhm, low.astype(BF16), n_blk, n_xt)
        back = sort_call(jnp.concatenate([slots[5:6], forces]))
        part_force = back[1:4].reshape(3, per_dev).T
        return part_force, energy.reshape(1)

    return jax.shard_map(
        device_body, mesh=mesh,
        in_specs=(P(slot_axes), P(slot_axes, None), P(slot_axes, None, None), P(slot_axes), P("rep", "row", "col")),
        out_specs=(P(slot_axes, None), P("rep")), check_vma=False)
```

```python
import functools
import math
import numpy as np
import jax
import jax.numpy as jnp
from jax import lax
from jax.sharding import PartitionSpec as P
from jax.experimental import pallas as pl
from jax.experimental.pallas import tpu as pltpu

MATMUL_PREC = lax.Precision.HIGHEST
GRAV_CONST = 1.0
F32 = jnp.float32
BF16 = jnp.bfloat16
LANES = 128
X_TILE = 96
X_ROWS = 112
Y_SHIFT = 15
X_SHIFT = 7
VMEM_BIG = 60 * 1024 * 1024


def split3(val):
    hi = val.astype(BF16)
    rest = val - hi.astype(F32)
    mid = rest.astype(BF16)
    lo = (rest - mid.astype(F32)).astype(BF16)
    return hi, mid, lo


def bitonic(bufs):
    sub = lax.broadcasted_iota(jnp.int32, (8, LANES), 0)
    lane = lax.broadcasted_iota(jnp.int32, (8, LANES), 1)
    base = lane * 128 + sub * 16

    def bit(rank, pos):
        return lax.shift_right_logical(rank, jnp.full_like(rank, pos)) & 1

    def vreg_stage(k, j):
        for v in range(16):
            if v & (1 << j):
                continue
            low, high = pl.ds(8 * v, 8), pl.ds(8 * (v + (1 << j)), 8)
            sgn = 1.0 - 2.0 * bit(base + v, k).astype(F32)
            a = [b[low, :] for b in bufs]
            c = [b[high, :] for b in bufs]
            swap = a[0] * sgn > c[0] * sgn
            for b, p, q in zip(bufs, a, c):
                b[low, :] = jnp.where(swap, q, p)
                b[high, :] = jnp.where(swap, p, q)

    def roll_stage(k, j, dist, axis):
        size = (8, LANES)[axis]
        upper = bit(base, j)
        keep_low = upper == 0
        for v in range(16):
            rows = pl.ds(8 * v, 8)
            sgn = 1.0 - 2.0 * (bit(base + v, k) ^ upper).astype(F32)
            own = [b[rows, :] for b in bufs]
            other = [jnp.where(keep_low, pltpu.roll(o, size - dist, axis), pltpu.roll(o, dist, axis)) for o in own]
            take = other[0] * sgn < own[0] * sgn
            for b, o, p in zip(bufs, own, other):
                b[rows, :] = jnp.where(take, p, o)

    for k in range(1, 8):
        for j in range(k - 1, -1, -1):
            if j >= 4:
                roll_stage(k, j, 1 << (j - 4), 0)
            else:
                vreg_stage(k, j)

    def phase(k, carry):
        def lane_stage(step, c):
            j = k - 1 - step
            roll_stage(k, j, jnp.left_shift(1, j - 7), 1)
            return c
        lax.fori_loop(0, k - 7, lane_stage, 0)
        for j in (6, 5, 4):
            roll_stage(k, j, 1 << (j - 4), 0)
        for j in (3, 2, 1, 0):
            vreg_stage(k, j)
        return carry
    lax.fori_loop(8, 15, phase, 0)


def sort_kernel(n_arr, in_ref, out_ref, *bufs):
    for n in range(n_arr):
        bufs[n][...] = in_ref[n]
    bitonic(bufs)
    for n in range(n_arr):
        out_ref[n] = bufs[n][...].T


def sort_call(stacked):
    n_arr = stacked.shape[0]
    return pl.pallas_call(
        functools.partial(sort_kernel, n_arr),
        out_shape=jax.ShapeDtypeStruct(stacked.shape, F32),
        in_specs=[pl.BlockSpec(memory_space=pltpu.VMEM)],
        out_specs=pl.BlockSpec(memory_space=pltpu.VMEM),
        scratch_shapes=[pltpu.VMEM((128, LANES), F32)] * n_arr,
        name="slot_sort",
    )(stacked)


def pair_table(key, n_blk, n_xt):
    b_ids = jnp.arange(n_blk + 1)
    bounds = ((b_ids // n_xt) << Y_SHIFT) | (((b_ids % n_xt) * X_TILE) << X_SHIFT)
    starts = jnp.sum((key[None, :] < bounds[:, None].astype(F32)).astype(jnp.int32), axis=1)
    first, last = starts[:-1], starts[1:]
    lo = first // LANES
    count = jnp.where(last > first, (last + LANES - 1) // LANES - lo, 0)
    ids = jnp.arange(n_blk)
    ends = jnp.sum(jnp.where(ids[None, :] <= ids[:, None], count[None, :], 0), axis=1)
    t_max = n_blk + 128
    t_ids = jnp.arange(t_max)
    blk = jnp.sum((ends[None, :] <= t_ids[:, None]).astype(jnp.int32), axis=1)
    chunk = t_ids + jnp.sum(jnp.where(ids[None, :] == blk[:, None], (lo - ends + count)[None, :], 0), axis=1)
    live = t_ids < ends[-1]
    table = jnp.stack([jnp.where(live, blk, n_blk + 7), jnp.where(live, chunk, 0)])
    return table.astype(jnp.int32), ends[-1:].astype(jnp.int32)


def read_pair(t, table_ref, slot_ref, n_blk, n_xt):
    blk = table_ref[0, t]
    chunk = table_ref[1, t]
    blk_in = jnp.minimum(blk, n_blk - 1)
    y_pl = blk_in // n_xt
    x_beg = pl.multiple_of((blk_in % n_xt) * X_TILE, 16)
    code = slot_ref[0, pl.ds(chunk, 1), :].astype(jnp.int32)
    x_c = (code >> X_SHIFT) & 255
    b_c = (code >> Y_SHIFT) * n_xt
    for m in range(1, n_xt):
        b_c = b_c + (x_c >= m * X_TILE).astype(jnp.int32)
    mask = b_c == blk
    vals = [slot_ref[n, pl.ds(chunk, 1), :] for n in range(1, 5)]
    return chunk, y_pl, x_beg, x_c - x_beg, code & 127, mask, vals


def deposit_kernel(n_blk, n_xt, grid_size, table_ref, num_ref, slot_ref, rho_ref):
    n_planes = rho_ref.shape[0]

    def clear(y, c):
        rho_ref[y] = jnp.zeros(rho_ref.shape[1:], F32)
        return c
    lax.fori_loop(0, n_planes, clear, 0)
    row_x = lax.broadcasted_iota(jnp.int32, (X_ROWS, LANES), 0)
    row_z = lax.broadcasted_iota(jnp.int32, (LANES, LANES), 0)

    def one(t):
        chunk, y_pl, x_beg, x_l, z_c, mask, (q, wx, wy, wz) = read_pair(t, table_ref, slot_ref, n_blk, n_xt)
        q = jnp.where(mask, q, 0.0)
        pick_x = jnp.concatenate([(row_x == x_l).astype(F32), (row_x == x_l + 1).astype(F32)], axis=1).astype(BF16)
        on_z = jnp.where(row_z == z_c, 1.0 - wz, jnp.where(row_z == z_c + 1, wz, 0.0))
        rows = []
        for w_y in (1.0 - wy, wy):
            rows.append(jnp.concatenate([on_z * (q * (1.0 - wx) * w_y), on_z * (q * wx * w_y)], axis=1))
        parts = split3(jnp.concatenate(rows, axis=0))
        res = None
        for part in parts:
            term = lax.dot_general(pick_x, part, (((1,), (1,)), ((), ())), preferred_element_type=F32)
            res = term if res is None else res + term
        for b in range(2):
            rho_ref[y_pl + b, pl.ds(x_beg, X_ROWS), :] += res[:, b * LANES:(b + 1) * LANES]

    def body(t, c):
        one(2 * t)
        one(2 * t + 1)
        return c
    lax.fori_loop(0, (num_ref[0] + 1) // 2, body, 0)

    def wrap(y, c):
        rho_ref[y, 0:8, :] += rho_ref[y, grid_size:grid_size + 8, :]
        return c
    lax.fori_loop(0, n_planes, wrap, 0)


def interp_kernel(n_blk, n_xt, table_ref, num_ref, slot_ref, fhm_ref, flo_ref, out_ref):
    out_ref[...] = jnp.zeros(out_ref.shape, F32)
    row_x = lax.broadcasted_iota(jnp.int32, (X_ROWS, LANES), 0)
    row_z = lax.broadcasted_iota(jnp.int32, (LANES, LANES), 0)

    def one(t):
        chunk, y_pl, x_beg, x_l, z_c, mask, (q, wx, wy, wz) = read_pair(t, table_ref, slot_ref, n_blk, n_xt)
        pick_z = jnp.concatenate([(row_z == z_c).astype(F32), (row_z == z_c + 1).astype(F32)], axis=1).astype(BF16)
        pick_2 = jnp.concatenate([pick_z, pick_z], axis=0)
        on_x = jnp.where(row_x == x_l, 1.0 - wx, jnp.where(row_x == x_l + 1, wx, 0.0))
        rows = pl.ds(x_beg, X_ROWS)
        wt = [on_x * (1.0 - wy), on_x * wy]
        for comp in range(3):
            acc = None
            for b in range(2):
                got = jnp.dot(fhm_ref[y_pl + b, comp, rows, :], pick_2, preferred_element_type=F32)
                got = got + jnp.dot(flo_ref[y_pl + b, comp, rows, :], pick_z, preferred_element_type=F32)
                term = (got[:, :LANES] * (1.0 - wz) + got[:, LANES:] * wz) * wt[b]
                acc = term if acc is None else acc + term
            grad = jnp.sum(acc, axis=0, keepdims=True)
            here = pl.ds(chunk, 1)
            out_ref[comp, here, :] = jnp.where(mask, -q * grad, out_ref[comp, here, :])

    def body(t, c):
        one(2 * t)
        one(2 * t + 1)
        return c
    lax.fori_loop(0, (num_ref[0] + 1) // 2, body, 0)


SMEM_SPEC = pl.BlockSpec(memory_space=pltpu.SMEM)
VMEM_SPEC = pl.BlockSpec(memory_space=pltpu.VMEM)


def deposit_call(table, num, slots, y_ext, grid_size, n_blk, n_xt):
    return pl.pallas_call(
        functools.partial(deposit_kernel, n_blk, n_xt, grid_size),
        out_shape=jax.ShapeDtypeStruct((y_ext, grid_size + 16, LANES), F32),
        in_specs=[SMEM_SPEC, SMEM_SPEC, VMEM_SPEC], out_specs=VMEM_SPEC,
        compiler_params=pltpu.CompilerParams(vmem_limit_bytes=VMEM_BIG), name="deposit",
    )(table, num, slots)


def interp_call(table, num, slots, fhm, flo, n_blk, n_xt):
    return pl.pallas_call(
        functools.partial(interp_kernel, n_blk, n_xt),
        out_shape=jax.ShapeDtypeStruct((3, 128, LANES), F32),
        in_specs=[SMEM_SPEC, SMEM_SPEC, VMEM_SPEC, VMEM_SPEC, VMEM_SPEC], out_specs=VMEM_SPEC,
        compiler_params=pltpu.CompilerParams(vmem_limit_bytes=VMEM_BIG), name="interp",
    )(table, num, slots, fhm, flo)


def slot_arrays(part_mass, cell_idx, cic_wts, live_mask, y_blk):
    charge = part_mass * live_mask.astype(F32)
    code = (cell_idx[:, 1] << Y_SHIFT) | (cell_idx[:, 0] << X_SHIFT) | cell_idx[:, 2]
    code = jnp.where(live_mask > 0, code, y_blk << Y_SHIFT).astype(F32)
    upper = cic_wts[:, :, 1]
    return jnp.stack([code, charge, upper[:, 0], upper[:, 1], upper[:, 2]]).reshape(5, 128, LANES)


def home_ranks():
    a = lax.broadcasted_iota(jnp.int32, (128, LANES), 0)
    b = lax.broadcasted_iota(jnp.int32, (128, LANES), 1)
    return (a * 128 + (b & 7) * 16 + (b >> 3)).astype(F32)


def mul6(a, b):
    res = None
    for m, n in ((2, 0), (0, 2), (1, 1), (1, 0), (0, 1), (0, 0)):
        term = jnp.dot(a[m], b[n], preferred_element_type=F32)
        res = term if res is None else res + term
    return res


def table3(mat):
    mat = mat.astype(np.float32)
    hi = mat.astype(BF16)
    mid = (mat - hi.astype(np.float32)).astype(BF16)
    lo = (mat - hi.astype(np.float32) - mid.astype(np.float32)).astype(BF16)
    return np.stack([hi, mid, lo])


class Plan:
    def __init__(self, n, n_chip, y_blk, z_blk):
        self.n, self.n_chip, self.y_blk, self.z_blk = n, n_chip, y_blk, z_blk
        self.y_ext = y_blk + 1
        self.z_ext = z_blk + 1
        self.y_pad = -(-self.y_ext // 8) * 8
        self.half_k = n // 2 + 1
        self.slots = -(-self.half_k // (2 * n_chip))
        self.per_core = self.slots * n_chip
        self.k_pad = -(-self.per_core // 8) * 8
        self.rows = -(-(self.slots * self.y_ext + 1) // 8) * 8
        self.y_even = self.y_ext + self.y_ext % 2
        self.x_pad = n + 16

    def angle(self, k, r):
        return 2.0 * np.pi / self.n * ((k[:, None] * r[None, :]) % self.n)

    def lane_order(self):
        kz = np.concatenate([np.arange(128), np.arange(128), np.arange(128, self.n), np.arange(128, self.n)])
        im = np.concatenate([np.zeros(128), np.ones(128), np.zeros(self.n - 128), np.ones(self.n - 128)]) > 0
        return kz, im

    def deriv(self, k):
        sgn = np.where(k < self.n // 2, k, k - self.n)
        return np.where(k == self.n // 2, 0, sgn) * (2.0 * np.pi / self.n)

    def tables(self):
        n = self.n
        out = {}
        mx = np.zeros((2, 2, self.k_pad, n))
        mi = np.zeros((2, 2, self.x_pad, 2, self.k_pad))
        for h in range(2):
            kx = h * self.per_core + np.arange(self.per_core)
            ok = (kx < self.half_k)[:, None]
            th = self.angle(kx, np.arange(n))
            mx[h, 0, :self.per_core] = np.where(ok, np.cos(th), 0.0)
            mx[h, 1, :self.per_core] = np.where(ok, -np.sin(th), 0.0)
            th = self.angle(kx, np.arange(self.x_pad))
            wt = np.where(kx < self.half_k, np.where((kx == 0) | (kx == n // 2), 1.0, 2.0), 0.0) / float(n) ** 3
            kd = np.where(kx < n // 2, kx, 0) * (2.0 * np.pi / n) * wt
            mi[h, 0, :, 0, :self.per_core] = (-kd[:, None] * np.sin(th)).T
            mi[h, 0, :, 1, :self.per_core] = (-kd[:, None] * np.cos(th)).T
            mi[h, 1, :, 0, :self.per_core] = (wt[:, None] * np.cos(th)).T
            mi[h, 1, :, 1, :self.per_core] = (-wt[:, None] * np.sin(th)).T
        out["mx"] = table3(mx.reshape(2, 2 * self.k_pad, n))
        out["mi"] = table3(mi.reshape(2, 2, self.x_pad, 2 * self.k_pad))
        kz, im = self.lane_order()
        wz = np.zeros((2, 2, LANES, 2 * n))
        wi = np.zeros((2, 2 * n, 4, LANES))
        kd = self.deriv(kz)[:, None]
        for h in range(2):
            z = (h * self.z_blk + np.arange(self.z_ext)) % n
            c, s = np.cos(self.angle(kz, z)), np.sin(self.angle(kz, z))
            wz[h, 0, :self.z_ext] = np.where(im[:, None], -s, c).T
            wz[h, 1, :self.z_ext] = np.where(im[:, None], c, s).T
            re_w, im_w = np.where(im[:, None], -s, c), np.where(im[:, None], c, s)
            wi[h, :, 0, :self.z_ext] = re_w
            wi[h, :, 1, :self.z_ext] = im_w
            wi[h, :, 2, :self.z_ext] = -kd * im_w
            wi[h, :, 3, :self.z_ext] = kd * re_w
        out["wz"] = table3(wz)
        out["wi"] = table3(wi.reshape(2, 2 * n, 4 * LANES))
        ky = np.arange(n)
        my = np.zeros((2, n, self.n_chip, self.y_pad))
        ei = np.zeros((self.n_chip, 4, self.y_pad, n))
        for i in range(self.n_chip):
            y = (i * self.y_blk + np.arange(self.y_ext)) % n
            th = self.angle(ky, y)
            my[0, :, i, :self.y_ext] = np.cos(th)
            my[1, :, i, :self.y_ext] = np.sin(th)
            ei[i, 0, :self.y_ext] = np.cos(th).T
            ei[i, 1, :self.y_ext] = np.sin(th).T
            ei[i, 2, :self.y_ext] = (self.deriv(ky)[:, None] * np.cos(th)).T
            ei[i, 3, :self.y_ext] = (self.deriv(ky)[:, None] * np.sin(th)).T
        out["my"] = table3(my.reshape(2 * n, self.n_chip * self.y_pad))
        out["ei"] = table3(ei.reshape(self.n_chip, 4 * self.y_pad, n))
        return out


def x_kernel(plan, core_ref, rho_ref, gas_ref, mx_ref, own_ref, send_ref, tmp_ref):
    step = pl.program_id(0)
    core = core_ref[0]
    n, kp = plan.n, plan.k_pad

    @pl.when(step == 0)
    def _():
        tmp_ref[...] = jnp.zeros(tmp_ref.shape, F32)

    live = (2 * step < plan.y_blk).astype(F32)
    tmp_ref[:, :, :plan.z_blk] = gas_ref[...] * live
    data = jnp.concatenate([rho_ref[y, :n, :] + tmp_ref[y] for y in range(2)], axis=1)
    parts = split3(data)
    for half, out in ((core, own_ref), (1 - core, send_ref)):
        res = mul6([mx_ref[m, half] for m in range(3)], parts)
        for y in range(2):
            for ri in range(2):
                out[ri, y] = res[ri * kp:(ri + 1) * kp, y * LANES:(y + 1) * LANES]


def x_call(plan, core, rho, gas, mx):
    steps = plan.y_even // 2
    last = plan.y_blk // 2 - 1
    shape = jax.ShapeDtypeStruct((2, plan.y_even, plan.k_pad, LANES), F32)
    out_spec = pl.BlockSpec((2, 2, plan.k_pad, LANES), lambda i: (0, i, 0, 0))
    return pl.pallas_call(
        functools.partial(x_kernel, plan), grid=(steps,), out_shape=(shape, shape),
        in_specs=[SMEM_SPEC, pl.BlockSpec((2, plan.x_pad, LANES), lambda i: (i, 0, 0)),
                  pl.BlockSpec((2, plan.n, plan.z_blk), lambda i: (jnp.minimum(i, last), 0, 0)),
                  pl.BlockSpec(mx.shape, lambda i: (0, 0, 0, 0))],
        out_specs=(out_spec, out_spec),
        scratch_shapes=[pltpu.VMEM((2, plan.n, LANES), F32)], name="dft_x",
    )(core, rho, gas, mx)


Z_BATCH = 5


def z_kernel(plan, core_ref, own_ref, rec_ref, wz_ref, out_ref):
    step = pl.program_id(0)
    core = core_ref[0]
    kp, sl, ye = plan.k_pad, plan.slots, plan.y_ext

    @pl.when(step == 0)
    def _():
        for t in range(plan.n_chip):
            for g in range(3):
                out_ref[t, g, plan.rows - 8:plan.rows, :] = jnp.zeros((8, LANES), F32)

    flat = (Z_BATCH * kp, LANES)
    data = jnp.concatenate([own_ref[0].reshape(flat), rec_ref[0].reshape(flat),
                            own_ref[1].reshape(flat), rec_ref[1].reshape(flat)], axis=1)
    wts = [jnp.concatenate([wz_ref[m, core, 0], wz_ref[m, 1 - core, 0], wz_ref[m, core, 1], wz_ref[m, 1 - core, 1]], axis=0)
           for m in range(3)]
    res = mul6(split3(data), wts)
    for b in range(Z_BATCH):
        y = step * Z_BATCH + b

        @pl.when(y < ye)
        def _():
            for t in range(plan.n_chip):
                for g in range(3):
                    r0 = b * kp + t * sl
                    out_ref[t, g, pl.ds(y, sl, stride=ye), :] = res[r0:r0 + sl, g * LANES:(g + 1) * LANES]


def z_call(plan, core, own, rec, wz):
    blk = pl.BlockSpec((2, Z_BATCH, plan.k_pad, LANES), lambda i: (0, i, 0, 0))
    shape = (plan.n_chip, 3, plan.rows, LANES)
    return pl.pallas_call(
        functools.partial(z_kernel, plan), grid=(plan.y_even // Z_BATCH,),
        out_shape=jax.ShapeDtypeStruct(shape, F32),
        in_specs=[SMEM_SPEC, blk, blk, pl.BlockSpec(wz.shape, lambda i: (0,) * 5)],
        out_specs=pl.BlockSpec(shape, lambda i: (0, 0, 0, 0)),
        compiler_params=pltpu.CompilerParams(vmem_limit_bytes=VMEM_BIG), name="dft_z",
    )(core, own, rec, wz)


def signed(ids, n):
    return jnp.where(ids < n // 2, ids, ids - n).astype(F32)


def y_kernel(plan, base_ref, rec_ref, my_ref, ei_ref, out_ref, buf_ref):
    n, ye, yp = plan.n, plan.y_ext, plan.y_pad
    k_unit = 2.0 * math.pi / n
    buf_ref[...] = jnp.zeros(buf_ref.shape, F32)
    tail = slice(plan.rows - 8, plan.rows)
    for i in range(plan.n_chip):
        for c in range(2):
            for g in range(3):
                out_ref[i, c, g, tail, :] = jnp.zeros((8, LANES), F32)
    lane = lax.broadcasted_iota(jnp.int32, (n, LANES), 1)
    ky = signed(lax.broadcasted_iota(jnp.int32, (n, LANES), 0), n)
    kz_a = signed(lane, n)
    kz_b = signed(128 + (lane & 63), n)
    yz_a, yz_b = ky * ky + kz_a * kz_a, ky * ky + kz_b * kz_b
    flip = jnp.where(lax.broadcasted_iota(jnp.int32, (1, LANES), 1) < 64, 1.0, -1.0)

    def slot(s, energy):
        rows = pl.ds(s * ye, ye)
        for i in range(plan.n_chip):
            for g in range(3):
                buf_ref[g, i * yp:i * yp + ye, :] = rec_ref[i, g, rows, :]
        data = jnp.concatenate([buf_ref[g] for g in range(3)], axis=1)
        q = mul6([my_ref[m] for m in range(3)], split3(data))
        c = [q[:n, g * LANES:(g + 1) * LANES] for g in range(3)]
        d = [q[n:, g * LANES:(g + 1) * LANES] for g in range(3)]
        r0 = c[0] + d[1]
        r1 = c[1] - d[0]
        r2 = c[2] + flip * pltpu.roll(d[2], 64, 1)
        kx_i = base_ref[0] + s
        kx = kx_i.astype(F32)
        weight = jnp.where(kx_i < n // 2, jnp.where(kx_i == 0, 1.0, 2.0), jnp.where(kx_i == n // 2, 1.0, 0.0))
        scale = -4.0 * math.pi * GRAV_CONST / (k_unit * k_unit)

        def influence(yz):
            sq = yz + kx * kx
            return jnp.where(sq > 0, scale / jnp.maximum(sq, 1.0), 0.0)
        g_a, g_b = influence(yz_a), influence(yz_b)
        power = g_a * (r0 * r0 + r1 * r1) + g_b * (r2 * r2)
        energy = energy + weight * jnp.sum(power, axis=0, keepdims=True)
        parts = split3(jnp.concatenate([g_a * r0, g_a * r1, g_b * r2], axis=1))
        for i in range(plan.n_chip):
            p = mul6([ei_ref[m, i] for m in range(3)], parts)
            blk = [[p[u * yp:(u + 1) * yp, g * LANES:(g + 1) * LANES] for g in range(3)] for u in range(4)]
            co, si, ck, sk = blk
            pot = (co[0] - si[1], co[1] + si[0], co[2] - flip * pltpu.roll(si[2], 64, 1))
            dy = (-(ck[1] + sk[0]), ck[0] - sk[1], -flip * pltpu.roll(ck[2], 64, 1) - sk[2])
            for comp, val in ((0, pot), (1, dy)):
                for g in range(3):
                    out_ref[i, comp, g, rows, :] = val[g][:ye]
        return energy

    energy = lax.fori_loop(0, plan.slots, slot, jnp.zeros((1, LANES), F32))
    e_row = plan.slots * ye
    for i in range(plan.n_chip):
        out_ref[i, 0, 0, e_row:e_row + 1, :] = energy


def y_call(plan, base, rec, my, ei):
    return pl.pallas_call(
        functools.partial(y_kernel, plan),
        out_shape=jax.ShapeDtypeStruct((plan.n_chip, 2, 3, plan.rows, LANES), F32),
        in_specs=[SMEM_SPEC, VMEM_SPEC, VMEM_SPEC, VMEM_SPEC], out_specs=VMEM_SPEC,
        scratch_shapes=[pltpu.VMEM((3, plan.n_chip * plan.y_pad, LANES), F32)],
        compiler_params=pltpu.CompilerParams(vmem_limit_bytes=VMEM_BIG), name="dft_y",
    )(base, rec, my, ei)


def zi_kernel(plan, core_ref, rec_ref, wi_ref, own_ref, send_ref, buf_ref):
    step = pl.program_id(0)
    core = core_ref[0]
    kp, sl, ye = plan.k_pad, plan.slots, plan.y_ext

    @pl.when(step == 0)
    def _():
        buf_ref[...] = jnp.zeros(buf_ref.shape, F32)

    for comp in range(2):
        for b in range(Z_BATCH):
            for t in range(plan.n_chip):
                for g in range(3):
                    buf_ref[comp, b, t * sl:(t + 1) * sl, g * LANES:(g + 1) * LANES] = (
                        rec_ref[t, comp, g, pl.ds(step * Z_BATCH + b, sl, stride=ye), :])
    half_rows = Z_BATCH * kp
    parts = split3(buf_ref[...].reshape(2 * half_rows, 2 * plan.n))
    pot = [p[:half_rows] for p in parts]
    for half, out in ((core, own_ref), (1 - core, send_ref)):
        plain = mul6(parts, [wi_ref[m, half, :, :2 * LANES] for m in range(3)])
        along = mul6(pot, [wi_ref[m, half, :, 2 * LANES:] for m in range(3)])
        for b in range(Z_BATCH):
            for ri in range(2):
                ln = slice(ri * LANES, (ri + 1) * LANES)
                out[0, ri, b] = plain[b * kp:(b + 1) * kp, ln]
                out[1, ri, b] = plain[half_rows + b * kp:half_rows + (b + 1) * kp, ln]
                out[2, ri, b] = along[b * kp:(b + 1) * kp, ln]

    @pl.when(step == pl.num_programs(0) - 1)
    def _():
        e_row = plan.slots * ye
        total = rec_ref[0, 0, 0, e_row:e_row + 1, :]
        for t in range(1, plan.n_chip):
            total = total + rec_ref[t, 0, 0, e_row:e_row + 1, :]
        own_ref[0, 0, Z_BATCH - 1, 0:1, :] = total
        send_ref[0, 0, Z_BATCH - 1, 0:1, :] = total


def zi_call(plan, core, rec, wi):
    shape = jax.ShapeDtypeStruct((3, 2, plan.y_even, plan.k_pad, LANES), F32)
    spec = pl.BlockSpec((3, 2, Z_BATCH, plan.k_pad, LANES), lambda i: (0, 0, i, 0, 0))
    return pl.pallas_call(
        functools.partial(zi_kernel, plan), grid=(plan.y_even // Z_BATCH,), out_shape=(shape, shape),
        in_specs=[SMEM_SPEC, pl.BlockSpec(rec.shape, lambda i: (0,) * 5), pl.BlockSpec(wi.shape, lambda i: (0,) * 4)],
        out_specs=(spec, spec),
        scratch_shapes=[pltpu.VMEM((2, Z_BATCH, plan.k_pad, 2 * plan.n), F32)],
        compiler_params=pltpu.CompilerParams(vmem_limit_bytes=VMEM_BIG), name="idft_z",
    )(core, rec, wi)


def field_kernel(plan, n_blk, n_xt, e_norm, core_ref, table_ref, num_ref, slot_ref, own_ref, rec_ref, mi_ref,
                 out_ref, energy_ref, fhm_ref, flo_ref, lhs_ref):
    core = core_ref[0]
    kp = plan.k_pad
    for m in range(3):
        for kind in range(2):
            lhs_ref[m, kind] = jnp.concatenate([mi_ref[m, core, kind], mi_ref[m, 1 - core, kind]], axis=1)

    def column(c, y):
        return jnp.concatenate([own_ref[c, 0, y], own_ref[c, 1, y], rec_ref[c, 0, y], rec_ref[c, 1, y]], axis=0)

    def put(res, spots):
        hi, mid, lo = split3(res)
        for pos, (y, c) in enumerate(spots):
            ln = slice(pos * LANES, (pos + 1) * LANES)
            fhm_ref[y, c, :, :LANES] = hi[:, ln]
            fhm_ref[y, c, :, LANES:] = mid[:, ln]
            flo_ref[y, c] = lo[:, ln]

    def planes(step, carry):
        y0 = 2 * step
        data = jnp.concatenate([column(0, y0), column(0, y0 + 1)], axis=1)
        put(mul6([lhs_ref[m, 0] for m in range(3)], split3(data)), ((y0, 0), (y0 + 1, 0)))
        for y in (y0, y0 + 1):
            data = jnp.concatenate([column(1, y), column(2, y)], axis=1)
            put(mul6([lhs_ref[m, 1] for m in range(3)], split3(data)), ((y, 1), (y, 2)))
        return carry
    lax.fori_loop(0, plan.y_even // 2, planes, 0)
    lanes = own_ref[0, 0, plan.y_even - 1, 0:1, :] + rec_ref[0, 0, plan.y_even - 1, 0:1, :]
    energy_ref[...] = jnp.broadcast_to(jnp.sum(lanes, axis=1, keepdims=True) * e_norm, energy_ref.shape)
    interp_kernel(n_blk, n_xt, table_ref, num_ref, slot_ref, fhm_ref, flo_ref, out_ref)


def field_call(plan, core, table, num, slots, own, rec, mi, n_blk, n_xt, e_norm):
    return pl.pallas_call(
        functools.partial(field_kernel, plan, n_blk, n_xt, e_norm),
        out_shape=(jax.ShapeDtypeStruct((3, 128, LANES), F32), jax.ShapeDtypeStruct((8, LANES), F32)),
        in_specs=[SMEM_SPEC, SMEM_SPEC, SMEM_SPEC] + [VMEM_SPEC] * 4, out_specs=(VMEM_SPEC, VMEM_SPEC),
        scratch_shapes=[pltpu.VMEM((plan.y_even, 3, plan.x_pad, 2 * LANES), BF16),
                        pltpu.VMEM((plan.y_even, 3, plan.x_pad, LANES), BF16),
                        pltpu.VMEM((3, 2, plan.x_pad, 4 * plan.k_pad), BF16)],
        compiler_params=pltpu.CompilerParams(vmem_limit_bytes=VMEM_BIG), name="idft_x_interp",
    )(core, table, num, slots, own, rec, mi)


def solution(mesh):
    n_cols = mesh.shape["col"]
    n_cx = mesh.shape["row"] // 2
    fine = jax.sharding.Mesh(mesh.devices.reshape(mesh.shape["rep"], n_cols, n_cx, 2), ("rep", "col", "cx", "core"))
    slot_axes = ("rep", "col", "cx", "core")
    chip_axes = ("cx", "col")
    turn = [(a * 2 + b, b * 2 + a) for a in range(n_cols) for b in range(2)]
    other_core = [(0, 1), (1, 0)]

    def device_body(part_mass, cell_idx, cic_wts, live_mask, gas_block):
        grid_size, y_blk, z_blk = gas_block.shape
        per_dev = part_mass.shape[0]
        n_chip = n_cx * n_cols
        n_slots = per_dev * n_chip * 2
        plan = Plan(grid_size, n_chip, y_blk, z_blk)
        tab = plan.tables()
        core = lax.axis_index("core").astype(jnp.int32)
        chip = (lax.axis_index("cx") * n_cols + lax.axis_index("col")).astype(jnp.int32)
        core_arr = core.reshape(1)
        base = (core * plan.per_core + chip * plan.slots).reshape(1)
        n_xt = grid_size // X_TILE
        n_blk = y_blk * n_xt

        raw = lax.ppermute(slot_arrays(part_mass, cell_idx, cic_wts, live_mask, y_blk), ("col", "core"), turn)
        gas = lax.ppermute(jnp.transpose(gas_block, (1, 0, 2)), ("col", "core"), turn)
        table, num = pair_table(raw[0].reshape(-1), n_blk, n_xt)
        slots = sort_call(jnp.concatenate([raw, home_ranks()[None]]))
        rho = deposit_call(table, num, slots, plan.y_even, grid_size, n_blk, n_xt)
        own, send = x_call(plan, core_arr, rho, gas, tab["mx"])
        rec = lax.ppermute(send, "core", other_core)
        to_y = z_call(plan, core_arr, own, rec, tab["wz"])
        at_y = lax.all_to_all(to_y, chip_axes, 0, 0, tiled=True)
        from_y = y_call(plan, base, at_y, tab["my"], tab["ei"])
        at_z = lax.all_to_all(from_y, chip_axes, 0, 0, tiled=True)
        own, send = zi_call(plan, core_arr, at_z, tab["wi"])
        rec = lax.ppermute(send, "core", other_core)
        e_norm = 0.5 / (grid_size ** 3 * n_slots)
        forces, energy = field_call(plan, core_arr, table, num, slots, own, rec, tab["mi"], n_blk, n_xt, e_norm)
        back = sort_call(jnp.concatenate([slots[5:6], forces]))
        home = lax.ppermute(back[1:4], ("col", "core"), turn)
        return home.reshape(3, per_dev).T, energy[0, 0:1]

    return jax.shard_map(
        device_body, mesh=fine,
        in_specs=(P(slot_axes), P(slot_axes, None), P(slot_axes, None, None), P(slot_axes), P("rep", ("cx", "core"), "col")),
        out_specs=(P(slot_axes, None), P("rep")), check_vma=False)
```

```python
import functools
import math
import numpy as np
import jax
import jax.numpy as jnp
from jax import lax
from jax.sharding import PartitionSpec as P
from jax.experimental import pallas as pl
from jax.experimental.pallas import tpu as pltpu

MATMUL_PREC = lax.Precision.HIGHEST
GRAV_CONST = 1.0
F32 = jnp.float32
BF16 = jnp.bfloat16
LANES = 128
X_TILE = 96
X_ROWS = 112
Y_SHIFT = 15
X_SHIFT = 7
VMEM_BIG = 60 * 1024 * 1024


def split3(val):
    hi = val.astype(BF16)
    rest = val - hi.astype(F32)
    mid = rest.astype(BF16)
    lo = (rest - mid.astype(F32)).astype(BF16)
    return hi, mid, lo


def bitonic(bufs):
    sub = lax.broadcasted_iota(jnp.int32, (8, LANES), 0)
    lane = lax.broadcasted_iota(jnp.int32, (8, LANES), 1)
    base = lane * 128 + sub

    def bit(rank, pos):
        return lax.shift_right_logical(rank, jnp.full_like(rank, pos)) & 1

    def vreg_stage(k, j):
        step = 1 << (j - 3)
        for v in range(16):
            if v & step:
                continue
            low, high = pl.ds(8 * v, 8), pl.ds(8 * (v + step), 8)
            sgn = 1.0 - 2.0 * bit(base + 8 * v, k).astype(F32)
            a = [b[low, :] for b in bufs]
            c = [b[high, :] for b in bufs]
            swap = a[0] * sgn > c[0] * sgn
            for b, p, q in zip(bufs, a, c):
                b[low, :] = jnp.where(swap, q, p)
                b[high, :] = jnp.where(swap, p, q)

    def roll_stage(k, j, dist, axis):
        size = (8, LANES)[axis]
        upper = bit(base, j)
        keep_low = upper == 0
        for v in range(16):
            rows = pl.ds(8 * v, 8)
            sgn = 1.0 - 2.0 * (bit(base + 8 * v, k) ^ upper).astype(F32)
            own = [b[rows, :] for b in bufs]
            other = [jnp.where(keep_low, pltpu.roll(o, size - dist, axis), pltpu.roll(o, dist, axis)) for o in own]
            take = other[0] * sgn < own[0] * sgn
            for b, o, p in zip(bufs, own, other):
                b[rows, :] = jnp.where(take, p, o)

    def stage(k, j):
        if j >= 3:
            vreg_stage(k, j)
        else:
            roll_stage(k, j, 1 << j, 0)

    for k in range(1, 8):
        for j in range(k - 1, -1, -1):
            stage(k, j)

    def phase(k, carry):
        def lane_stage(step, c):
            j = k - 1 - step
            roll_stage(k, j, jnp.left_shift(1, j - 7), 1)
            return c
        lax.fori_loop(0, k - 7, lane_stage, 0)
        for j in range(6, -1, -1):
            stage(k, j)
        return carry
    lax.fori_loop(8, 15, phase, 0)


CHUNKS = 128
SLOT_ROWS = 8 * (CHUNKS + 1)


def sort_kernel(in_ref, out_ref, *bufs):
    for n in range(5):
        bufs[n][...] = in_ref[n]
    row = lax.broadcasted_iota(jnp.int32, (CHUNKS, LANES), 0)
    col = lax.broadcasted_iota(jnp.int32, (CHUNKS, LANES), 1)
    bufs[5][...] = (row * LANES + col).astype(F32)
    bitonic(bufs)
    zero = jnp.zeros((CHUNKS, LANES), F32)
    for n in range(8):
        out_ref[pl.ds(n, CHUNKS, stride=8), :] = bufs[n][...].T if n < 6 else zero
    out_ref[8 * CHUNKS:, :] = jnp.zeros((8, LANES), F32)


def unsort_kernel(slot_ref, force_ref, out_ref, *bufs):
    bufs[0][...] = slot_ref[pl.ds(5, CHUNKS, stride=8), :]
    for n in range(3):
        bufs[n + 1][...] = force_ref[pl.ds(n, CHUNKS, stride=8), :]
    bitonic(bufs)
    for n in range(3):
        out_ref[n] = bufs[n + 1][...].T


def pair_table(key, n_blk, n_xt):
    b_ids = jnp.arange(n_blk + 1)
    bounds = ((b_ids // n_xt) << Y_SHIFT) | (((b_ids % n_xt) * X_TILE) << X_SHIFT)
    starts = jnp.sum((key[None, :] < bounds[:, None].astype(F32)).astype(jnp.int32), axis=1)
    first, last = starts[:-1], starts[1:]
    count = (last - first + LANES - 1) // LANES
    ids = jnp.arange(n_blk)
    ends = jnp.sum(jnp.where(ids[None, :] <= ids[:, None], count[None, :], 0), axis=1)
    t_ids = jnp.arange(n_blk + CHUNKS)
    blk = jnp.sum((ends[None, :] <= t_ids[:, None]).astype(jnp.int32), axis=1)
    hot = ids[None, :] == blk[:, None]
    beg = jnp.sum(jnp.where(hot, (first - LANES * (ends - count))[None, :], 0), axis=1) + LANES * t_ids
    size = jnp.minimum(jnp.sum(jnp.where(hot, last[None, :], 0), axis=1) - beg, LANES)
    live = t_ids < ends[-1]
    table = jnp.stack([jnp.where(live, blk, 0), jnp.where(live, beg, 0), jnp.where(live, size, 0)])
    return table.astype(jnp.int32), ends[-1:].astype(jnp.int32)


def read_window(t, table_ref, slot_ref, n_xt):
    blk = table_ref[0, t]
    beg = table_ref[1, t]
    size = table_ref[2, t]
    y_pl = blk // n_xt
    x_beg = pl.multiple_of((blk % n_xt) * X_TILE, 16)
    row = pl.multiple_of((beg >> 7) * 8, 8)
    off = beg & 127
    back = (LANES - off) & 127
    lane = lax.broadcasted_iota(jnp.int32, (8, LANES), 1)
    win = jnp.where(lane < LANES - off, pltpu.roll(slot_ref[pl.ds(row, 8), :], back, 1),
                    pltpu.roll(slot_ref[pl.ds(row + 8, 8), :], back, 1))
    code = win[0:1].astype(jnp.int32)
    x_c = (code >> X_SHIFT) & 255
    vals = [win[n:n + 1] for n in range(1, 5)]
    return row, off, size, lane, y_pl, x_beg, x_c - x_beg, code & 127, vals


def spread_rows(row):
    return jnp.broadcast_to(row, (16, LANES)).astype(BF16)


def deposit_kernel(n_xt, grid_size, table_ref, num_ref, slot_ref, rho_ref):
    n_planes = rho_ref.shape[0]

    def clear(y, c):
        rho_ref[y] = jnp.zeros(rho_ref.shape[1:], F32)
        return c
    lax.fori_loop(0, n_planes, clear, 0)
    row_x = lax.broadcasted_iota(jnp.int32, (X_ROWS, LANES), 0)
    row_z = lax.broadcasted_iota(jnp.int32, (LANES, LANES), 0)

    def one(t):
        row, off, size, lane, y_pl, x_beg, x_l, z_c, (q, wx, wy, wz) = read_window(t, table_ref, slot_ref, n_xt)
        q = jnp.where(lane[0:1] < size, q, 0.0)
        pick_x = jnp.concatenate([(row_x == x_l).astype(F32), (row_x == x_l + 1).astype(F32)], axis=1).astype(BF16)
        pick_z = [(row_z == z_c + c).astype(F32).astype(BF16).reshape(8, 16, LANES) for c in range(2)]
        cols = [[], [], []]
        for w_y in (1.0 - wy, wy):
            pieces = [[], [], []]
            for w_x in (1.0 - wx, wx):
                base = q * w_x * w_y
                lower, upper = split3(base * (1.0 - wz)), split3(base * wz)
                for m in range(3):
                    low = spread_rows(lower[m].astype(F32))[None]
                    high = spread_rows(upper[m].astype(F32))[None]
                    pieces[m].append((pick_z[0] * low + pick_z[1] * high).reshape(LANES, LANES))
            for m in range(3):
                cols[m].append(jnp.concatenate(pieces[m], axis=1))
        res = None
        for m in (2, 1, 0):
            part = jnp.concatenate(cols[m], axis=0)
            term = lax.dot_general(pick_x, part, (((1,), (1,)), ((), ())), preferred_element_type=F32)
            res = term if res is None else res + term
        for b in range(2):
            rho_ref[y_pl + b, pl.ds(x_beg, X_ROWS), :] += res[:, b * LANES:(b + 1) * LANES]

    def body(t, c):
        one(2 * t)
        one(2 * t + 1)
        return c
    lax.fori_loop(0, (num_ref[0] + 1) // 2, body, 0)

    def wrap(y, c):
        rho_ref[y, 0:8, :] += rho_ref[y, grid_size:grid_size + 8, :]
        return c
    lax.fori_loop(0, n_planes, wrap, 0)


def interp_kernel(n_xt, table_ref, num_ref, slot_ref, fhm_ref, flo_ref, out_ref):
    row_x = lax.broadcasted_iota(jnp.int32, (X_ROWS, LANES), 0)
    row_z = lax.broadcasted_iota(jnp.int32, (LANES, LANES), 0)
    out_ref[...] = jnp.zeros(out_ref.shape, F32)

    def one(t):
        row, off, size, lane, y_pl, x_beg, x_l, z_c, (q, wx, wy, wz) = read_window(t, table_ref, slot_ref, n_xt)
        pick_z = jnp.concatenate([(row_z == z_c).astype(F32), (row_z == z_c + 1).astype(F32)], axis=1).astype(BF16)
        pick_2 = jnp.concatenate([pick_z, pick_z], axis=0)
        on_x = jnp.where(row_x == x_l, 1.0 - wx, jnp.where(row_x == x_l + 1, wx, 0.0))
        rows = pl.ds(x_beg, X_ROWS)
        wt = [on_x * (1.0 - wy), on_x * wy]
        grads = []
        for comp in range(3):
            top = jnp.concatenate([fhm_ref[y_pl + b, comp, rows, :] for b in range(2)], axis=0)
            low = jnp.concatenate([flo_ref[y_pl + b, comp, rows, :] for b in range(2)], axis=0)
            got = jnp.dot(low, pick_z, preferred_element_type=F32) + jnp.dot(top, pick_2, preferred_element_type=F32)
            got = got[:, :LANES] * (1.0 - wz) + got[:, LANES:] * wz
            acc = got[:X_ROWS] * wt[0] + got[X_ROWS:] * wt[1]
            grads.append(-q * jnp.sum(acc, axis=0, keepdims=True))
        full = pltpu.roll(jnp.concatenate(grads + [jnp.zeros((5, LANES), F32)], axis=0), off, 1)
        here, after = pl.ds(row, 8), pl.ds(row + 8, 8)
        out_ref[here, :] = jnp.where((lane >= off) & (lane - off < size), full, out_ref[here, :])
        out_ref[after, :] = jnp.where((lane < off) & (lane + LANES - off < size), full, out_ref[after, :])

    def body(t, c):
        one(2 * t)
        one(2 * t + 1)
        return c
    lax.fori_loop(0, (num_ref[0] + 1) // 2, body, 0)


SMEM_SPEC = pl.BlockSpec(memory_space=pltpu.SMEM)
VMEM_SPEC = pl.BlockSpec(memory_space=pltpu.VMEM)


def sort_call(raw):
    return pl.pallas_call(
        sort_kernel, out_shape=jax.ShapeDtypeStruct((SLOT_ROWS, LANES), F32), in_specs=[VMEM_SPEC], out_specs=VMEM_SPEC,
        scratch_shapes=[pltpu.VMEM((CHUNKS, LANES), F32)] * 6, name="slot_sort",
    )(raw)


def unsort_call(slots, forces):
    return pl.pallas_call(
        unsort_kernel, out_shape=jax.ShapeDtypeStruct((3, CHUNKS, LANES), F32),
        in_specs=[VMEM_SPEC, VMEM_SPEC], out_specs=VMEM_SPEC,
        scratch_shapes=[pltpu.VMEM((CHUNKS, LANES), F32)] * 4, name="slot_unsort",
    )(slots, forces)


def deposit_call(table, num, slots, y_ext, grid_size, n_xt):
    return pl.pallas_call(
        functools.partial(deposit_kernel, n_xt, grid_size),
        out_shape=jax.ShapeDtypeStruct((y_ext, grid_size + 16, LANES), F32),
        in_specs=[SMEM_SPEC, SMEM_SPEC, VMEM_SPEC], out_specs=VMEM_SPEC,
        compiler_params=pltpu.CompilerParams(vmem_limit_bytes=VMEM_BIG), name="deposit",
    )(table, num, slots)


def slot_arrays(part_mass, cell_idx, cic_wts, live_mask, y_blk):
    charge = part_mass * live_mask.astype(F32)
    code = (cell_idx[:, 1] << Y_SHIFT) | (cell_idx[:, 0] << X_SHIFT) | cell_idx[:, 2]
    code = jnp.where(live_mask > 0, code, y_blk << Y_SHIFT).astype(F32)
    upper = cic_wts[:, :, 1]
    return jnp.stack([code, charge, upper[:, 0], upper[:, 1], upper[:, 2]]).reshape(5, CHUNKS, LANES)


def mul6(a, b):
    res = None
    for m, n in ((2, 0), (0, 2), (1, 1), (1, 0), (0, 1), (0, 0)):
        term = jnp.dot(a[m], b[n], preferred_element_type=F32)
        res = term if res is None else res + term
    return res


def table3(mat):
    mat = mat.astype(np.float32)
    hi = mat.astype(BF16)
    mid = (mat - hi.astype(np.float32)).astype(BF16)
    lo = (mat - hi.astype(np.float32) - mid.astype(np.float32)).astype(BF16)
    return np.stack([hi, mid, lo])


class Plan:
    def __init__(self, n, n_chip, y_blk, z_blk):
        self.n, self.n_chip, self.y_blk, self.z_blk = n, n_chip, y_blk, z_blk
        self.y_ext = y_blk + 1
        self.z_ext = z_blk + 1
        self.y_pad = -(-self.y_ext // 8) * 8
        self.half_k = n // 2 + 1
        self.slots = -(-self.half_k // (2 * n_chip))
        self.per_core = self.slots * n_chip
        self.k_pad = -(-self.per_core // 8) * 8
        self.rows = -(-(self.slots * self.y_ext + 1) // 8) * 8
        self.y_even = self.y_ext + self.y_ext % 2
        self.x_pad = n + 16

    def angle(self, k, r):
        return 2.0 * np.pi / self.n * ((k[:, None] * r[None, :]) % self.n)

    def lane_order(self):
        kz = np.concatenate([np.arange(128), np.arange(128), np.arange(128, self.n), np.arange(128, self.n)])
        im = np.concatenate([np.zeros(128), np.ones(128), np.zeros(self.n - 128), np.ones(self.n - 128)]) > 0
        return kz, im

    def deriv(self, k):
        sgn = np.where(k < self.n // 2, k, k - self.n)
        return np.where(k == self.n // 2, 0, sgn) * (2.0 * np.pi / self.n)

    def tables(self):
        n = self.n
        out = {}
        mx = np.zeros((2, 2, self.k_pad, n))
        mi = np.zeros((2, 2, self.x_pad, 2, self.k_pad))
        for h in range(2):
            kx = h * self.per_core + np.arange(self.per_core)
            ok = (kx < self.half_k)[:, None]
            th = self.angle(kx, np.arange(n))
            mx[h, 0, :self.per_core] = np.where(ok, np.cos(th), 0.0)
            mx[h, 1, :self.per_core] = np.where(ok, -np.sin(th), 0.0)
            th = self.angle(kx, np.arange(self.x_pad))
            wt = np.where(kx < self.half_k, np.where((kx == 0) | (kx == n // 2), 1.0, 2.0), 0.0) / float(n) ** 3
            kd = np.where(kx < n // 2, kx, 0) * (2.0 * np.pi / n) * wt
            mi[h, 0, :, 0, :self.per_core] = (-kd[:, None] * np.sin(th)).T
            mi[h, 0, :, 1, :self.per_core] = (-kd[:, None] * np.cos(th)).T
            mi[h, 1, :, 0, :self.per_core] = (wt[:, None] * np.cos(th)).T
            mi[h, 1, :, 1, :self.per_core] = (-wt[:, None] * np.sin(th)).T
        out["mx"] = table3(mx.reshape(2, 2 * self.k_pad, n))
        out["mi"] = table3(mi.reshape(2, 2, self.x_pad, 2 * self.k_pad))
        kz, im = self.lane_order()
        wz = np.zeros((2, 2, LANES, 2 * n))
        wi = np.zeros((2, 2 * n, 4, LANES))
        kd = self.deriv(kz)[:, None]
        for h in range(2):
            z = (h * self.z_blk + np.arange(self.z_ext)) % n
            c, s = np.cos(self.angle(kz, z)), np.sin(self.angle(kz, z))
            wz[h, 0, :self.z_ext] = np.where(im[:, None], -s, c).T
            wz[h, 1, :self.z_ext] = np.where(im[:, None], c, s).T
            re_w, im_w = np.where(im[:, None], -s, c), np.where(im[:, None], c, s)
            wi[h, :, 0, :self.z_ext] = re_w
            wi[h, :, 1, :self.z_ext] = im_w
            wi[h, :, 2, :self.z_ext] = -kd * im_w
            wi[h, :, 3, :self.z_ext] = kd * re_w
        out["wz"] = table3(wz)
        out["wi"] = table3(wi.reshape(2, 2 * n, 4 * LANES))
        ky = np.arange(n)
        my = np.zeros((2, n, self.n_chip, self.y_pad))
        ei = np.zeros((self.n_chip, 4, self.y_pad, n))
        for i in range(self.n_chip):
            y = (i * self.y_blk + np.arange(self.y_ext)) % n
            th = self.angle(ky, y)
            my[0, :, i, :self.y_ext] = np.cos(th)
            my[1, :, i, :self.y_ext] = np.sin(th)
            ei[i, 0, :self.y_ext] = np.cos(th).T
            ei[i, 1, :self.y_ext] = np.sin(th).T
            ei[i, 2, :self.y_ext] = (self.deriv(ky)[:, None] * np.cos(th)).T
            ei[i, 3, :self.y_ext] = (self.deriv(ky)[:, None] * np.sin(th)).T
        out["my"] = table3(my.reshape(2 * n, self.n_chip * self.y_pad))
        out["ei"] = table3(ei.reshape(self.n_chip, 4 * self.y_pad, n))
        return out


def x_kernel(plan, core_ref, rho_ref, gas_ref, far_ref, mx_ref, own_ref, send_ref, tmp_ref):
    step = pl.program_id(0)
    core = core_ref[0]
    n, kp = plan.n, plan.k_pad

    @pl.when(step == 0)
    def _():
        tmp_ref[...] = jnp.zeros(tmp_ref.shape, F32)

    live = (2 * step < plan.y_blk).astype(F32)
    keep = live * core_ref[1].astype(F32)
    tmp_ref[:, :, :plan.z_blk] = gas_ref[...] * keep + far_ref[...] * live
    data = jnp.concatenate([rho_ref[y, :n, :] + tmp_ref[y] for y in range(2)], axis=1)
    parts = split3(data)
    lhs = [jnp.concatenate([mx_ref[m, core], mx_ref[m, 1 - core]], axis=0) for m in range(3)]
    res = mul6(lhs, parts)
    for h, out in enumerate((own_ref, send_ref)):
        for y in range(2):
            for ri in range(2):
                r0 = (2 * h + ri) * kp
                out[ri, y] = res[r0:r0 + kp, y * LANES:(y + 1) * LANES]


def x_call(plan, core, rho, gas, far, mx):
    steps = plan.y_even // 2
    last = plan.y_blk // 2 - 1
    shape = jax.ShapeDtypeStruct((2, plan.y_even, plan.k_pad, LANES), F32)
    out_spec = pl.BlockSpec((2, 2, plan.k_pad, LANES), lambda i: (0, i, 0, 0))
    gas_spec = pl.BlockSpec((2, plan.n, plan.z_blk), lambda i: (jnp.minimum(i, last), 0, 0))
    return pl.pallas_call(
        functools.partial(x_kernel, plan), grid=(steps,), out_shape=(shape, shape),
        in_specs=[SMEM_SPEC, pl.BlockSpec((2, plan.x_pad, LANES), lambda i: (i, 0, 0)),
                  gas_spec, gas_spec,
                  pl.BlockSpec(mx.shape, lambda i: (0, 0, 0, 0))],
        out_specs=(out_spec, out_spec),
        scratch_shapes=[pltpu.VMEM((2, plan.n, LANES), F32)], name="dft_x",
    )(core, rho, gas, far, mx)


Z_BATCH = 5


def z_kernel(plan, core_ref, own_ref, rec_ref, wz_ref, out_ref):
    step = pl.program_id(0)
    core = core_ref[0]
    kp, sl, ye = plan.k_pad, plan.slots, plan.y_ext

    @pl.when(step == 0)
    def _():
        for t in range(plan.n_chip):
            for g in range(3):
                out_ref[t, g, plan.rows - 8:plan.rows, :] = jnp.zeros((8, LANES), F32)

    flat = (Z_BATCH * kp, LANES)
    data = jnp.concatenate([own_ref[0].reshape(flat), rec_ref[0].reshape(flat),
                            own_ref[1].reshape(flat), rec_ref[1].reshape(flat)], axis=1)
    wts = [jnp.concatenate([wz_ref[m, core, 0], wz_ref[m, 1 - core, 0], wz_ref[m, core, 1], wz_ref[m, 1 - core, 1]], axis=0)
           for m in range(3)]
    res = mul6(split3(data), wts)
    for b in range(Z_BATCH):
        y = step * Z_BATCH + b

        @pl.when(y < ye)
        def _():
            for t in range(plan.n_chip):
                for g in range(3):
                    r0 = b * kp + t * sl
                    out_ref[t, g, pl.ds(y, sl, stride=ye), :] = res[r0:r0 + sl, g * LANES:(g + 1) * LANES]


def z_call(plan, core, own, rec, wz):
    blk = pl.BlockSpec((2, Z_BATCH, plan.k_pad, LANES), lambda i: (0, i, 0, 0))
    shape = (plan.n_chip, 3, plan.rows, LANES)
    return pl.pallas_call(
        functools.partial(z_kernel, plan), grid=(plan.y_even // Z_BATCH,),
        out_shape=jax.ShapeDtypeStruct(shape, F32),
        in_specs=[SMEM_SPEC, blk, blk, pl.BlockSpec(wz.shape, lambda i: (0,) * 5)],
        out_specs=pl.BlockSpec(shape, lambda i: (0, 0, 0, 0)),
        compiler_params=pltpu.CompilerParams(vmem_limit_bytes=VMEM_BIG), name="dft_z",
    )(core, own, rec, wz)


def signed(ids, n):
    return jnp.where(ids < n // 2, ids, ids - n).astype(F32)


def y_kernel(plan, base_ref, rec_ref, my_ref, ei_ref, out_ref, buf_ref):
    n, ye, yp = plan.n, plan.y_ext, plan.y_pad
    k_unit = 2.0 * math.pi / n
    buf_ref[...] = jnp.zeros(buf_ref.shape, F32)
    tail = slice(plan.rows - 8, plan.rows)
    for i in range(plan.n_chip):
        for c in range(2):
            for g in range(3):
                out_ref[i, c, g, tail, :] = jnp.zeros((8, LANES), F32)
    lane = lax.broadcasted_iota(jnp.int32, (n, LANES), 1)
    ky = signed(lax.broadcasted_iota(jnp.int32, (n, LANES), 0), n)
    kz_a = signed(lane, n)
    kz_b = signed(128 + (lane & 63), n)
    yz_a, yz_b = ky * ky + kz_a * kz_a, ky * ky + kz_b * kz_b
    flip = jnp.where(lax.broadcasted_iota(jnp.int32, (1, LANES), 1) < 64, 1.0, -1.0)

    def slot(s, energy):
        rows = pl.ds(s * ye, ye)
        for i in range(plan.n_chip):
            for g in range(3):
                buf_ref[g, i * yp:i * yp + ye, :] = rec_ref[i, g, rows, :]
        data = jnp.concatenate([buf_ref[g] for g in range(3)], axis=1)
        q = mul6([my_ref[m] for m in range(3)], split3(data))
        c = [q[:n, g * LANES:(g + 1) * LANES] for g in range(3)]
        d = [q[n:, g * LANES:(g + 1) * LANES] for g in range(3)]
        r0 = c[0] + d[1]
        r1 = c[1] - d[0]
        r2 = c[2] + flip * pltpu.roll(d[2], 64, 1)
        kx_i = base_ref[0] + s
        kx = kx_i.astype(F32)
        weight = jnp.where(kx_i < n // 2, jnp.where(kx_i == 0, 1.0, 2.0), jnp.where(kx_i == n // 2, 1.0, 0.0))
        scale = -4.0 * math.pi * GRAV_CONST / (k_unit * k_unit)

        def influence(yz):
            sq = yz + kx * kx
            return jnp.where(sq > 0, scale / jnp.maximum(sq, 1.0), 0.0)
        g_a, g_b = influence(yz_a), influence(yz_b)
        power = g_a * (r0 * r0 + r1 * r1) + g_b * (r2 * r2)
        energy = energy + weight * jnp.sum(power, axis=0, keepdims=True)
        parts = split3(jnp.concatenate([g_a * r0, g_a * r1, g_b * r2], axis=1))
        for i in range(plan.n_chip):
            if i % 2 == 0:
                two = mul6([ei_ref[m, i:i + 2].reshape(8 * yp, n) for m in range(3)], parts)
            p = two[(i % 2) * 4 * yp:(i % 2 + 1) * 4 * yp]
            blk = [[p[u * yp:(u + 1) * yp, g * LANES:(g + 1) * LANES] for g in range(3)] for u in range(4)]
            co, si, ck, sk = blk
            pot = (co[0] - si[1], co[1] + si[0], co[2] - flip * pltpu.roll(si[2], 64, 1))
            dy = (-(ck[1] + sk[0]), ck[0] - sk[1], -flip * pltpu.roll(ck[2], 64, 1) - sk[2])
            for comp, val in ((0, pot), (1, dy)):
                for g in range(3):
                    out_ref[i, comp, g, rows, :] = val[g][:ye]
        return energy

    energy = lax.fori_loop(0, plan.slots, slot, jnp.zeros((1, LANES), F32))
    e_row = plan.slots * ye
    for i in range(plan.n_chip):
        out_ref[i, 0, 0, e_row:e_row + 1, :] = energy


def y_call(plan, base, rec, my, ei):
    return pl.pallas_call(
        functools.partial(y_kernel, plan),
        out_shape=jax.ShapeDtypeStruct((plan.n_chip, 2, 3, plan.rows, LANES), F32),
        in_specs=[SMEM_SPEC, VMEM_SPEC, VMEM_SPEC, VMEM_SPEC], out_specs=VMEM_SPEC,
        scratch_shapes=[pltpu.VMEM((3, plan.n_chip * plan.y_pad, LANES), F32)],
        compiler_params=pltpu.CompilerParams(vmem_limit_bytes=VMEM_BIG), name="dft_y",
    )(base, rec, my, ei)


def zi_kernel(plan, core_ref, rec_ref, wi_ref, own_ref, send_ref, buf_ref):
    step = pl.program_id(0)
    core = core_ref[0]
    kp, sl, ye = plan.k_pad, plan.slots, plan.y_ext

    @pl.when(step == 0)
    def _():
        buf_ref[...] = jnp.zeros(buf_ref.shape, F32)

    for comp in range(2):
        for b in range(Z_BATCH):
            for t in range(plan.n_chip):
                for g in range(3):
                    buf_ref[comp, b, t * sl:(t + 1) * sl, g * LANES:(g + 1) * LANES] = (
                        rec_ref[t, comp, g, pl.ds(step * Z_BATCH + b, sl, stride=ye), :])
    half_rows = Z_BATCH * kp
    parts = split3(buf_ref[...].reshape(2 * half_rows, 2 * plan.n))
    pot = [p[:half_rows] for p in parts]
    for half, out in ((core, own_ref), (1 - core, send_ref)):
        plain = mul6(parts, [wi_ref[m, half, :, :2 * LANES] for m in range(3)])
        along = mul6(pot, [wi_ref[m, half, :, 2 * LANES:] for m in range(3)])
        for b in range(Z_BATCH):
            for ri in range(2):
                ln = slice(ri * LANES, (ri + 1) * LANES)
                out[0, ri, b] = plain[b * kp:(b + 1) * kp, ln]
                out[1, ri, b] = plain[half_rows + b * kp:half_rows + (b + 1) * kp, ln]
                out[2, ri, b] = along[b * kp:(b + 1) * kp, ln]

    @pl.when(step == pl.num_programs(0) - 1)
    def _():
        e_row = plan.slots * ye
        total = rec_ref[0, 0, 0, e_row:e_row + 1, :]
        for t in range(1, plan.n_chip):
            total = total + rec_ref[t, 0, 0, e_row:e_row + 1, :]
        own_ref[0, 0, Z_BATCH - 1, 0:1, :] = total
        send_ref[0, 0, Z_BATCH - 1, 0:1, :] = total


def zi_call(plan, core, rec, wi):
    shape = jax.ShapeDtypeStruct((3, 2, plan.y_even, plan.k_pad, LANES), F32)
    spec = pl.BlockSpec((3, 2, Z_BATCH, plan.k_pad, LANES), lambda i: (0, 0, i, 0, 0))
    return pl.pallas_call(
        functools.partial(zi_kernel, plan), grid=(plan.y_even // Z_BATCH,), out_shape=(shape, shape),
        in_specs=[SMEM_SPEC, pl.BlockSpec(rec.shape, lambda i: (0,) * 5), pl.BlockSpec(wi.shape, lambda i: (0,) * 4)],
        out_specs=(spec, spec),
        scratch_shapes=[pltpu.VMEM((2, Z_BATCH, plan.k_pad, 2 * plan.n), F32)],
        compiler_params=pltpu.CompilerParams(vmem_limit_bytes=VMEM_BIG), name="idft_z",
    )(core, rec, wi)


def field_kernel(plan, n_xt, e_norm, core_ref, table_ref, num_ref, slot_ref, own_ref, rec_ref, mi_ref,
                 out_ref, energy_ref, fhm_ref, flo_ref, lhs_ref):
    core = core_ref[0]
    kp = plan.k_pad
    for m in range(3):
        for kind in range(2):
            lhs_ref[m, kind] = jnp.concatenate([mi_ref[m, core, kind], mi_ref[m, 1 - core, kind]], axis=1)

    def column(c, y):
        return jnp.concatenate([own_ref[c, 0, y], own_ref[c, 1, y], rec_ref[c, 0, y], rec_ref[c, 1, y]], axis=0)

    def put(res, spots):
        hi, mid, lo = split3(res)
        for pos, (y, c) in enumerate(spots):
            ln = slice(pos * LANES, (pos + 1) * LANES)
            fhm_ref[y, c, :, :LANES] = hi[:, ln]
            fhm_ref[y, c, :, LANES:] = mid[:, ln]
            flo_ref[y, c] = lo[:, ln]

    def planes(step, carry):
        y0 = 2 * step
        data = jnp.concatenate([column(0, y0), column(0, y0 + 1)], axis=1)
        put(mul6([lhs_ref[m, 0] for m in range(3)], split3(data)), ((y0, 0), (y0 + 1, 0)))
        for y in (y0, y0 + 1):
            data = jnp.concatenate([column(1, y), column(2, y)], axis=1)
            put(mul6([lhs_ref[m, 1] for m in range(3)], split3(data)), ((y, 1), (y, 2)))
        return carry
    lax.fori_loop(0, plan.y_even // 2, planes, 0)
    lanes = own_ref[0, 0, plan.y_even - 1, 0:1, :] + rec_ref[0, 0, plan.y_even - 1, 0:1, :]
    energy_ref[...] = jnp.broadcast_to(jnp.sum(lanes, axis=1, keepdims=True) * e_norm, energy_ref.shape)
    interp_kernel(n_xt, table_ref, num_ref, slot_ref, fhm_ref, flo_ref, out_ref)


def field_call(plan, core, table, num, slots, own, rec, mi, n_xt, e_norm):
    return pl.pallas_call(
        functools.partial(field_kernel, plan, n_xt, e_norm),
        out_shape=(jax.ShapeDtypeStruct((SLOT_ROWS, LANES), F32), jax.ShapeDtypeStruct((8, LANES), F32)),
        in_specs=[SMEM_SPEC, SMEM_SPEC, SMEM_SPEC] + [VMEM_SPEC] * 4, out_specs=(VMEM_SPEC, VMEM_SPEC),
        scratch_shapes=[pltpu.VMEM((plan.y_even, 3, plan.x_pad, 2 * LANES), BF16),
                        pltpu.VMEM((plan.y_even, 3, plan.x_pad, LANES), BF16),
                        pltpu.VMEM((3, 2, plan.x_pad, 4 * plan.k_pad), BF16)],
        compiler_params=pltpu.CompilerParams(vmem_limit_bytes=VMEM_BIG), name="idft_x_interp",
    )(core, table, num, slots, own, rec, mi)


def solution(mesh):
    n_cols = mesh.shape["col"]
    n_cx = mesh.shape["row"] // 2
    fine = jax.sharding.Mesh(mesh.devices.reshape(mesh.shape["rep"], n_cols, n_cx, 2), ("rep", "col", "cx", "core"))
    slot_axes = ("rep", "col", "cx", "core")
    chip_axes = ("cx", "col")
    turn = [(a * 2 + b, b * 2 + a) for a in range(n_cols) for b in range(2) if a != b]
    other_core = [(0, 1), (1, 0)]

    def device_body(part_mass, cell_idx, cic_wts, live_mask, gas_block):
        grid_size, y_blk, z_blk = gas_block.shape
        per_dev = part_mass.shape[0]
        n_chip = n_cx * n_cols
        n_slots = per_dev * n_chip * 2
        plan = Plan(grid_size, n_chip, y_blk, z_blk)
        tab = plan.tables()
        core = lax.axis_index("core").astype(jnp.int32)
        chip = (lax.axis_index("cx") * n_cols + lax.axis_index("col")).astype(jnp.int32)
        core_arr = core.reshape(1)
        base = (core * plan.per_core + chip * plan.slots).reshape(1)
        n_xt = grid_size // X_TILE
        n_blk = y_blk * n_xt

        keep = (core == lax.axis_index("col")).astype(jnp.int32)

        def swap(arr):
            return lax.ppermute(arr, ("col", "core"), turn)

        raw = slot_arrays(part_mass, cell_idx, cic_wts, live_mask, y_blk)
        raw = swap(raw) + raw * keep.astype(F32)
        raw, gas = lax.optimization_barrier((raw, jnp.transpose(gas_block, (1, 0, 2))))
        gas_far = swap(gas)
        table, num = pair_table(raw[0].reshape(-1), n_blk, n_xt)
        slots = sort_call(raw)
        rho = deposit_call(table, num, slots, plan.y_even, grid_size, n_xt)
        own, send = x_call(plan, jnp.stack([core, keep]), rho, gas, gas_far, tab["mx"])
        rec = lax.ppermute(send, "core", other_core)
        to_y = z_call(plan, core_arr, own, rec, tab["wz"])
        at_y = lax.all_to_all(to_y, chip_axes, 0, 0, tiled=True)
        from_y = y_call(plan, base, at_y, tab["my"], tab["ei"])
        at_z = lax.all_to_all(from_y, chip_axes, 0, 0, tiled=True)
        own, send = zi_call(plan, core_arr, at_z, tab["wi"])
        rec = lax.ppermute(send, "core", other_core)
        e_norm = 0.5 / (grid_size ** 3 * n_slots)
        forces, energy = field_call(plan, core_arr, table, num, slots, own, rec, tab["mi"], n_xt, e_norm)
        back = unsort_call(slots, forces)
        home = swap(back) + back * keep.astype(F32)
        return home.reshape(3, per_dev).T, energy[0, 0:1]

    return jax.shard_map(
        device_body, mesh=fine,
        in_specs=(P(slot_axes), P(slot_axes, None), P(slot_axes, None, None), P(slot_axes), P("rep", ("cx", "core"), "col")),
        out_specs=(P(slot_axes, None), P("rep")), check_vma=False)
```

```python
import functools
import math
import numpy as np
import jax
import jax.numpy as jnp
from jax import lax
from jax.sharding import PartitionSpec as P
from jax.experimental import pallas as pl
from jax.experimental.pallas import tpu as pltpu

MATMUL_PREC = lax.Precision.HIGHEST
GRAV_CONST = 1.0
F32 = jnp.float32
BF16 = jnp.bfloat16
LANES = 128
X_TILE = 96
X_ROWS = 112
Y_SHIFT = 15
X_SHIFT = 7
VMEM_BIG = 60 * 1024 * 1024


def split3(val):
    hi = val.astype(BF16)
    rest = val - hi.astype(F32)
    mid = rest.astype(BF16)
    lo = (rest - mid.astype(F32)).astype(BF16)
    return hi, mid, lo


def bitonic(bufs):
    sub = lax.broadcasted_iota(jnp.int32, (8, LANES), 0)
    lane = lax.broadcasted_iota(jnp.int32, (8, LANES), 1)
    base = lane * 128 + sub

    def bit(rank, pos):
        return lax.shift_right_logical(rank, jnp.full_like(rank, pos)) & 1

    def vreg_stage(k, j):
        step = 1 << (j - 3)
        for v in range(16):
            if v & step:
                continue
            low, high = pl.ds(8 * v, 8), pl.ds(8 * (v + step), 8)
            sgn = 1.0 - 2.0 * bit(base + 8 * v, k).astype(F32)
            a = [b[low, :] for b in bufs]
            c = [b[high, :] for b in bufs]
            swap = a[0] * sgn > c[0] * sgn
            for b, p, q in zip(bufs, a, c):
                b[low, :] = jnp.where(swap, q, p)
                b[high, :] = jnp.where(swap, p, q)

    def roll_stage(k, j, dist, axis):
        size = (8, LANES)[axis]
        upper = bit(base, j)
        keep_low = upper == 0
        for v in range(16):
            rows = pl.ds(8 * v, 8)
            sgn = 1.0 - 2.0 * (bit(base + 8 * v, k) ^ upper).astype(F32)
            own = [b[rows, :] for b in bufs]
            other = [jnp.where(keep_low, pltpu.roll(o, size - dist, axis), pltpu.roll(o, dist, axis)) for o in own]
            take = other[0] * sgn < own[0] * sgn
            for b, o, p in zip(bufs, own, other):
                b[rows, :] = jnp.where(take, p, o)

    def stage(k, j):
        if j >= 3:
            vreg_stage(k, j)
        else:
            roll_stage(k, j, 1 << j, 0)

    for k in range(1, 8):
        for j in range(k - 1, -1, -1):
            stage(k, j)

    def phase(k, carry):
        def lane_stage(step, c):
            j = k - 1 - step
            roll_stage(k, j, jnp.left_shift(1, j - 7), 1)
            return c
        lax.fori_loop(0, k - 7, lane_stage, 0)
        for j in range(6, -1, -1):
            stage(k, j)
        return carry
    lax.fori_loop(8, 15, phase, 0)


CHUNKS = 128
SLOT_ROWS = 8 * (CHUNKS + 1)


def sort_kernel(in_ref, out_ref, *bufs):
    for n in range(5):
        bufs[n][...] = in_ref[n]
    row = lax.broadcasted_iota(jnp.int32, (CHUNKS, LANES), 0)
    col = lax.broadcasted_iota(jnp.int32, (CHUNKS, LANES), 1)
    bufs[5][...] = (row * LANES + col).astype(F32)
    bitonic(bufs)
    zero = jnp.zeros((CHUNKS, LANES), F32)
    for n in range(8):
        out_ref[pl.ds(n, CHUNKS, stride=8), :] = bufs[n][...].T if n < 6 else zero
    out_ref[8 * CHUNKS:, :] = jnp.zeros((8, LANES), F32)


def unsort_kernel(slot_ref, force_ref, out_ref, *bufs):
    bufs[0][...] = slot_ref[pl.ds(5, CHUNKS, stride=8), :]
    for n in range(3):
        bufs[n + 1][...] = force_ref[pl.ds(n, CHUNKS, stride=8), :]
    bitonic(bufs)
    for n in range(3):
        out_ref[n] = bufs[n + 1][...].T


def pair_table(key, n_blk, n_xt):
    b_ids = jnp.arange(n_blk + 1)
    bounds = ((b_ids // n_xt) << Y_SHIFT) | (((b_ids % n_xt) * X_TILE) << X_SHIFT)
    starts = jnp.sum((key[None, :] < bounds[:, None].astype(F32)).astype(jnp.int32), axis=1)
    first, last = starts[:-1], starts[1:]
    count = (last - first + LANES - 1) // LANES
    ids = jnp.arange(n_blk)
    ends = jnp.sum(jnp.where(ids[None, :] <= ids[:, None], count[None, :], 0), axis=1)
    t_ids = jnp.arange(n_blk + CHUNKS)
    blk = jnp.sum((ends[None, :] <= t_ids[:, None]).astype(jnp.int32), axis=1)
    hot = ids[None, :] == blk[:, None]
    beg = jnp.sum(jnp.where(hot, (first - LANES * (ends - count))[None, :], 0), axis=1) + LANES * t_ids
    size = jnp.minimum(jnp.sum(jnp.where(hot, last[None, :], 0), axis=1) - beg, LANES)
    live = t_ids < ends[-1]
    table = jnp.stack([jnp.where(live, blk, 0), jnp.where(live, beg, 0), jnp.where(live, size, 0)])
    return table.astype(jnp.int32), ends[-1:].astype(jnp.int32)


def read_window(t, table_ref, slot_ref, n_xt):
    blk = table_ref[0, t]
    beg = table_ref[1, t]
    size = table_ref[2, t]
    y_pl = blk // n_xt
    x_beg = pl.multiple_of((blk % n_xt) * X_TILE, 16)
    row = pl.multiple_of((beg >> 7) * 8, 8)
    off = beg & 127
    back = (LANES - off) & 127
    lane = lax.broadcasted_iota(jnp.int32, (8, LANES), 1)
    win = jnp.where(lane < LANES - off, pltpu.roll(slot_ref[pl.ds(row, 8), :], back, 1),
                    pltpu.roll(slot_ref[pl.ds(row + 8, 8), :], back, 1))
    code = win[0:1].astype(jnp.int32)
    x_c = (code >> X_SHIFT) & 255
    vals = [win[n:n + 1] for n in range(1, 5)]
    return row, off, size, lane, y_pl, x_beg, x_c - x_beg, code & 127, vals


def spread_rows(row):
    return jnp.broadcast_to(row, (16, LANES)).astype(BF16)


def deposit_kernel(n_xt, grid_size, table_ref, num_ref, slot_ref, rho_ref):
    n_planes = rho_ref.shape[0]

    def clear(y, c):
        rho_ref[y] = jnp.zeros(rho_ref.shape[1:], F32)
        return c
    lax.fori_loop(0, n_planes, clear, 0)
    row_x = lax.broadcasted_iota(jnp.int32, (X_ROWS, LANES), 0)
    row_z = lax.broadcasted_iota(jnp.int32, (LANES, LANES), 0)

    def one(t):
        row, off, size, lane, y_pl, x_beg, x_l, z_c, (q, wx, wy, wz) = read_window(t, table_ref, slot_ref, n_xt)
        q = jnp.where(lane[0:1] < size, q, 0.0)
        pick_x = jnp.concatenate([(row_x == x_l).astype(F32), (row_x == x_l + 1).astype(F32)], axis=1).astype(BF16)
        pick_z = [(row_z == z_c + c).astype(F32).astype(BF16).reshape(8, 16, LANES) for c in range(2)]
        cols = [[], [], []]
        for w_y in (1.0 - wy, wy):
            pieces = [[], [], []]
            for w_x in (1.0 - wx, wx):
                base = q * w_x * w_y
                lower, upper = split3(base * (1.0 - wz)), split3(base * wz)
                for m in range(3):
                    low = spread_rows(lower[m].astype(F32))[None]
                    high = spread_rows(upper[m].astype(F32))[None]
                    pieces[m].append((pick_z[0] * low + pick_z[1] * high).reshape(LANES, LANES))
            for m in range(3):
                cols[m].append(jnp.concatenate(pieces[m], axis=1))
        res = None
        for m in (2, 1, 0):
            part = jnp.concatenate(cols[m], axis=0)
            term = lax.dot_general(pick_x, part, (((1,), (1,)), ((), ())), preferred_element_type=F32)
            res = term if res is None else res + term
        for b in range(2):
            rho_ref[y_pl + b, pl.ds(x_beg, X_ROWS), :] += res[:, b * LANES:(b + 1) * LANES]

    def body(t, c):
        one(2 * t)
        one(2 * t + 1)
        return c
    lax.fori_loop(0, (num_ref[0] + 1) // 2, body, 0)

    def wrap(y, c):
        rho_ref[y, 0:8, :] += rho_ref[y, grid_size:grid_size + 8, :]
        return c
    lax.fori_loop(0, n_planes, wrap, 0)


def interp_kernel(n_xt, table_ref, num_ref, slot_ref, fhm_ref, flo_ref, out_ref):
    row_x = lax.broadcasted_iota(jnp.int32, (X_ROWS, LANES), 0)
    row_z = lax.broadcasted_iota(jnp.int32, (LANES, LANES), 0)
    out_ref[...] = jnp.zeros(out_ref.shape, F32)

    def one(t):
        row, off, size, lane, y_pl, x_beg, x_l, z_c, (q, wx, wy, wz) = read_window(t, table_ref, slot_ref, n_xt)
        pick_z = jnp.concatenate([(row_z == z_c).astype(F32), (row_z == z_c + 1).astype(F32)], axis=1).astype(BF16)
        pick_2 = jnp.concatenate([pick_z, pick_z], axis=0)
        on_x = jnp.where(row_x == x_l, 1.0 - wx, jnp.where(row_x == x_l + 1, wx, 0.0))
        rows = pl.ds(x_beg, X_ROWS)
        wt = [on_x * (1.0 - wy), on_x * wy]
        grads = []
        for comp in range(3):
            top = jnp.concatenate([fhm_ref[y_pl + b, comp, rows, :] for b in range(2)], axis=0)
            low = jnp.concatenate([flo_ref[y_pl + b, comp, rows, :] for b in range(2)], axis=0)
            got = jnp.dot(low, pick_z, preferred_element_type=F32) + jnp.dot(top, pick_2, preferred_element_type=F32)
            got = got[:, :LANES] * (1.0 - wz) + got[:, LANES:] * wz
            acc = got[:X_ROWS] * wt[0] + got[X_ROWS:] * wt[1]
            grads.append(-q * jnp.sum(acc, axis=0, keepdims=True))
        full = pltpu.roll(jnp.concatenate(grads + [jnp.zeros((5, LANES), F32)], axis=0), off, 1)
        here, after = pl.ds(row, 8), pl.ds(row + 8, 8)
        out_ref[here, :] = jnp.where((lane >= off) & (lane - off < size), full, out_ref[here, :])
        out_ref[after, :] = jnp.where((lane < off) & (lane + LANES - off < size), full, out_ref[after, :])

    def body(t, c):
        one(2 * t)
        one(2 * t + 1)
        return c
    lax.fori_loop(0, (num_ref[0] + 1) // 2, body, 0)


SMEM_SPEC = pl.BlockSpec(memory_space=pltpu.SMEM)
VMEM_SPEC = pl.BlockSpec(memory_space=pltpu.VMEM)


def sort_call(raw):
    return pl.pallas_call(
        sort_kernel, out_shape=jax.ShapeDtypeStruct((SLOT_ROWS, LANES), F32), in_specs=[VMEM_SPEC], out_specs=VMEM_SPEC,
        scratch_shapes=[pltpu.VMEM((CHUNKS, LANES), F32)] * 6, name="slot_sort",
    )(raw)


def unsort_call(slots, forces):
    return pl.pallas_call(
        unsort_kernel, out_shape=jax.ShapeDtypeStruct((3, CHUNKS, LANES), F32),
        in_specs=[VMEM_SPEC, VMEM_SPEC], out_specs=VMEM_SPEC,
        scratch_shapes=[pltpu.VMEM((CHUNKS, LANES), F32)] * 4, name="slot_unsort",
    )(slots, forces)


def deposit_call(table, num, slots, y_ext, grid_size, n_xt):
    return pl.pallas_call(
        functools.partial(deposit_kernel, n_xt, grid_size),
        out_shape=jax.ShapeDtypeStruct((y_ext, grid_size + 16, LANES), F32),
        in_specs=[SMEM_SPEC, SMEM_SPEC, VMEM_SPEC], out_specs=VMEM_SPEC,
        compiler_params=pltpu.CompilerParams(vmem_limit_bytes=VMEM_BIG), name="deposit",
    )(table, num, slots)


def slot_arrays(part_mass, cell_idx, cic_wts, live_mask, y_blk):
    charge = part_mass * live_mask.astype(F32)
    code = (cell_idx[:, 1] << Y_SHIFT) | (cell_idx[:, 0] << X_SHIFT) | cell_idx[:, 2]
    code = jnp.where(live_mask > 0, code, y_blk << Y_SHIFT).astype(F32)
    upper = cic_wts[:, :, 1]
    return jnp.stack([code, charge, upper[:, 0], upper[:, 1], upper[:, 2]]).reshape(5, CHUNKS, LANES)


def mul6(a, b):
    res = None
    for m, n in ((2, 0), (0, 2), (1, 1), (1, 0), (0, 1), (0, 0)):
        term = jnp.dot(a[m], b[n], preferred_element_type=F32)
        res = term if res is None else res + term
    return res


def table3(mat):
    mat = mat.astype(np.float32)
    hi = mat.astype(BF16)
    mid = (mat - hi.astype(np.float32)).astype(BF16)
    lo = (mat - hi.astype(np.float32) - mid.astype(np.float32)).astype(BF16)
    return np.stack([hi, mid, lo])


GROUP_SLOTS = (5, 4, 4)


class Plan:
    def __init__(self, n, n_chip, y_blk, z_blk):
        self.n, self.n_chip, self.y_blk, self.z_blk = n, n_chip, y_blk, z_blk
        self.y_ext = y_blk + 1
        self.z_ext = z_blk + 1
        self.y_pad = -(-self.y_ext // 8) * 8
        self.half_k = n // 2 + 1
        self.slots = -(-self.half_k // (2 * n_chip))
        self.per_core = self.slots * n_chip
        left, self.groups = self.slots, []
        for size in GROUP_SLOTS:
            self.groups.append(size)
            left -= size
        assert left == 0
        self.k_rows = [-(-size * n_chip // 8) * 8 for size in self.groups]
        self.k_beg = [sum(self.k_rows[:g]) for g in range(len(self.groups))]
        self.s_beg = [sum(self.groups[:g]) for g in range(len(self.groups))]
        self.k_pad = sum(self.k_rows)
        self.rows = [-(-(size * self.y_ext + 1) // 8) * 8 for size in self.groups]
        self.y_even = self.y_ext + self.y_ext % 2
        self.x_pad = n + 16

    def row_slots(self):
        ids = -np.ones(self.k_pad, np.int64)
        for g, size in enumerate(self.groups):
            for t in range(self.n_chip):
                r0 = self.k_beg[g] + t * size
                ids[r0:r0 + size] = t * self.slots + self.s_beg[g] + np.arange(size)
        return ids

    def angle(self, k, r):
        return 2.0 * np.pi / self.n * ((k[:, None] * r[None, :]) % self.n)

    def lane_order(self):
        kz = np.concatenate([np.arange(128), np.arange(128), np.arange(128, self.n), np.arange(128, self.n)])
        im = np.concatenate([np.zeros(128), np.ones(128), np.zeros(self.n - 128), np.ones(self.n - 128)]) > 0
        return kz, im

    def deriv(self, k):
        sgn = np.where(k < self.n // 2, k, k - self.n)
        return np.where(k == self.n // 2, 0, sgn) * (2.0 * np.pi / self.n)

    def tables(self):
        n = self.n
        out = {}
        mx = np.zeros((2, 2, self.k_pad, n))
        mi = np.zeros((2, 2, self.x_pad, 2, self.k_pad))
        ids = self.row_slots()
        for h in range(2):
            kx = np.where(ids >= 0, h * self.per_core + ids, n)
            ok = (kx < self.half_k)[:, None]
            th = self.angle(kx, np.arange(n))
            mx[h, 0] = np.where(ok, np.cos(th), 0.0)
            mx[h, 1] = np.where(ok, -np.sin(th), 0.0)
            th = self.angle(kx, np.arange(self.x_pad))
            wt = np.where(kx < self.half_k, np.where((kx == 0) | (kx == n // 2), 1.0, 2.0), 0.0) / float(n) ** 3
            kd = np.where(kx < n // 2, kx, 0) * (2.0 * np.pi / n) * wt
            mi[h, 0, :, 0] = (-kd[:, None] * np.sin(th)).T
            mi[h, 0, :, 1] = (-kd[:, None] * np.cos(th)).T
            mi[h, 1, :, 0] = (wt[:, None] * np.cos(th)).T
            mi[h, 1, :, 1] = (-wt[:, None] * np.sin(th)).T
        out["mx"] = table3(mx.reshape(2, 2 * self.k_pad, n))
        out["mi"] = table3(mi.reshape(2, 2, self.x_pad, 2 * self.k_pad))
        kz, im = self.lane_order()
        wz = np.zeros((2, 2, LANES, 2 * n))
        wi = np.zeros((2, 2 * n, 4, LANES))
        kd = self.deriv(kz)[:, None]
        for h in range(2):
            z = (h * self.z_blk + np.arange(self.z_ext)) % n
            c, s = np.cos(self.angle(kz, z)), np.sin(self.angle(kz, z))
            wz[h, 0, :self.z_ext] = np.where(im[:, None], -s, c).T
            wz[h, 1, :self.z_ext] = np.where(im[:, None], c, s).T
            re_w, im_w = np.where(im[:, None], -s, c), np.where(im[:, None], c, s)
            wi[h, :, 0, :self.z_ext] = re_w
            wi[h, :, 1, :self.z_ext] = im_w
            wi[h, :, 2, :self.z_ext] = -kd * im_w
            wi[h, :, 3, :self.z_ext] = kd * re_w
        out["wz"] = table3(wz)
        out["wi"] = table3(wi.reshape(2, 2 * n, 4 * LANES))
        ky = np.arange(n)
        my = np.zeros((2, n, self.n_chip, self.y_pad))
        ei = np.zeros((self.n_chip, 4, self.y_pad, n))
        for i in range(self.n_chip):
            y = (i * self.y_blk + np.arange(self.y_ext)) % n
            th = self.angle(ky, y)
            my[0, :, i, :self.y_ext] = np.cos(th)
            my[1, :, i, :self.y_ext] = np.sin(th)
            ei[i, 0, :self.y_ext] = np.cos(th).T
            ei[i, 1, :self.y_ext] = np.sin(th).T
            ei[i, 2, :self.y_ext] = (self.deriv(ky)[:, None] * np.cos(th)).T
            ei[i, 3, :self.y_ext] = (self.deriv(ky)[:, None] * np.sin(th)).T
        out["my"] = table3(my.reshape(2 * n, self.n_chip * self.y_pad))
        out["ei"] = table3(ei.reshape(self.n_chip, 4 * self.y_pad, n))
        return out


def cost(flops):
    return pl.CostEstimate(flops=int(flops), bytes_accessed=1 << 20, transcendentals=0)


def x_kernel(plan, core_ref, rho_ref, gas_ref, far_ref, mx_ref, *rest):
    tmp_ref = rest[-1]
    step = pl.program_id(0)
    core = core_ref[0]
    n, kp = plan.n, plan.k_pad

    @pl.when(step == 0)
    def _():
        tmp_ref[...] = jnp.zeros(tmp_ref.shape, F32)

    live = (2 * step < plan.y_blk).astype(F32)
    keep = live * core_ref[2].astype(F32)
    tmp_ref[:, :, :plan.z_blk] = gas_ref[...] * keep + far_ref[...] * live
    data = jnp.concatenate([rho_ref[y, :n, :] + tmp_ref[y] for y in range(2)], axis=1)
    lhs = [jnp.concatenate([mx_ref[m, core], mx_ref[m, 1 - core]], axis=0) for m in range(3)]
    res = mul6(lhs, split3(data))
    n_grp = len(plan.groups)
    for h in range(2):
        for g in range(n_grp):
            out = rest[h * n_grp + g]
            for y in range(2):
                for ri in range(2):
                    r0 = (2 * h + ri) * kp + plan.k_beg[g]
                    out[ri, y] = res[r0:r0 + plan.k_rows[g], y * LANES:(y + 1) * LANES]


def x_call(plan, ids, rho, gas, far, mx):
    steps = plan.y_even // 2
    last = plan.y_blk // 2 - 1
    shapes = tuple(jax.ShapeDtypeStruct((2, plan.y_even, k, LANES), F32) for k in plan.k_rows)
    out_specs = tuple(pl.BlockSpec((2, 2, k, LANES), lambda i: (0, i, 0, 0)) for k in plan.k_rows)
    gas_spec = pl.BlockSpec((2, plan.n, plan.z_blk), lambda i: (jnp.minimum(i, last), 0, 0))
    outs = pl.pallas_call(
        functools.partial(x_kernel, plan), grid=(steps,), out_shape=shapes + shapes,
        in_specs=[SMEM_SPEC, pl.BlockSpec((2, plan.x_pad, LANES), lambda i: (i, 0, 0)),
                  gas_spec, gas_spec,
                  pl.BlockSpec(mx.shape, lambda i: (0, 0, 0, 0))],
        out_specs=out_specs + out_specs,
        scratch_shapes=[pltpu.VMEM((2, plan.n, LANES), F32)], name="dft_x",
    )(ids, rho, gas, far, mx)
    return outs[:len(shapes)], outs[len(shapes):]


Z_BATCH = 10


def z_kernel(plan, grp, ids_ref, own_ref, rec_ref, wz_ref, *rest):
    outs, tmp_ref = rest[:-1], rest[-1]
    step = pl.program_id(0)
    core, chip = ids_ref[0], ids_ref[1]
    kp, sl, ye, rows = plan.k_rows[grp], plan.groups[grp], plan.y_ext, plan.rows[grp]

    @pl.when(step == 0)
    def _():
        for out in outs:
            for g in range(3):
                out[g, rows - 8:rows, :] = jnp.zeros((8, LANES), F32)

    flat = (Z_BATCH * kp, LANES)
    data = jnp.concatenate([own_ref[0].reshape(flat), rec_ref[0].reshape(flat),
                            own_ref[1].reshape(flat), rec_ref[1].reshape(flat)], axis=1)
    wts = [jnp.concatenate([wz_ref[m, core, 0], wz_ref[m, 1 - core, 0], wz_ref[m, core, 1], wz_ref[m, 1 - core, 1]], axis=0)
           for m in range(3)]
    res = mul6(split3(data), wts)
    for g in range(3):
        tmp_ref[g] = res[:, g * LANES:(g + 1) * LANES]
    for b in range(Z_BATCH):
        y = step * Z_BATCH + b

        @pl.when(y < ye)
        def _():
            for r, out in enumerate(outs):
                for g in range(3):
                    out[g, pl.ds(y, sl, stride=ye), :] = tmp_ref[g, pl.ds(b * kp + (chip ^ r) * sl, sl), :]


def z_call(plan, grp, ids, own, rec, wz):
    kp = plan.k_rows[grp]
    blk = pl.BlockSpec((2, Z_BATCH, kp, LANES), lambda i: (0, i, 0, 0))
    shape = (3, plan.rows[grp], LANES)
    return pl.pallas_call(
        functools.partial(z_kernel, plan, grp), grid=(plan.y_even // Z_BATCH,),
        out_shape=(jax.ShapeDtypeStruct(shape, F32),) * plan.n_chip,
        in_specs=[SMEM_SPEC, blk, blk, pl.BlockSpec(wz.shape, lambda i: (0,) * 5)],
        out_specs=(pl.BlockSpec(shape, lambda i: (0, 0, 0)),) * plan.n_chip,
        scratch_shapes=[pltpu.VMEM((3, Z_BATCH * kp, LANES), F32)],
        cost_estimate=cost(12 * 50 * kp * 512 * 384),
        compiler_params=pltpu.CompilerParams(vmem_limit_bytes=24 << 20), name="dft_z",
    )(ids, own, rec, wz)


def signed(ids, n):
    return jnp.where(ids < n // 2, ids, ids - n).astype(F32)


def y_kernel(plan, grp, ids_ref, *refs):
    nc = plan.n_chip
    recs, (my_ref, ei_ref), outs, buf_ref = refs[:nc], refs[nc:nc + 2], refs[nc + 2:2 * nc + 2], refs[-1]
    n, ye, yp, n_rows = plan.n, plan.y_ext, plan.y_pad, plan.rows[grp]
    core, chip = ids_ref[0], ids_ref[1]
    kx_beg = core * plan.per_core + chip * plan.slots + plan.s_beg[grp]
    k_unit = 2.0 * math.pi / n
    buf_ref[...] = jnp.zeros(buf_ref.shape, F32)
    for out in outs:
        for c in range(2):
            for g in range(3):
                out[c, g, n_rows - 8:n_rows, :] = jnp.zeros((8, LANES), F32)
    lane = lax.broadcasted_iota(jnp.int32, (n, LANES), 1)
    ky = signed(lax.broadcasted_iota(jnp.int32, (n, LANES), 0), n)
    kz_a = signed(lane, n)
    kz_b = signed(128 + (lane & 63), n)
    yz_a, yz_b = ky * ky + kz_a * kz_a, ky * ky + kz_b * kz_b
    flip = jnp.where(lax.broadcasted_iota(jnp.int32, (1, LANES), 1) < 64, 1.0, -1.0)

    def slot(s, energy):
        rows = pl.ds(s * ye, ye)
        for r, rec in enumerate(recs):
            for g in range(3):
                buf_ref[g, pl.ds(pl.multiple_of((chip ^ r) * yp, 8), ye), :] = rec[g, rows, :]
        data = jnp.concatenate([buf_ref[g] for g in range(3)], axis=1)
        q = mul6([my_ref[m] for m in range(3)], split3(data))
        c = [q[:n, g * LANES:(g + 1) * LANES] for g in range(3)]
        d = [q[n:, g * LANES:(g + 1) * LANES] for g in range(3)]
        r0 = c[0] + d[1]
        r1 = c[1] - d[0]
        r2 = c[2] + flip * pltpu.roll(d[2], 64, 1)
        kx_i = kx_beg + s
        kx = kx_i.astype(F32)
        weight = jnp.where(kx_i < n // 2, jnp.where(kx_i == 0, 1.0, 2.0), jnp.where(kx_i == n // 2, 1.0, 0.0))
        scale = -4.0 * math.pi * GRAV_CONST / (k_unit * k_unit)

        def influence(yz):
            sq = yz + kx * kx
            return jnp.where(sq > 0, scale / jnp.maximum(sq, 1.0), 0.0)
        g_a, g_b = influence(yz_a), influence(yz_b)
        power = g_a * (r0 * r0 + r1 * r1) + g_b * (r2 * r2)
        energy = energy + weight * jnp.sum(power, axis=0, keepdims=True)
        parts = split3(jnp.concatenate([g_a * r0, g_a * r1, g_b * r2], axis=1))
        for r, out in enumerate(outs):
            if r % 2 == 0:
                lhs = [jnp.concatenate([ei_ref[m, chip ^ r], ei_ref[m, chip ^ (r + 1)]], axis=0) for m in range(3)]
                two = mul6(lhs, parts)
            p = two[(r % 2) * 4 * yp:(r % 2 + 1) * 4 * yp]
            co, si, ck, sk = [[p[u * yp:(u + 1) * yp, g * LANES:(g + 1) * LANES] for g in range(3)] for u in range(4)]
            pot = (co[0] - si[1], co[1] + si[0], co[2] - flip * pltpu.roll(si[2], 64, 1))
            dy = (-(ck[1] + sk[0]), ck[0] - sk[1], -flip * pltpu.roll(ck[2], 64, 1) - sk[2])
            for comp, val in ((0, pot), (1, dy)):
                for g in range(3):
                    out[comp, g, rows, :] = val[g][:ye]
        return energy

    energy = lax.fori_loop(0, plan.groups[grp], slot, jnp.zeros((1, LANES), F32))
    e_row = plan.groups[grp] * ye
    for out in outs:
        out[0, 0, e_row:e_row + 1, :] = energy


def y_call(plan, grp, ids, recs, my, ei):
    shape = jax.ShapeDtypeStruct((2, 3, plan.rows[grp], LANES), F32)
    return pl.pallas_call(
        functools.partial(y_kernel, plan, grp),
        out_shape=(shape,) * plan.n_chip,
        in_specs=[SMEM_SPEC] + [VMEM_SPEC] * (plan.n_chip + 2), out_specs=(VMEM_SPEC,) * plan.n_chip,
        scratch_shapes=[pltpu.VMEM((3, plan.n_chip * plan.y_pad, LANES), F32)],
        cost_estimate=cost(12 * plan.groups[grp] * 384 * (384 * 224 + 896 * 192)),
        compiler_params=pltpu.CompilerParams(vmem_limit_bytes=24 << 20), name="dft_y",
    )(ids, *recs, my, ei)


def zi_kernel(plan, grp, ids_ref, *refs):
    nc = plan.n_chip
    recs, wi_ref, own_ref, send_ref, buf_ref, e_ref = refs[:nc], *refs[nc:]
    step = pl.program_id(0)
    core, chip = ids_ref[0], ids_ref[1]
    kp, sl, ye = plan.k_rows[grp], plan.groups[grp], plan.y_ext

    @pl.when(step == 0)
    def _():
        buf_ref[...] = jnp.zeros(buf_ref.shape, F32)

    for comp in range(2):
        for b in range(Z_BATCH):
            for r, rec in enumerate(recs):
                for g in range(3):
                    buf_ref[g, pl.ds((comp * Z_BATCH + b) * kp + (chip ^ r) * sl, sl), :] = (
                        rec[comp, g, pl.ds(step * Z_BATCH + b, sl, stride=ye), :])
    half_rows = Z_BATCH * kp
    parts = split3(jnp.concatenate([buf_ref[g] for g in range(3)], axis=1))
    pot = [p[:half_rows] for p in parts]
    for half, out in ((core, own_ref), (1 - core, send_ref)):
        plain = mul6(parts, [wi_ref[m, half, :, :2 * LANES] for m in range(3)])
        along = mul6(pot, [wi_ref[m, half, :, 2 * LANES:] for m in range(3)])
        for b in range(Z_BATCH):
            for ri in range(2):
                ln = slice(ri * LANES, (ri + 1) * LANES)
                out[0, ri, b] = plain[b * kp:(b + 1) * kp, ln]
                out[1, ri, b] = plain[half_rows + b * kp:half_rows + (b + 1) * kp, ln]
                out[2, ri, b] = along[b * kp:(b + 1) * kp, ln]

    @pl.when(step == pl.num_programs(0) - 1)
    def _():
        e_row = sl * ye
        for r, rec in enumerate(recs):
            e_ref[pl.ds(chip ^ r, 1), :] = rec[0, 0, e_row:e_row + 1, :]
        total = e_ref[0:1, :]
        for t in range(1, nc):
            total = total + e_ref[t:t + 1, :]
        own_ref[0, 0, Z_BATCH - 1, 0:1, :] = total
        send_ref[0, 0, Z_BATCH - 1, 0:1, :] = total


def zi_call(plan, grp, ids, recs, wi):
    kp = plan.k_rows[grp]
    shape = jax.ShapeDtypeStruct((3, 2, plan.y_even, kp, LANES), F32)
    spec = pl.BlockSpec((3, 2, Z_BATCH, kp, LANES), lambda i: (0, 0, i, 0, 0))
    return pl.pallas_call(
        functools.partial(zi_kernel, plan, grp), grid=(plan.y_even // Z_BATCH,), out_shape=(shape, shape),
        in_specs=[SMEM_SPEC] + [pl.BlockSpec(r.shape, lambda i: (0,) * 4) for r in recs]
        + [pl.BlockSpec(wi.shape, lambda i: (0,) * 4)],
        out_specs=(spec, spec),
        scratch_shapes=[pltpu.VMEM((3, 2 * Z_BATCH * kp, LANES), F32), pltpu.VMEM((8, LANES), F32)],
        cost_estimate=cost(12 * 50 * kp * 384 * 512 * 3),
        compiler_params=pltpu.CompilerParams(vmem_limit_bytes=32 << 20), name="idft_z",
    )(ids, *recs, wi)


def field_kernel(plan, n_xt, e_norm, ids_ref, table_ref, num_ref, slot_ref, mi_ref, *refs):
    n_grp = len(plan.groups)
    sides = (refs[:n_grp], refs[n_grp:2 * n_grp])
    out_ref, energy_ref, fhm_ref, flo_ref, lhs_ref = refs[2 * n_grp:]
    core = ids_ref[0]
    for m in range(3):
        for kind in range(2):
            lhs_ref[m, kind] = jnp.concatenate([mi_ref[m, core, kind], mi_ref[m, 1 - core, kind]], axis=1)

    def column(c, y):
        return jnp.concatenate([ref[c, ri, y] for side in sides for ri in range(2) for ref in side], axis=0)

    def put(res, spots):
        hi, mid, lo = split3(res)
        for pos, (y, c) in enumerate(spots):
            ln = slice(pos * LANES, (pos + 1) * LANES)
            fhm_ref[y, c, :, :LANES] = hi[:, ln]
            fhm_ref[y, c, :, LANES:] = mid[:, ln]
            flo_ref[y, c] = lo[:, ln]

    def planes(step, carry):
        y0 = 2 * step
        data = jnp.concatenate([column(0, y0), column(0, y0 + 1)], axis=1)
        put(mul6([lhs_ref[m, 0] for m in range(3)], split3(data)), ((y0, 0), (y0 + 1, 0)))
        for y in (y0, y0 + 1):
            data = jnp.concatenate([column(1, y), column(2, y)], axis=1)
            put(mul6([lhs_ref[m, 1] for m in range(3)], split3(data)), ((y, 1), (y, 2)))
        return carry
    lax.fori_loop(0, plan.y_even // 2, planes, 0)
    lanes = None
    for own, rec in zip(*sides):
        pair = own[0, 0, plan.y_even - 1, 0:1, :] + rec[0, 0, plan.y_even - 1, 0:1, :]
        lanes = pair if lanes is None else lanes + pair
    energy_ref[...] = jnp.broadcast_to(jnp.sum(lanes, axis=1, keepdims=True) * e_norm, energy_ref.shape)
    interp_kernel(n_xt, table_ref, num_ref, slot_ref, fhm_ref, flo_ref, out_ref)


def field_call(plan, ids, table, num, slots, own, rec, mi, n_xt, e_norm):
    return pl.pallas_call(
        functools.partial(field_kernel, plan, n_xt, e_norm),
        out_shape=(jax.ShapeDtypeStruct((SLOT_ROWS, LANES), F32), jax.ShapeDtypeStruct((8, LANES), F32)),
        in_specs=[SMEM_SPEC, SMEM_SPEC, SMEM_SPEC] + [VMEM_SPEC] * (2 + 2 * len(own)), out_specs=(VMEM_SPEC, VMEM_SPEC),
        scratch_shapes=[pltpu.VMEM((plan.y_even, 3, plan.x_pad, 2 * LANES), BF16),
                        pltpu.VMEM((plan.y_even, 3, plan.x_pad, LANES), BF16),
                        pltpu.VMEM((3, 2, plan.x_pad, 4 * plan.k_pad), BF16)],
        compiler_params=pltpu.CompilerParams(vmem_limit_bytes=VMEM_BIG), name="idft_x_interp",
    )(ids, table, num, slots, mi, *own, *rec)


def solution(mesh):
    n_cols = mesh.shape["col"]
    n_cx = mesh.shape["row"] // 2
    fine = jax.sharding.Mesh(mesh.devices.reshape(mesh.shape["rep"], n_cols, n_cx, 2), ("rep", "col", "cx", "core"))
    slot_axes = ("rep", "col", "cx", "core")
    chip_axes = ("col", "cx")
    turn = [(a * 2 + b, b * 2 + a) for a in range(n_cols) for b in range(2) if a != b]
    other_core = [(0, 1), (1, 0)]

    def device_body(part_mass, cell_idx, cic_wts, live_mask, gas_block):
        grid_size, y_blk, z_blk = gas_block.shape
        per_dev = part_mass.shape[0]
        n_chip = n_cx * n_cols
        n_slots = per_dev * n_chip * 2
        plan = Plan(grid_size, n_chip, y_blk, z_blk)
        tab = plan.tables()
        core = lax.axis_index("core").astype(jnp.int32)
        chip = (lax.axis_index("cx") * n_cols + lax.axis_index("col")).astype(jnp.int32)
        n_xt = grid_size // X_TILE
        n_blk = y_blk * n_xt

        keep = (core == lax.axis_index("col")).astype(jnp.int32)

        def swap(arr):
            return lax.ppermute(arr, ("col", "core"), turn)

        raw = slot_arrays(part_mass, cell_idx, cic_wts, live_mask, y_blk)
        raw = swap(raw) + raw * keep.astype(F32)
        raw, gas = lax.optimization_barrier((raw, jnp.transpose(gas_block, (1, 0, 2))))
        gas_far = swap(gas)
        table, num = pair_table(raw[0].reshape(-1), n_blk, n_xt)
        slots = sort_call(raw)
        rho = deposit_call(table, num, slots, plan.y_even, grid_size, n_xt)
        ids = jnp.stack([core, chip, keep])
        own, send = x_call(plan, ids, rho, gas, gas_far, tab["mx"])

        def exchange(parts):
            out = [parts[0]]
            for r in range(1, n_chip):
                flip = (r >> 1) | ((r & 1) << 1)
                out.append(lax.ppermute(parts[r], chip_axes, [(t, t ^ flip) for t in range(n_chip)]))
            return out

        grps = range(len(plan.groups))

        def chain(token, outs):
            return lax.optimization_barrier((token, tuple(outs)))

        rec = [lax.ppermute(s, "core", other_core) for s in send]
        at_y, at_z, halves = [], [], []
        for g in grps:
            ids, out = chain(ids, z_call(plan, g, ids, own[g], rec[g], tab["wz"]))
            at_y.append(exchange(out))
        for g in grps:
            ids, out = chain(ids, y_call(plan, g, ids, at_y[g], tab["my"], tab["ei"]))
            at_z.append(exchange(out))
        for g in grps:
            ids, out = chain(ids, zi_call(plan, g, ids, at_z[g], tab["wi"]))
            halves.append(out)
        rec = [lax.ppermute(h[1], "core", other_core) for h in halves]
        e_norm = 0.5 / (grid_size ** 3 * n_slots)
        forces, energy = field_call(plan, ids, table, num, slots, [h[0] for h in halves], rec, tab["mi"], n_xt, e_norm)
        back = unsort_call(slots, forces)
        home = swap(back) + back * keep.astype(F32)
        return home.reshape(3, per_dev).T, energy[0, 0:1]

    return jax.shard_map(
        device_body, mesh=fine,
        in_specs=(P(slot_axes), P(slot_axes, None), P(slot_axes, None, None), P(slot_axes), P("rep", ("cx", "core"), "col")),
        out_specs=(P(slot_axes, None), P("rep")), check_vma=False)
```

```python
import functools
import math
import numpy as np
import jax
import jax.numpy as jnp
from jax import lax
from jax.sharding import PartitionSpec as P
from jax.experimental import pallas as pl
from jax.experimental.pallas import tpu as pltpu

MATMUL_PREC = lax.Precision.HIGHEST
GRAV_CONST = 1.0
F32 = jnp.float32
BF16 = jnp.bfloat16
LANES = 128
X_TILE = 96
X_ROWS = 112
Y_SHIFT = 15
X_SHIFT = 7
VMEM_BIG = 60 * 1024 * 1024


def split3(val):
    hi = val.astype(BF16)
    rest = val - hi.astype(F32)
    mid = rest.astype(BF16)
    lo = (rest - mid.astype(F32)).astype(BF16)
    return hi, mid, lo


def bitonic(bufs):
    sub = lax.broadcasted_iota(jnp.int32, (8, LANES), 0)
    lane = lax.broadcasted_iota(jnp.int32, (8, LANES), 1)
    base = lane * 128 + sub

    def bit(rank, pos):
        return lax.shift_right_logical(rank, jnp.full_like(rank, pos)) & 1

    def vreg_stage(k, j):
        step = 1 << (j - 3)
        for v in range(16):
            if v & step:
                continue
            low, high = pl.ds(8 * v, 8), pl.ds(8 * (v + step), 8)
            sgn = 1.0 - 2.0 * bit(base + 8 * v, k).astype(F32)
            a = [b[low, :] for b in bufs]
            c = [b[high, :] for b in bufs]
            swap = a[0] * sgn > c[0] * sgn
            for b, p, q in zip(bufs, a, c):
                b[low, :] = jnp.where(swap, q, p)
                b[high, :] = jnp.where(swap, p, q)

    def roll_stage(k, j, dist, axis):
        size = (8, LANES)[axis]
        upper = bit(base, j)
        keep_low = upper == 0
        for v in range(16):
            rows = pl.ds(8 * v, 8)
            sgn = 1.0 - 2.0 * (bit(base + 8 * v, k) ^ upper).astype(F32)
            own = [b[rows, :] for b in bufs]
            other = [jnp.where(keep_low, pltpu.roll(o, size - dist, axis), pltpu.roll(o, dist, axis)) for o in own]
            take = other[0] * sgn < own[0] * sgn
            for b, o, p in zip(bufs, own, other):
                b[rows, :] = jnp.where(take, p, o)

    def stage(k, j):
        if j >= 3:
            vreg_stage(k, j)
        else:
            roll_stage(k, j, 1 << j, 0)

    for k in range(1, 8):
        for j in range(k - 1, -1, -1):
            stage(k, j)

    def phase(k, carry):
        def lane_stage(step, c):
            j = k - 1 - step
            roll_stage(k, j, jnp.left_shift(1, j - 7), 1)
            return c
        lax.fori_loop(0, k - 7, lane_stage, 0)
        for j in range(6, -1, -1):
            stage(k, j)
        return carry
    lax.fori_loop(8, 15, phase, 0)


CHUNKS = 128
UNROLL = 4
SLOT_ROWS = 8 * (CHUNKS + 1)


def sort_kernel(in_ref, out_ref, *bufs):
    for n in range(5):
        bufs[n][...] = in_ref[n]
    row = lax.broadcasted_iota(jnp.int32, (CHUNKS, LANES), 0)
    col = lax.broadcasted_iota(jnp.int32, (CHUNKS, LANES), 1)
    bufs[5][...] = (row * LANES + col).astype(F32)
    bitonic(bufs)
    zero = jnp.zeros((CHUNKS, LANES), F32)
    for n in range(8):
        out_ref[pl.ds(n, CHUNKS, stride=8), :] = bufs[n][...].T if n < 6 else zero
    out_ref[8 * CHUNKS:, :] = jnp.zeros((8, LANES), F32)


def unsort_kernel(slot_ref, force_ref, out_ref, *bufs):
    bufs[0][...] = slot_ref[pl.ds(5, CHUNKS, stride=8), :]
    for n in range(3):
        bufs[n + 1][...] = force_ref[pl.ds(n, CHUNKS, stride=8), :]
    bitonic(bufs)
    for n in range(3):
        out_ref[n] = bufs[n + 1][...].T


def pair_table(key, n_blk, n_xt):
    b_ids = jnp.arange(n_blk + 1)
    bounds = ((b_ids // n_xt) << Y_SHIFT) | (((b_ids % n_xt) * X_TILE) << X_SHIFT)
    starts = jnp.sum((key[None, :] < bounds[:, None].astype(F32)).astype(jnp.int32), axis=1)
    first, last = starts[:-1], starts[1:]
    count = (last - first + LANES - 1) // LANES
    ids = jnp.arange(n_blk)
    ends = jnp.sum(jnp.where(ids[None, :] <= ids[:, None], count[None, :], 0), axis=1)
    t_ids = jnp.arange(n_blk + CHUNKS)
    blk = jnp.sum((ends[None, :] <= t_ids[:, None]).astype(jnp.int32), axis=1)
    hot = ids[None, :] == blk[:, None]
    beg = jnp.sum(jnp.where(hot, (first - LANES * (ends - count))[None, :], 0), axis=1) + LANES * t_ids
    size = jnp.minimum(jnp.sum(jnp.where(hot, last[None, :], 0), axis=1) - beg, LANES)
    live = t_ids < ends[-1]
    table = jnp.stack([jnp.where(live, blk, 0), jnp.where(live, beg, 0), jnp.where(live, size, 0)])
    return table.astype(jnp.int32), ends[-1:].astype(jnp.int32)


def read_window(t, table_ref, slot_ref, n_xt):
    blk = table_ref[0, t]
    beg = table_ref[1, t]
    size = table_ref[2, t]
    y_pl = blk // n_xt
    x_beg = pl.multiple_of((blk % n_xt) * X_TILE, 16)
    row = pl.multiple_of((beg >> 7) * 8, 8)
    off = beg & 127
    back = (LANES - off) & 127
    lane = lax.broadcasted_iota(jnp.int32, (8, LANES), 1)
    win = jnp.where(lane < LANES - off, pltpu.roll(slot_ref[pl.ds(row, 8), :], back, 1),
                    pltpu.roll(slot_ref[pl.ds(row + 8, 8), :], back, 1))
    code = win[0:1].astype(jnp.int32)
    x_c = (code >> X_SHIFT) & 255
    vals = [win[n:n + 1] for n in range(1, 5)]
    return row, off, size, lane, y_pl, x_beg, x_c - x_beg, code & 127, vals


def spread_rows(row):
    return jnp.broadcast_to(row, (16, LANES)).astype(BF16)


def deposit_kernel(n_xt, grid_size, table_ref, num_ref, slot_ref, rho_ref):
    n_planes = rho_ref.shape[0]

    def clear(y, c):
        rho_ref[y] = jnp.zeros(rho_ref.shape[1:], F32)
        return c
    lax.fori_loop(0, n_planes, clear, 0)
    row_x = lax.broadcasted_iota(jnp.int32, (X_ROWS, LANES), 0)
    row_z = lax.broadcasted_iota(jnp.int32, (LANES, LANES), 0)

    def one(t):
        row, off, size, lane, y_pl, x_beg, x_l, z_c, (q, wx, wy, wz) = read_window(t, table_ref, slot_ref, n_xt)
        q = jnp.where(lane[0:1] < size, q, 0.0)
        pick_x = jnp.concatenate([(row_x == x_l).astype(F32), (row_x == x_l + 1).astype(F32)], axis=1).astype(BF16)
        pick_z = [(row_z == z_c + c).astype(F32).astype(BF16).reshape(8, 16, LANES) for c in range(2)]
        cols = [[], [], []]
        for w_y in (1.0 - wy, wy):
            pieces = [[], [], []]
            for w_x in (1.0 - wx, wx):
                base = q * w_x * w_y
                lower, upper = split3(base * (1.0 - wz)), split3(base * wz)
                for m in range(3):
                    low = spread_rows(lower[m].astype(F32))[None]
                    high = spread_rows(upper[m].astype(F32))[None]
                    pieces[m].append((pick_z[0] * low + pick_z[1] * high).reshape(LANES, LANES))
            for m in range(3):
                cols[m].append(jnp.concatenate(pieces[m], axis=1))
        res = None
        for m in (2, 1, 0):
            part = jnp.concatenate(cols[m], axis=0)
            term = lax.dot_general(pick_x, part, (((1,), (1,)), ((), ())), preferred_element_type=F32)
            res = term if res is None else res + term
        for b in range(2):
            rho_ref[y_pl + b, pl.ds(x_beg, X_ROWS), :] += res[:, b * LANES:(b + 1) * LANES]

    def body(t, c):
        for u in range(UNROLL):
            one(UNROLL * t + u)
        return c
    lax.fori_loop(0, (num_ref[0] + UNROLL - 1) // UNROLL, body, 0)

    def wrap(y, c):
        rho_ref[y, 0:8, :] += rho_ref[y, grid_size:grid_size + 8, :]
        return c
    lax.fori_loop(0, n_planes, wrap, 0)


def interp_kernel(n_xt, table_ref, num_ref, slot_ref, fhm_ref, flo_ref, out_ref):
    row_x = lax.broadcasted_iota(jnp.int32, (X_ROWS, LANES), 0)
    row_z = lax.broadcasted_iota(jnp.int32, (LANES, LANES), 0)
    out_ref[...] = jnp.zeros(out_ref.shape, F32)

    def one(t):
        row, off, size, lane, y_pl, x_beg, x_l, z_c, (q, wx, wy, wz) = read_window(t, table_ref, slot_ref, n_xt)
        pick_z = jnp.concatenate([(row_z == z_c).astype(F32), (row_z == z_c + 1).astype(F32)], axis=1).astype(BF16)
        pick_2 = jnp.concatenate([pick_z, pick_z], axis=0)
        on_x = jnp.where(row_x == x_l, 1.0 - wx, jnp.where(row_x == x_l + 1, wx, 0.0))
        rows = pl.ds(x_beg, X_ROWS)
        wt = [on_x * (1.0 - wy), on_x * wy]
        grads = []
        for comp in range(3):
            top = jnp.concatenate([fhm_ref[y_pl + b, comp, rows, :] for b in range(2)], axis=0)
            low = jnp.concatenate([flo_ref[y_pl + b, comp, rows, :] for b in range(2)], axis=0)
            got = jnp.dot(low, pick_z, preferred_element_type=F32) + jnp.dot(top, pick_2, preferred_element_type=F32)
            got = got[:, :LANES] * (1.0 - wz) + got[:, LANES:] * wz
            acc = got[:X_ROWS] * wt[0] + got[X_ROWS:] * wt[1]
            grads.append(-q * jnp.sum(acc, axis=0, keepdims=True))
        full = pltpu.roll(jnp.concatenate(grads + [jnp.zeros((5, LANES), F32)], axis=0), off, 1)
        here, after = pl.ds(row, 8), pl.ds(row + 8, 8)
        out_ref[here, :] = jnp.where((lane >= off) & (lane - off < size), full, out_ref[here, :])
        out_ref[after, :] = jnp.where((lane < off) & (lane + LANES - off < size), full, out_ref[after, :])

    def body(t, c):
        for u in range(UNROLL):
            one(UNROLL * t + u)
        return c
    lax.fori_loop(0, (num_ref[0] + UNROLL - 1) // UNROLL, body, 0)


SMEM_SPEC = pl.BlockSpec(memory_space=pltpu.SMEM)
VMEM_SPEC = pl.BlockSpec(memory_space=pltpu.VMEM)


def sort_call(raw):
    return pl.pallas_call(
        sort_kernel, out_shape=jax.ShapeDtypeStruct((SLOT_ROWS, LANES), F32), in_specs=[VMEM_SPEC], out_specs=VMEM_SPEC,
        scratch_shapes=[pltpu.VMEM((CHUNKS, LANES), F32)] * 6, name="slot_sort",
    )(raw)


def unsort_call(slots, forces):
    return pl.pallas_call(
        unsort_kernel, out_shape=jax.ShapeDtypeStruct((3, CHUNKS, LANES), F32),
        in_specs=[VMEM_SPEC, VMEM_SPEC], out_specs=VMEM_SPEC,
        scratch_shapes=[pltpu.VMEM((CHUNKS, LANES), F32)] * 4, name="slot_unsort",
    )(slots, forces)


def deposit_call(table, num, slots, y_ext, grid_size, n_xt):
    return pl.pallas_call(
        functools.partial(deposit_kernel, n_xt, grid_size),
        out_shape=jax.ShapeDtypeStruct((y_ext, grid_size + 16, LANES), F32),
        in_specs=[SMEM_SPEC, SMEM_SPEC, VMEM_SPEC], out_specs=VMEM_SPEC,
        compiler_params=pltpu.CompilerParams(vmem_limit_bytes=VMEM_BIG), name="deposit",
    )(table, num, slots)


def slot_arrays(part_mass, cell_idx, cic_wts, live_mask, y_blk):
    charge = part_mass * live_mask.astype(F32)
    code = (cell_idx[:, 1] << Y_SHIFT) | (cell_idx[:, 0] << X_SHIFT) | cell_idx[:, 2]
    code = jnp.where(live_mask > 0, code, y_blk << Y_SHIFT).astype(F32)
    upper = cic_wts[:, :, 1]
    return jnp.stack([code, charge, upper[:, 0], upper[:, 1], upper[:, 2]]).reshape(5, CHUNKS, LANES)


def mul6(a, b):
    res = None
    for m, n in ((2, 0), (0, 2), (1, 1), (1, 0), (0, 1), (0, 0)):
        term = jnp.dot(a[m], b[n], preferred_element_type=F32)
        res = term if res is None else res + term
    return res


def table3(mat):
    mat = mat.astype(np.float32)
    hi = mat.astype(BF16)
    mid = (mat - hi.astype(np.float32)).astype(BF16)
    lo = (mat - hi.astype(np.float32) - mid.astype(np.float32)).astype(BF16)
    return np.stack([hi, mid, lo])


GROUP_SLOTS = (5, 4, 4)


class Plan:
    def __init__(self, n, n_chip, y_blk, z_blk):
        self.n, self.n_chip, self.y_blk, self.z_blk = n, n_chip, y_blk, z_blk
        self.y_ext = y_blk + 1
        self.z_ext = z_blk + 1
        self.y_pad = -(-self.y_ext // 8) * 8
        self.half_k = n // 2 + 1
        self.slots = -(-self.half_k // (2 * n_chip))
        self.per_core = self.slots * n_chip
        left, self.groups = self.slots, []
        for size in GROUP_SLOTS:
            self.groups.append(size)
            left -= size
        assert left == 0
        self.k_rows = [-(-size * n_chip // 8) * 8 for size in self.groups]
        self.k_beg = [sum(self.k_rows[:g]) for g in range(len(self.groups))]
        self.s_beg = [sum(self.groups[:g]) for g in range(len(self.groups))]
        self.k_pad = sum(self.k_rows)
        self.rows = [-(-(size * self.y_ext + 1) // 8) * 8 for size in self.groups]
        self.y_even = self.y_ext + self.y_ext % 2
        self.x_pad = n + 16

    def row_slots(self):
        ids = -np.ones(self.k_pad, np.int64)
        for g, size in enumerate(self.groups):
            for t in range(self.n_chip):
                r0 = self.k_beg[g] + t * size
                ids[r0:r0 + size] = t * self.slots + self.s_beg[g] + np.arange(size)
        return ids

    def angle(self, k, r):
        return 2.0 * np.pi / self.n * ((k[:, None] * r[None, :]) % self.n)

    def lane_order(self):
        kz = np.concatenate([np.arange(128), np.arange(128), np.arange(128, self.n), np.arange(128, self.n)])
        im = np.concatenate([np.zeros(128), np.ones(128), np.zeros(self.n - 128), np.ones(self.n - 128)]) > 0
        return kz, im

    def deriv(self, k):
        sgn = np.where(k < self.n // 2, k, k - self.n)
        return np.where(k == self.n // 2, 0, sgn) * (2.0 * np.pi / self.n)

    def tables(self):
        n = self.n
        out = {}
        mx = np.zeros((2, 2, self.k_pad, n))
        mi = np.zeros((2, 2, self.x_pad, 2, self.k_pad))
        ids = self.row_slots()
        for h in range(2):
            kx = np.where(ids >= 0, h * self.per_core + ids, n)
            ok = (kx < self.half_k)[:, None]
            th = self.angle(kx, np.arange(n))
            mx[h, 0] = np.where(ok, np.cos(th), 0.0)
            mx[h, 1] = np.where(ok, -np.sin(th), 0.0)
            th = self.angle(kx, np.arange(self.x_pad))
            wt = np.where(kx < self.half_k, np.where((kx == 0) | (kx == n // 2), 1.0, 2.0), 0.0) / float(n) ** 3
            kd = np.where(kx < n // 2, kx, 0) * (2.0 * np.pi / n) * wt
            mi[h, 0, :, 0] = (-kd[:, None] * np.sin(th)).T
            mi[h, 0, :, 1] = (-kd[:, None] * np.cos(th)).T
            mi[h, 1, :, 0] = (wt[:, None] * np.cos(th)).T
            mi[h, 1, :, 1] = (-wt[:, None] * np.sin(th)).T
        out["mx"] = table3(mx.reshape(2, 2 * self.k_pad, n))
        out["mi"] = table3(mi.reshape(2, 2, self.x_pad, 2 * self.k_pad))
        kz, im = self.lane_order()
        wz = np.zeros((2, 2, LANES, 2 * n))
        wi = np.zeros((2, 2 * n, 4, LANES))
        kd = self.deriv(kz)[:, None]
        for h in range(2):
            z = (h * self.z_blk + np.arange(self.z_ext)) % n
            c, s = np.cos(self.angle(kz, z)), np.sin(self.angle(kz, z))
            wz[h, 0, :self.z_ext] = np.where(im[:, None], -s, c).T
            wz[h, 1, :self.z_ext] = np.where(im[:, None], c, s).T
            re_w, im_w = np.where(im[:, None], -s, c), np.where(im[:, None], c, s)
            wi[h, :, 0, :self.z_ext] = re_w
            wi[h, :, 1, :self.z_ext] = im_w
            wi[h, :, 2, :self.z_ext] = -kd * im_w
            wi[h, :, 3, :self.z_ext] = kd * re_w
        out["wz"] = table3(wz)
        out["wi"] = table3(wi.reshape(2, 2 * n, 4 * LANES))
        ky = np.arange(n)
        my = np.zeros((2, n, self.n_chip, self.y_pad))
        ei = np.zeros((self.n_chip, 4, self.y_pad, n))
        for i in range(self.n_chip):
            y = (i * self.y_blk + np.arange(self.y_ext)) % n
            th = self.angle(ky, y)
            my[0, :, i, :self.y_ext] = np.cos(th)
            my[1, :, i, :self.y_ext] = np.sin(th)
            ei[i, 0, :self.y_ext] = np.cos(th).T
            ei[i, 1, :self.y_ext] = np.sin(th).T
            ei[i, 2, :self.y_ext] = (self.deriv(ky)[:, None] * np.cos(th)).T
            ei[i, 3, :self.y_ext] = (self.deriv(ky)[:, None] * np.sin(th)).T
        out["my"] = table3(my.reshape(2 * n, self.n_chip * self.y_pad))
        out["ei"] = table3(ei.reshape(self.n_chip, 4 * self.y_pad, n))
        return out


def cost(flops):
    return pl.CostEstimate(flops=int(flops), bytes_accessed=1 << 20, transcendentals=0)


X_BATCH = 10


def x_kernel(plan, ids_ref, rho_ref, gas_ref, far_ref, mx_ref, *rest):
    lhs_ref, tmp_ref = rest[-2:]
    core = ids_ref[0]
    n, kp = plan.n, plan.k_pad

    @pl.when(pl.program_id(0) == 0)
    def _():
        tmp_ref[...] = jnp.zeros(tmp_ref.shape, F32)
        for m in range(3):
            lhs_ref[m] = jnp.concatenate([mx_ref[m, core], mx_ref[m, 1 - core]], axis=0)

    keep = ids_ref[2].astype(F32)
    tmp_ref[:, :, :plan.z_blk] = gas_ref[...] * keep + far_ref[...]
    n_grp = len(plan.groups)
    lhs = [lhs_ref[m] for m in range(3)]
    for pair in range(X_BATCH // 2):
        ys = (2 * pair, 2 * pair + 1)
        data = jnp.concatenate([rho_ref[y, :n, :] + tmp_ref[y] for y in ys], axis=1)
        res = mul6(lhs, split3(data))
        for h in range(2):
            for g in range(n_grp):
                out = rest[h * n_grp + g]
                for pos, y in enumerate(ys):
                    for ri in range(2):
                        r0 = (2 * h + ri) * kp + plan.k_beg[g]
                        out[ri, y] = res[r0:r0 + plan.k_rows[g], pos * LANES:(pos + 1) * LANES]


def x_call(plan, ids, rho, gas, far, mx):
    steps = plan.y_even // X_BATCH
    shapes = tuple(jax.ShapeDtypeStruct((2, plan.y_even, k, LANES), F32) for k in plan.k_rows)
    out_specs = tuple(pl.BlockSpec((2, X_BATCH, k, LANES), lambda i: (0, i, 0, 0)) for k in plan.k_rows)
    gas_spec = pl.BlockSpec((X_BATCH, plan.n, plan.z_blk), lambda i: (i, 0, 0))
    outs = pl.pallas_call(
        functools.partial(x_kernel, plan), grid=(steps,), out_shape=shapes + shapes,
        in_specs=[SMEM_SPEC, pl.BlockSpec((X_BATCH, plan.x_pad, LANES), lambda i: (i, 0, 0)),
                  gas_spec, gas_spec,
                  pl.BlockSpec(mx.shape, lambda i: (0, 0, 0, 0))],
        out_specs=out_specs + out_specs,
        scratch_shapes=[pltpu.VMEM((3, 4 * plan.k_pad, plan.n), BF16), pltpu.VMEM((X_BATCH, plan.n, LANES), F32)],
        compiler_params=pltpu.CompilerParams(vmem_limit_bytes=32 << 20), name="dft_x",
    )(ids, rho, gas, far, mx)
    return outs[:len(shapes)], outs[len(shapes):]


Z_BATCH = 10


def z_kernel(plan, grp, ids_ref, own_ref, rec_ref, wz_ref, *rest):
    outs, tmp_ref = rest[:-1], rest[-1]
    step = pl.program_id(0)
    core, chip = ids_ref[0], ids_ref[1]
    kp, sl, ye, rows = plan.k_rows[grp], plan.groups[grp], plan.y_ext, plan.rows[grp]

    @pl.when(step == 0)
    def _():
        for out in outs:
            for g in range(3):
                out[g, rows - 8:rows, :] = jnp.zeros((8, LANES), F32)

    flat = (Z_BATCH * kp, LANES)
    data = jnp.concatenate([own_ref[0].reshape(flat), rec_ref[0].reshape(flat),
                            own_ref[1].reshape(flat), rec_ref[1].reshape(flat)], axis=1)
    wts = [jnp.concatenate([wz_ref[m, core, 0], wz_ref[m, 1 - core, 0], wz_ref[m, core, 1], wz_ref[m, 1 - core, 1]], axis=0)
           for m in range(3)]
    res = mul6(split3(data), wts)
    for g in range(3):
        tmp_ref[g] = res[:, g * LANES:(g + 1) * LANES]
    for b in range(Z_BATCH):
        y = step * Z_BATCH + b

        @pl.when(y < ye)
        def _():
            for r, out in enumerate(outs):
                for g in range(3):
                    out[g, pl.ds(y, sl, stride=ye), :] = tmp_ref[g, pl.ds(b * kp + (chip ^ r) * sl, sl), :]


def z_call(plan, grp, ids, own, rec, wz):
    kp = plan.k_rows[grp]
    blk = pl.BlockSpec((2, Z_BATCH, kp, LANES), lambda i: (0, i, 0, 0))
    shape = (3, plan.rows[grp], LANES)
    return pl.pallas_call(
        functools.partial(z_kernel, plan, grp), grid=(plan.y_even // Z_BATCH,),
        out_shape=(jax.ShapeDtypeStruct(shape, F32),) * plan.n_chip,
        in_specs=[SMEM_SPEC, blk, blk, pl.BlockSpec(wz.shape, lambda i: (0,) * 5)],
        out_specs=(pl.BlockSpec(shape, lambda i: (0, 0, 0)),) * plan.n_chip,
        scratch_shapes=[pltpu.VMEM((3, Z_BATCH * kp, LANES), F32)],
        cost_estimate=cost(12 * 50 * kp * 512 * 384),
        compiler_params=pltpu.CompilerParams(vmem_limit_bytes=24 << 20), name="dft_z",
    )(ids, own, rec, wz)


def signed(ids, n):
    return jnp.where(ids < n // 2, ids, ids - n).astype(F32)


def y_kernel(plan, grp, ids_ref, *refs):
    nc = plan.n_chip
    recs, (my_ref, ei_ref), outs, buf_ref = refs[:nc], refs[nc:nc + 2], refs[nc + 2:2 * nc + 2], refs[-1]
    n, ye, yp, n_rows = plan.n, plan.y_ext, plan.y_pad, plan.rows[grp]
    core, chip = ids_ref[0], ids_ref[1]
    kx_beg = core * plan.per_core + chip * plan.slots + plan.s_beg[grp]
    k_unit = 2.0 * math.pi / n
    buf_ref[...] = jnp.zeros(buf_ref.shape, F32)
    for out in outs:
        for c in range(2):
            for g in range(3):
                out[c, g, n_rows - 8:n_rows, :] = jnp.zeros((8, LANES), F32)
    lane = lax.broadcasted_iota(jnp.int32, (n, LANES), 1)
    ky = signed(lax.broadcasted_iota(jnp.int32, (n, LANES), 0), n)
    kz_a = signed(lane, n)
    kz_b = signed(128 + (lane & 63), n)
    yz_a, yz_b = ky * ky + kz_a * kz_a, ky * ky + kz_b * kz_b
    flip = jnp.where(lax.broadcasted_iota(jnp.int32, (1, LANES), 1) < 64, 1.0, -1.0)

    def slot(s, energy):
        rows = pl.ds(s * ye, ye)
        for r, rec in enumerate(recs):
            for g in range(3):
                buf_ref[g, pl.ds(pl.multiple_of((chip ^ r) * yp, 8), ye), :] = rec[g, rows, :]
        data = jnp.concatenate([buf_ref[g] for g in range(3)], axis=1)
        q = mul6([my_ref[m] for m in range(3)], split3(data))
        c = [q[:n, g * LANES:(g + 1) * LANES] for g in range(3)]
        d = [q[n:, g * LANES:(g + 1) * LANES] for g in range(3)]
        r0 = c[0] + d[1]
        r1 = c[1] - d[0]
        r2 = c[2] + flip * pltpu.roll(d[2], 64, 1)
        kx_i = kx_beg + s
        kx = kx_i.astype(F32)
        weight = jnp.where(kx_i < n // 2, jnp.where(kx_i == 0, 1.0, 2.0), jnp.where(kx_i == n // 2, 1.0, 0.0))
        scale = -4.0 * math.pi * GRAV_CONST / (k_unit * k_unit)

        def influence(yz):
            sq = yz + kx * kx
            return jnp.where(sq > 0, scale / jnp.maximum(sq, 1.0), 0.0)
        g_a, g_b = influence(yz_a), influence(yz_b)
        power = g_a * (r0 * r0 + r1 * r1) + g_b * (r2 * r2)
        energy = energy + weight * jnp.sum(power, axis=0, keepdims=True)
        parts = split3(jnp.concatenate([g_a * r0, g_a * r1, g_b * r2], axis=1))
        for r, out in enumerate(outs):
            if r % 2 == 0:
                lhs = [jnp.concatenate([ei_ref[m, chip ^ r], ei_ref[m, chip ^ (r + 1)]], axis=0) for m in range(3)]
                two = mul6(lhs, parts)
            p = two[(r % 2) * 4 * yp:(r % 2 + 1) * 4 * yp]
            co, si, ck, sk = [[p[u * yp:(u + 1) * yp, g * LANES:(g + 1) * LANES] for g in range(3)] for u in range(4)]
            pot = (co[0] - si[1], co[1] + si[0], co[2] - flip * pltpu.roll(si[2], 64, 1))
            dy = (-(ck[1] + sk[0]), ck[0] - sk[1], -flip * pltpu.roll(ck[2], 64, 1) - sk[2])
            for comp, val in ((0, pot), (1, dy)):
                for g in range(3):
                    out[comp, g, rows, :] = val[g][:ye]
        return energy

    energy = lax.fori_loop(0, plan.groups[grp], slot, jnp.zeros((1, LANES), F32))
    e_row = plan.groups[grp] * ye
    for out in outs:
        out[0, 0, e_row:e_row + 1, :] = energy


def y_call(plan, grp, ids, recs, my, ei):
    shape = jax.ShapeDtypeStruct((2, 3, plan.rows[grp], LANES), F32)
    return pl.pallas_call(
        functools.partial(y_kernel, plan, grp),
        out_shape=(shape,) * plan.n_chip,
        in_specs=[SMEM_SPEC] + [VMEM_SPEC] * (plan.n_chip + 2), out_specs=(VMEM_SPEC,) * plan.n_chip,
        scratch_shapes=[pltpu.VMEM((3, plan.n_chip * plan.y_pad, LANES), F32)],
        cost_estimate=cost(12 * plan.groups[grp] * 384 * (384 * 224 + 896 * 192)),
        compiler_params=pltpu.CompilerParams(vmem_limit_bytes=24 << 20), name="dft_y",
    )(ids, *recs, my, ei)


def zi_kernel(plan, grp, ids_ref, *refs):
    nc = plan.n_chip
    recs, wi_ref, own_ref, send_ref, buf_ref, e_ref = refs[:nc], *refs[nc:]
    step = pl.program_id(0)
    core, chip = ids_ref[0], ids_ref[1]
    kp, sl, ye = plan.k_rows[grp], plan.groups[grp], plan.y_ext

    @pl.when(step == 0)
    def _():
        buf_ref[...] = jnp.zeros(buf_ref.shape, F32)

    for comp in range(2):
        for b in range(Z_BATCH):
            for r, rec in enumerate(recs):
                for g in range(3):
                    buf_ref[g, pl.ds((comp * Z_BATCH + b) * kp + (chip ^ r) * sl, sl), :] = (
                        rec[comp, g, pl.ds(step * Z_BATCH + b, sl, stride=ye), :])
    half_rows = Z_BATCH * kp
    parts = split3(jnp.concatenate([buf_ref[g] for g in range(3)], axis=1))
    pot = [p[:half_rows] for p in parts]
    for half, out in ((core, own_ref), (1 - core, send_ref)):
        plain = mul6(parts, [wi_ref[m, half, :, :2 * LANES] for m in range(3)])
        along = mul6(pot, [wi_ref[m, half, :, 2 * LANES:] for m in range(3)])
        for b in range(Z_BATCH):
            for ri in range(2):
                ln = slice(ri * LANES, (ri + 1) * LANES)
                out[0, ri, b] = plain[b * kp:(b + 1) * kp, ln]
                out[1, ri, b] = plain[half_rows + b * kp:half_rows + (b + 1) * kp, ln]
                out[2, ri, b] = along[b * kp:(b + 1) * kp, ln]

    @pl.when(step == pl.num_programs(0) - 1)
    def _():
        e_row = sl * ye
        for r, rec in enumerate(recs):
            e_ref[pl.ds(chip ^ r, 1), :] = rec[0, 0, e_row:e_row + 1, :]
        total = e_ref[0:1, :]
        for t in range(1, nc):
            total = total + e_ref[t:t + 1, :]
        own_ref[0, 0, Z_BATCH - 1, 0:1, :] = total
        send_ref[0, 0, Z_BATCH - 1, 0:1, :] = total


def zi_call(plan, grp, ids, recs, wi):
    kp = plan.k_rows[grp]
    shape = jax.ShapeDtypeStruct((3, 2, plan.y_even, kp, LANES), F32)
    spec = pl.BlockSpec((3, 2, Z_BATCH, kp, LANES), lambda i: (0, 0, i, 0, 0))
    return pl.pallas_call(
        functools.partial(zi_kernel, plan, grp), grid=(plan.y_even // Z_BATCH,), out_shape=(shape, shape),
        in_specs=[SMEM_SPEC] + [pl.BlockSpec(r.shape, lambda i: (0,) * 4) for r in recs]
        + [pl.BlockSpec(wi.shape, lambda i: (0,) * 4)],
        out_specs=(spec, spec),
        scratch_shapes=[pltpu.VMEM((3, 2 * Z_BATCH * kp, LANES), F32), pltpu.VMEM((8, LANES), F32)],
        cost_estimate=cost(12 * 50 * kp * 384 * 512 * 3),
        compiler_params=pltpu.CompilerParams(vmem_limit_bytes=32 << 20), name="idft_z",
    )(ids, *recs, wi)


def field_kernel(plan, n_xt, e_norm, ids_ref, table_ref, num_ref, slot_ref, mi_ref, *refs):
    n_grp = len(plan.groups)
    sides = (refs[:n_grp], refs[n_grp:2 * n_grp])
    out_ref, energy_ref, fhm_ref, flo_ref, lhs_ref = refs[2 * n_grp:]
    core = ids_ref[0]
    for m in range(3):
        for kind in range(2):
            lhs_ref[m, kind] = jnp.concatenate([mi_ref[m, core, kind], mi_ref[m, 1 - core, kind]], axis=1)

    def column(c, y):
        return jnp.concatenate([ref[c, ri, y] for side in sides for ri in range(2) for ref in side], axis=0)

    def put(res, spots):
        hi, mid, lo = split3(res)
        for pos, (y, c) in enumerate(spots):
            ln = slice(pos * LANES, (pos + 1) * LANES)
            fhm_ref[y, c, :, :LANES] = hi[:, ln]
            fhm_ref[y, c, :, LANES:] = mid[:, ln]
            flo_ref[y, c] = lo[:, ln]

    def planes(step, carry):
        y0 = 2 * step
        data = jnp.concatenate([column(0, y0), column(0, y0 + 1)], axis=1)
        put(mul6([lhs_ref[m, 0] for m in range(3)], split3(data)), ((y0, 0), (y0 + 1, 0)))
        for y in (y0, y0 + 1):
            data = jnp.concatenate([column(1, y), column(2, y)], axis=1)
            put(mul6([lhs_ref[m, 1] for m in range(3)], split3(data)), ((y, 1), (y, 2)))
        return carry
    lax.fori_loop(0, plan.y_even // 2, planes, 0)
    lanes = None
    for own, rec in zip(*sides):
        pair = own[0, 0, plan.y_even - 1, 0:1, :] + rec[0, 0, plan.y_even - 1, 0:1, :]
        lanes = pair if lanes is None else lanes + pair
    energy_ref[...] = jnp.broadcast_to(jnp.sum(lanes, axis=1, keepdims=True) * e_norm, energy_ref.shape)
    interp_kernel(n_xt, table_ref, num_ref, slot_ref, fhm_ref, flo_ref, out_ref)


def field_call(plan, ids, table, num, slots, own, rec, mi, n_xt, e_norm):
    return pl.pallas_call(
        functools.partial(field_kernel, plan, n_xt, e_norm),
        out_shape=(jax.ShapeDtypeStruct((SLOT_ROWS, LANES), F32), jax.ShapeDtypeStruct((8, LANES), F32)),
        in_specs=[SMEM_SPEC, SMEM_SPEC, SMEM_SPEC] + [VMEM_SPEC] * (2 + 2 * len(own)), out_specs=(VMEM_SPEC, VMEM_SPEC),
        scratch_shapes=[pltpu.VMEM((plan.y_even, 3, plan.x_pad, 2 * LANES), BF16),
                        pltpu.VMEM((plan.y_even, 3, plan.x_pad, LANES), BF16),
                        pltpu.VMEM((3, 2, plan.x_pad, 4 * plan.k_pad), BF16)],
        compiler_params=pltpu.CompilerParams(vmem_limit_bytes=VMEM_BIG), name="idft_x_interp",
    )(ids, table, num, slots, mi, *own, *rec)


def solution(mesh):
    n_cols = mesh.shape["col"]
    n_cx = mesh.shape["row"] // 2
    fine = jax.sharding.Mesh(mesh.devices.reshape(mesh.shape["rep"], n_cols, n_cx, 2), ("rep", "col", "cx", "core"))
    slot_axes = ("rep", "col", "cx", "core")
    chip_axes = ("col", "cx")
    turn = [(a * 2 + b, b * 2 + a) for a in range(n_cols) for b in range(2) if a != b]
    other_core = [(0, 1), (1, 0)]

    def device_body(part_mass, cell_idx, cic_wts, live_mask, gas_block):
        grid_size, y_blk, z_blk = gas_block.shape
        per_dev = part_mass.shape[0]
        n_chip = n_cx * n_cols
        n_slots = per_dev * n_chip * 2
        plan = Plan(grid_size, n_chip, y_blk, z_blk)
        tab = plan.tables()
        core = lax.axis_index("core").astype(jnp.int32)
        chip = (lax.axis_index("cx") * n_cols + lax.axis_index("col")).astype(jnp.int32)
        n_xt = grid_size // X_TILE
        n_blk = y_blk * n_xt

        keep = (core == lax.axis_index("col")).astype(jnp.int32)

        def swap(arr):
            return lax.ppermute(arr, ("col", "core"), turn)

        raw = slot_arrays(part_mass, cell_idx, cic_wts, live_mask, y_blk)
        raw = swap(raw) + raw * keep.astype(F32)
        gas = jnp.pad(jnp.transpose(gas_block, (1, 0, 2)), ((0, plan.y_even - y_blk), (0, 0), (0, 0)))
        raw, gas = lax.optimization_barrier((raw, gas))
        gas_far = swap(gas)
        table, num = pair_table(raw[0].reshape(-1), n_blk, n_xt)
        slots = sort_call(raw)
        rho = deposit_call(table, num, slots, plan.y_even, grid_size, n_xt)
        ids = jnp.stack([core, chip, keep])
        own, send = x_call(plan, ids, rho, gas, gas_far, tab["mx"])

        def exchange(parts):
            out = [parts[0]]
            for r in range(1, n_chip):
                flip = (r >> 1) | ((r & 1) << 1)
                out.append(lax.ppermute(parts[r], chip_axes, [(t, t ^ flip) for t in range(n_chip)]))
            return out

        grps = range(len(plan.groups))

        def chain(token, outs):
            return lax.optimization_barrier((token, tuple(outs)))

        rec = [lax.ppermute(s, "core", other_core) for s in send]
        at_y, at_z, halves = [], [], []
        for g in grps:
            ids, out = chain(ids, z_call(plan, g, ids, own[g], rec[g], tab["wz"]))
            at_y.append(exchange(out))
        for g in grps:
            ids, out = chain(ids, y_call(plan, g, ids, at_y[g], tab["my"], tab["ei"]))
            at_z.append(exchange(out))
        for g in grps:
            ids, out = chain(ids, zi_call(plan, g, ids, at_z[g], tab["wi"]))
            halves.append(out)
        rec = [lax.ppermute(h[1], "core", other_core) for h in halves]
        e_norm = 0.5 / (grid_size ** 3 * n_slots)
        forces, energy = field_call(plan, ids, table, num, slots, [h[0] for h in halves], rec, tab["mi"], n_xt, e_norm)
        back = unsort_call(slots, forces)
        home = swap(back) + back * keep.astype(F32)
        return home.reshape(3, per_dev).T, energy[0, 0:1]

    return jax.shard_map(
        device_body, mesh=fine,
        in_specs=(P(slot_axes), P(slot_axes, None), P(slot_axes, None, None), P(slot_axes), P("rep", ("cx", "core"), "col")),
        out_specs=(P(slot_axes, None), P("rep")), check_vma=False)
```

```python
import functools
import math
import numpy as np
import jax
import jax.numpy as jnp
from jax import lax
from jax.sharding import PartitionSpec as P
from jax.experimental import pallas as pl
from jax.experimental.pallas import tpu as pltpu

MATMUL_PREC = lax.Precision.HIGHEST
GRAV_CONST = 1.0
F32 = jnp.float32
BF16 = jnp.bfloat16
LANES = 128
X_TILE = 96
X_ROWS = 112
Y_SHIFT = 15
X_SHIFT = 7
VMEM_BIG = 60 * 1024 * 1024


def split3(val):
    hi = val.astype(BF16)
    rest = val - hi.astype(F32)
    mid = rest.astype(BF16)
    lo = (rest - mid.astype(F32)).astype(BF16)
    return hi, mid, lo


def bitonic(bufs):
    sub = lax.broadcasted_iota(jnp.int32, (8, LANES), 0)
    lane = lax.broadcasted_iota(jnp.int32, (8, LANES), 1)
    base = lane * 128 + sub

    def bit(rank, pos):
        return lax.shift_right_logical(rank, jnp.full_like(rank, pos)) & 1

    def vreg_stage(k, j):
        step = 1 << (j - 3)
        for v in range(16):
            if v & step:
                continue
            low, high = pl.ds(8 * v, 8), pl.ds(8 * (v + step), 8)
            sgn = 1.0 - 2.0 * bit(base + 8 * v, k).astype(F32)
            a = [b[low, :] for b in bufs]
            c = [b[high, :] for b in bufs]
            swap = a[0] * sgn > c[0] * sgn
            for b, p, q in zip(bufs, a, c):
                b[low, :] = jnp.where(swap, q, p)
                b[high, :] = jnp.where(swap, p, q)

    def roll_stage(k, j, dist, axis):
        size = (8, LANES)[axis]
        upper = bit(base, j)
        keep_low = upper == 0
        for v in range(16):
            rows = pl.ds(8 * v, 8)
            sgn = 1.0 - 2.0 * (bit(base + 8 * v, k) ^ upper).astype(F32)
            own = [b[rows, :] for b in bufs]
            other = [jnp.where(keep_low, pltpu.roll(o, size - dist, axis), pltpu.roll(o, dist, axis)) for o in own]
            take = other[0] * sgn < own[0] * sgn
            for b, o, p in zip(bufs, own, other):
                b[rows, :] = jnp.where(take, p, o)

    def stage(k, j):
        if j >= 3:
            vreg_stage(k, j)
        else:
            roll_stage(k, j, 1 << j, 0)

    for k in range(1, 8):
        for j in range(k - 1, -1, -1):
            stage(k, j)

    def phase(k, carry):
        def lane_stage(step, c):
            j = k - 1 - step
            roll_stage(k, j, jnp.left_shift(1, j - 7), 1)
            return c
        lax.fori_loop(0, k - 7, lane_stage, 0)
        for j in range(6, -1, -1):
            stage(k, j)
        return carry
    lax.fori_loop(8, 15, phase, 0)


CHUNKS = 128
UNROLL = 4
SLOT_ROWS = 8 * (CHUNKS + 1)


def sort_kernel(in_ref, out_ref, *bufs):
    for n in range(5):
        bufs[n][...] = in_ref[n]
    row = lax.broadcasted_iota(jnp.int32, (CHUNKS, LANES), 0)
    col = lax.broadcasted_iota(jnp.int32, (CHUNKS, LANES), 1)
    bufs[5][...] = (row * LANES + col).astype(F32)
    bitonic(bufs)
    zero = jnp.zeros((CHUNKS, LANES), F32)
    for n in range(8):
        out_ref[pl.ds(n, CHUNKS, stride=8), :] = bufs[n][...].T if n < 6 else zero
    out_ref[8 * CHUNKS:, :] = jnp.zeros((8, LANES), F32)


def unsort_kernel(slot_ref, low_ref, high_ref, out_ref, *bufs):
    bufs[0][...] = slot_ref[pl.ds(5, CHUNKS, stride=8), :]
    for n in range(3):
        rows = pl.ds(n, CHUNKS, stride=8)
        bufs[n + 1][...] = low_ref[rows, :] + high_ref[rows, :]
    bitonic(bufs)
    for n in range(3):
        out_ref[n] = bufs[n + 1][...].T


def pair_table(key, n_blk, n_xt):
    b_ids = jnp.arange(n_blk + 1)
    bounds = ((b_ids // n_xt) << Y_SHIFT) | (((b_ids % n_xt) * X_TILE) << X_SHIFT)
    starts = jnp.sum((key[None, :] < bounds[:, None].astype(F32)).astype(jnp.int32), axis=1)
    first, last = starts[:-1], starts[1:]
    count = (last - first + LANES - 1) // LANES
    ids = jnp.arange(n_blk)
    ends = jnp.sum(jnp.where(ids[None, :] <= ids[:, None], count[None, :], 0), axis=1)
    t_ids = jnp.arange(n_blk + CHUNKS + 2 * UNROLL)
    blk = jnp.sum((ends[None, :] <= t_ids[:, None]).astype(jnp.int32), axis=1)
    hot = ids[None, :] == blk[:, None]
    beg = jnp.sum(jnp.where(hot, (first - LANES * (ends - count))[None, :], 0), axis=1) + LANES * t_ids
    size = jnp.minimum(jnp.sum(jnp.where(hot, last[None, :], 0), axis=1) - beg, LANES)
    live = t_ids < ends[-1]
    table = jnp.stack([jnp.where(live, blk, 0), jnp.where(live, beg, 0), jnp.where(live, size, 0)])
    bounds = jnp.stack([jnp.zeros_like(ends[0]), ends[n_blk // 2 - 1], ends[-1]])
    return table.astype(jnp.int32), bounds.astype(jnp.int32)


def read_window(t, table_ref, slot_ref, n_xt):
    blk = table_ref[0, t]
    beg = table_ref[1, t]
    size = table_ref[2, t]
    y_pl = blk // n_xt
    x_beg = pl.multiple_of((blk % n_xt) * X_TILE, 16)
    row = pl.multiple_of((beg >> 7) * 8, 8)
    off = beg & 127
    back = (LANES - off) & 127
    lane = lax.broadcasted_iota(jnp.int32, (8, LANES), 1)
    win = jnp.where(lane < LANES - off, pltpu.roll(slot_ref[pl.ds(row, 8), :], back, 1),
                    pltpu.roll(slot_ref[pl.ds(row + 8, 8), :], back, 1))
    code = win[0:1].astype(jnp.int32)
    x_c = (code >> X_SHIFT) & 255
    vals = [win[n:n + 1] for n in range(1, 5)]
    return row, off, size, lane, y_pl, x_beg, x_c - x_beg, code & 127, vals


def spread_rows(row):
    return jnp.broadcast_to(row, (16, LANES)).astype(BF16)


def deposit_kernel(n_xt, grid_size, table_ref, num_ref, slot_ref, rho_ref):
    n_planes = rho_ref.shape[0]

    def clear(y, c):
        rho_ref[y] = jnp.zeros(rho_ref.shape[1:], F32)
        return c
    lax.fori_loop(0, n_planes, clear, 0)
    row_x = lax.broadcasted_iota(jnp.int32, (X_ROWS, LANES), 0)
    row_z = lax.broadcasted_iota(jnp.int32, (LANES, LANES), 0)

    def one(t):
        row, off, size, lane, y_pl, x_beg, x_l, z_c, (q, wx, wy, wz) = read_window(t, table_ref, slot_ref, n_xt)
        q = jnp.where(lane[0:1] < size, q, 0.0)
        pick_x = jnp.concatenate([(row_x == x_l).astype(F32), (row_x == x_l + 1).astype(F32)], axis=1).astype(BF16)
        pick_z = [(row_z == z_c + c).astype(F32).astype(BF16).reshape(8, 16, LANES) for c in range(2)]
        cols = [[], [], []]
        for w_y in (1.0 - wy, wy):
            pieces = [[], [], []]
            for w_x in (1.0 - wx, wx):
                base = q * w_x * w_y
                lower, upper = split3(base * (1.0 - wz)), split3(base * wz)
                for m in range(3):
                    low = spread_rows(lower[m].astype(F32))[None]
                    high = spread_rows(upper[m].astype(F32))[None]
                    pieces[m].append((pick_z[0] * low + pick_z[1] * high).reshape(LANES, LANES))
            for m in range(3):
                cols[m].append(jnp.concatenate(pieces[m], axis=1))
        res = None
        for m in (2, 1, 0):
            part = jnp.concatenate(cols[m], axis=0)
            term = lax.dot_general(pick_x, part, (((1,), (1,)), ((), ())), preferred_element_type=F32)
            res = term if res is None else res + term
        for b in range(2):
            rho_ref[y_pl + b, pl.ds(x_beg, X_ROWS), :] += res[:, b * LANES:(b + 1) * LANES]

    def body(t, c):
        for u in range(UNROLL):
            one(UNROLL * t + u)
        return c
    lax.fori_loop(0, (num_ref[2] + UNROLL - 1) // UNROLL, body, 0)

    def wrap(y, c):
        rho_ref[y, 0:8, :] += rho_ref[y, grid_size:grid_size + 8, :]
        return c
    lax.fori_loop(0, n_planes, wrap, 0)


def interp_kernel(n_xt, y_beg, n_y, t_beg, t_end, table_ref, slot_ref, fhm_ref, flo_ref, out_ref):
    row_x = lax.broadcasted_iota(jnp.int32, (X_ROWS, LANES), 0)
    row_z = lax.broadcasted_iota(jnp.int32, (LANES, LANES), 0)
    out_ref[...] = jnp.zeros(out_ref.shape, F32)

    def one(t):
        row, off, size, lane, y_pl, x_beg, x_l, z_c, (q, wx, wy, wz) = read_window(t, table_ref, slot_ref, n_xt)
        size = jnp.where(t < t_end, size, 0)
        y_pl = jnp.clip(y_pl - y_beg, 0, n_y - 2)
        pick_z = jnp.concatenate([(row_z == z_c).astype(F32), (row_z == z_c + 1).astype(F32)], axis=1).astype(BF16)
        pick_2 = jnp.concatenate([pick_z, pick_z], axis=0)
        on_x = jnp.where(row_x == x_l, 1.0 - wx, jnp.where(row_x == x_l + 1, wx, 0.0))
        rows = pl.ds(x_beg, X_ROWS)
        wt = [on_x * (1.0 - wy), on_x * wy]
        grads = []
        for comp in range(3):
            top = jnp.concatenate([fhm_ref[y_pl + b, comp, rows, :] for b in range(2)], axis=0)
            low = jnp.concatenate([flo_ref[y_pl + b, comp, rows, :] for b in range(2)], axis=0)
            got = jnp.dot(low, pick_z, preferred_element_type=F32) + jnp.dot(top, pick_2, preferred_element_type=F32)
            got = got[:, :LANES] * (1.0 - wz) + got[:, LANES:] * wz
            acc = got[:X_ROWS] * wt[0] + got[X_ROWS:] * wt[1]
            grads.append(-q * jnp.sum(acc, axis=0, keepdims=True))
        full = pltpu.roll(jnp.concatenate(grads + [jnp.zeros((5, LANES), F32)], axis=0), off, 1)
        here, after = pl.ds(row, 8), pl.ds(row + 8, 8)
        out_ref[here, :] = jnp.where((lane >= off) & (lane - off < size), full, out_ref[here, :])
        out_ref[after, :] = jnp.where((lane < off) & (lane + LANES - off < size), full, out_ref[after, :])

    def body(t, c):
        for u in range(UNROLL):
            one(t_beg + UNROLL * t + u)
        return c
    lax.fori_loop(0, (t_end - t_beg + UNROLL - 1) // UNROLL, body, 0)


SMEM_SPEC = pl.BlockSpec(memory_space=pltpu.SMEM)
VMEM_SPEC = pl.BlockSpec(memory_space=pltpu.VMEM)


def sort_call(raw):
    return pl.pallas_call(
        sort_kernel, out_shape=jax.ShapeDtypeStruct((SLOT_ROWS, LANES), F32), in_specs=[VMEM_SPEC], out_specs=VMEM_SPEC,
        scratch_shapes=[pltpu.VMEM((CHUNKS, LANES), F32)] * 6, name="slot_sort",
    )(raw)


def unsort_call(slots, low, high):
    return pl.pallas_call(
        unsort_kernel, out_shape=jax.ShapeDtypeStruct((3, CHUNKS, LANES), F32),
        in_specs=[VMEM_SPEC] * 3, out_specs=VMEM_SPEC,
        scratch_shapes=[pltpu.VMEM((CHUNKS, LANES), F32)] * 4, name="slot_unsort",
    )(slots, low, high)


def deposit_call(table, num, slots, y_ext, grid_size, n_xt):
    return pl.pallas_call(
        functools.partial(deposit_kernel, n_xt, grid_size),
        out_shape=jax.ShapeDtypeStruct((y_ext, grid_size + 16, LANES), F32),
        in_specs=[SMEM_SPEC, SMEM_SPEC, VMEM_SPEC], out_specs=VMEM_SPEC,
        compiler_params=pltpu.CompilerParams(vmem_limit_bytes=VMEM_BIG), name="deposit",
    )(table, num, slots)


def slot_arrays(part_mass, cell_idx, cic_wts, live_mask, y_blk):
    charge = part_mass * live_mask.astype(F32)
    code = (cell_idx[:, 1] << Y_SHIFT) | (cell_idx[:, 0] << X_SHIFT) | cell_idx[:, 2]
    code = jnp.where(live_mask > 0, code, y_blk << Y_SHIFT).astype(F32)
    upper = cic_wts[:, :, 1]
    return jnp.stack([code, charge, upper[:, 0], upper[:, 1], upper[:, 2]]).reshape(5, CHUNKS, LANES)


def mul6(a, b):
    res = None
    for m, n in ((2, 0), (0, 2), (1, 1), (1, 0), (0, 1), (0, 0)):
        term = jnp.dot(a[m], b[n], preferred_element_type=F32)
        res = term if res is None else res + term
    return res


def table3(mat):
    mat = mat.astype(np.float32)
    hi = mat.astype(BF16)
    mid = (mat - hi.astype(np.float32)).astype(BF16)
    lo = (mat - hi.astype(np.float32) - mid.astype(np.float32)).astype(BF16)
    return np.stack([hi, mid, lo])


GROUP_SLOTS = (6, 7)


class Plan:
    def __init__(self, n, n_chip, y_blk, z_blk):
        self.n, self.n_chip, self.y_blk, self.z_blk = n, n_chip, y_blk, z_blk
        self.y_ext = y_blk + 1
        self.z_ext = z_blk + 1
        self.y_pad = -(-self.y_ext // 8) * 8
        self.half_k = n // 2 + 1
        self.slots = -(-self.half_k // (2 * n_chip))
        self.per_core = self.slots * n_chip
        left, self.groups = self.slots, []
        for size in GROUP_SLOTS:
            self.groups.append(size)
            left -= size
        assert left == 0
        self.k_rows = [-(-size * n_chip // 8) * 8 for size in self.groups]
        self.k_beg = [sum(self.k_rows[:g]) for g in range(len(self.groups))]
        self.s_beg = [sum(self.groups[:g]) for g in range(len(self.groups))]
        self.k_pad = sum(self.k_rows)
        self.rows = [-(-(size * self.y_ext + 1) // 8) * 8 for size in self.groups]
        self.y_half = y_blk // 2 + 1
        self.half_rows = [-(-(size * self.y_half + 1) // 8) * 8 for size in self.groups]
        self.y_even = self.y_ext + self.y_ext % 2
        self.x_pad = n + 16

    def row_slots(self):
        ids = -np.ones(self.k_pad, np.int64)
        for g, size in enumerate(self.groups):
            for t in range(self.n_chip):
                r0 = self.k_beg[g] + t * size
                ids[r0:r0 + size] = t * self.slots + self.s_beg[g] + np.arange(size)
        return ids

    def angle(self, k, r):
        return 2.0 * np.pi / self.n * ((k[:, None] * r[None, :]) % self.n)

    def lane_order(self):
        kz = np.concatenate([np.arange(128), np.arange(128), np.arange(128, self.n), np.arange(128, self.n)])
        im = np.concatenate([np.zeros(128), np.ones(128), np.zeros(self.n - 128), np.ones(self.n - 128)]) > 0
        return kz, im

    def deriv(self, k):
        sgn = np.where(k < self.n // 2, k, k - self.n)
        return np.where(k == self.n // 2, 0, sgn) * (2.0 * np.pi / self.n)

    def tables(self):
        n = self.n
        out = {}
        mx = np.zeros((2, 2, self.k_pad, n))
        mi = np.zeros((2, 2, self.x_pad, 2, self.k_pad))
        ids = self.row_slots()
        for h in range(2):
            kx = np.where(ids >= 0, h * self.per_core + ids, n)
            ok = (kx < self.half_k)[:, None]
            th = self.angle(kx, np.arange(n))
            mx[h, 0] = np.where(ok, np.cos(th), 0.0)
            mx[h, 1] = np.where(ok, -np.sin(th), 0.0)
            th = self.angle(kx, np.arange(self.x_pad))
            wt = np.where(kx < self.half_k, np.where((kx == 0) | (kx == n // 2), 1.0, 2.0), 0.0) / float(n) ** 3
            kd = np.where(kx < n // 2, kx, 0) * (2.0 * np.pi / n) * wt
            mi[h, 0, :, 0] = (-kd[:, None] * np.sin(th)).T
            mi[h, 0, :, 1] = (-kd[:, None] * np.cos(th)).T
            mi[h, 1, :, 0] = (wt[:, None] * np.cos(th)).T
            mi[h, 1, :, 1] = (-wt[:, None] * np.sin(th)).T
        out["mx"] = table3(mx.reshape(2, 2 * self.k_pad, n))
        out["mi"] = table3(mi.reshape(2, 2, self.x_pad, 2 * self.k_pad))
        kz, im = self.lane_order()
        wz = np.zeros((2, 2, LANES, 2 * n))
        wi = np.zeros((2, 2 * n, 4, LANES))
        kd = self.deriv(kz)[:, None]
        for h in range(2):
            z = (h * self.z_blk + np.arange(self.z_ext)) % n
            c, s = np.cos(self.angle(kz, z)), np.sin(self.angle(kz, z))
            wz[h, 0, :self.z_ext] = np.where(im[:, None], -s, c).T
            wz[h, 1, :self.z_ext] = np.where(im[:, None], c, s).T
            re_w, im_w = np.where(im[:, None], -s, c), np.where(im[:, None], c, s)
            wi[h, :, 0, :self.z_ext] = re_w
            wi[h, :, 1, :self.z_ext] = im_w
            wi[h, :, 2, :self.z_ext] = -kd * im_w
            wi[h, :, 3, :self.z_ext] = kd * re_w
        out["wz"] = table3(wz)
        out["wi"] = table3(wi.reshape(2, 2 * n, 4 * LANES))
        ky = np.arange(n)
        my = np.zeros((2, n, self.n_chip, self.y_pad))
        ei = np.zeros((self.n_chip, 4, self.y_pad, n))
        for i in range(self.n_chip):
            y = (i * self.y_blk + np.arange(self.y_ext)) % n
            th = self.angle(ky, y)
            my[0, :, i, :self.y_ext] = np.cos(th)
            my[1, :, i, :self.y_ext] = np.sin(th)
            ei[i, 0, :self.y_ext] = np.cos(th).T
            ei[i, 1, :self.y_ext] = np.sin(th).T
            ei[i, 2, :self.y_ext] = (self.deriv(ky)[:, None] * np.cos(th)).T
            ei[i, 3, :self.y_ext] = (self.deriv(ky)[:, None] * np.sin(th)).T
        out["my"] = table3(my.reshape(2 * n, self.n_chip * self.y_pad))
        out["ei"] = table3(ei.reshape(self.n_chip, 4 * self.y_pad, n))
        return out


def cost(flops):
    return pl.CostEstimate(flops=int(flops), bytes_accessed=1 << 20, transcendentals=0)


X_BATCH = 10


def x_kernel(plan, ids_ref, rho_ref, gas_ref, far_ref, mx_ref, *rest):
    lhs_ref, tmp_ref = rest[-2:]
    core = ids_ref[0]
    n, kp = plan.n, plan.k_pad

    @pl.when(pl.program_id(0) == 0)
    def _():
        tmp_ref[...] = jnp.zeros(tmp_ref.shape, F32)
        for m in range(3):
            lhs_ref[m] = jnp.concatenate([mx_ref[m, core], mx_ref[m, 1 - core]], axis=0)

    keep = ids_ref[2].astype(F32)
    tmp_ref[:, :, :plan.z_blk] = gas_ref[...] * keep + far_ref[...]
    n_grp = len(plan.groups)
    lhs = [lhs_ref[m] for m in range(3)]
    for pair in range(X_BATCH // 2):
        ys = (2 * pair, 2 * pair + 1)
        data = jnp.concatenate([rho_ref[y, :n, :] + tmp_ref[y] for y in ys], axis=1)
        res = mul6(lhs, split3(data))
        for h in range(2):
            for g in range(n_grp):
                out = rest[h * n_grp + g]
                for pos, y in enumerate(ys):
                    for ri in range(2):
                        r0 = (2 * h + ri) * kp + plan.k_beg[g]
                        out[ri, y] = res[r0:r0 + plan.k_rows[g], pos * LANES:(pos + 1) * LANES]


def x_call(plan, ids, rho, gas, far, mx):
    steps = plan.y_even // X_BATCH
    shapes = tuple(jax.ShapeDtypeStruct((2, plan.y_even, k, LANES), F32) for k in plan.k_rows)
    out_specs = tuple(pl.BlockSpec((2, X_BATCH, k, LANES), lambda i: (0, i, 0, 0)) for k in plan.k_rows)
    gas_spec = pl.BlockSpec((X_BATCH, plan.n, plan.z_blk), lambda i: (i, 0, 0))
    outs = pl.pallas_call(
        functools.partial(x_kernel, plan), grid=(steps,), out_shape=shapes + shapes,
        in_specs=[SMEM_SPEC, pl.BlockSpec((X_BATCH, plan.x_pad, LANES), lambda i: (i, 0, 0)),
                  gas_spec, gas_spec,
                  pl.BlockSpec(mx.shape, lambda i: (0, 0, 0, 0))],
        out_specs=out_specs + out_specs,
        scratch_shapes=[pltpu.VMEM((3, 4 * plan.k_pad, plan.n), BF16), pltpu.VMEM((X_BATCH, plan.n, LANES), F32)],
        compiler_params=pltpu.CompilerParams(vmem_limit_bytes=32 << 20), name="dft_x",
    )(ids, rho, gas, far, mx)
    return outs[:len(shapes)], outs[len(shapes):]


Z_BATCH = 10


def z_kernel(plan, grp, ids_ref, own_ref, rec_ref, wz_ref, *rest):
    outs, tmp_ref = rest[:-1], rest[-1]
    step = pl.program_id(0)
    core, chip = ids_ref[0], ids_ref[1]
    kp, sl, ye, rows = plan.k_rows[grp], plan.groups[grp], plan.y_ext, plan.rows[grp]

    @pl.when(step == 0)
    def _():
        for out in outs:
            for g in range(3):
                out[g, rows - 8:rows, :] = jnp.zeros((8, LANES), F32)

    flat = (Z_BATCH * kp, LANES)
    data = jnp.concatenate([own_ref[0].reshape(flat), rec_ref[0].reshape(flat),
                            own_ref[1].reshape(flat), rec_ref[1].reshape(flat)], axis=1)
    wts = [jnp.concatenate([wz_ref[m, core, 0], wz_ref[m, 1 - core, 0], wz_ref[m, core, 1], wz_ref[m, 1 - core, 1]], axis=0)
           for m in range(3)]
    res = mul6(split3(data), wts)
    for g in range(3):
        tmp_ref[g] = res[:, g * LANES:(g + 1) * LANES]
    for b in range(Z_BATCH):
        y = step * Z_BATCH + b

        @pl.when(y < ye)
        def _():
            for r, out in enumerate(outs):
                for g in range(3):
                    out[g, pl.ds(y, sl, stride=ye), :] = tmp_ref[g, pl.ds(b * kp + (chip ^ r) * sl, sl), :]


def z_call(plan, grp, ids, own, rec, wz):
    kp = plan.k_rows[grp]
    blk = pl.BlockSpec((2, Z_BATCH, kp, LANES), lambda i: (0, i, 0, 0))
    shape = (3, plan.rows[grp], LANES)
    return pl.pallas_call(
        functools.partial(z_kernel, plan, grp), grid=(plan.y_even // Z_BATCH,),
        out_shape=(jax.ShapeDtypeStruct(shape, F32),) * plan.n_chip,
        in_specs=[SMEM_SPEC, blk, blk, pl.BlockSpec(wz.shape, lambda i: (0,) * 5)],
        out_specs=(pl.BlockSpec(shape, lambda i: (0, 0, 0)),) * plan.n_chip,
        scratch_shapes=[pltpu.VMEM((3, Z_BATCH * kp, LANES), F32)],
        cost_estimate=cost(12 * 50 * kp * 512 * 384),
        compiler_params=pltpu.CompilerParams(vmem_limit_bytes=24 << 20), name="dft_z",
    )(ids, own, rec, wz)


def signed(ids, n):
    return jnp.where(ids < n // 2, ids, ids - n).astype(F32)


def y_kernel(plan, grp, ids_ref, *refs):
    nc = plan.n_chip
    recs, (my_ref, ei_ref, e_in_ref) = refs[:nc], refs[nc:nc + 3]
    highs, lows, e_out_ref, buf_ref = refs[nc + 3:2 * nc + 3], refs[2 * nc + 3:3 * nc + 3], refs[-2], refs[-1]
    n, ye, yp, yh, n_rows = plan.n, plan.y_ext, plan.y_pad, plan.y_half, plan.half_rows[grp]
    core, chip = ids_ref[0], ids_ref[1]
    kx_beg = core * plan.per_core + chip * plan.slots + plan.s_beg[grp]
    k_unit = 2.0 * math.pi / n
    buf_ref[...] = jnp.zeros(buf_ref.shape, F32)
    for out in highs + lows:
        for c in range(2):
            for g in range(3):
                out[c, g, n_rows - 8:n_rows, :] = jnp.zeros((8, LANES), F32)
    lane = lax.broadcasted_iota(jnp.int32, (n, LANES), 1)
    ky = signed(lax.broadcasted_iota(jnp.int32, (n, LANES), 0), n)
    kz_a = signed(lane, n)
    kz_b = signed(128 + (lane & 63), n)
    yz_a, yz_b = ky * ky + kz_a * kz_a, ky * ky + kz_b * kz_b
    flip = jnp.where(lax.broadcasted_iota(jnp.int32, (1, LANES), 1) < 64, 1.0, -1.0)

    def slot(s, energy):
        rows = pl.ds(s * ye, ye)
        for r, rec in enumerate(recs):
            for g in range(3):
                buf_ref[g, pl.ds(pl.multiple_of((chip ^ r) * yp, 8), ye), :] = rec[g, rows, :]
        data = jnp.concatenate([buf_ref[g] for g in range(3)], axis=1)
        q = mul6([my_ref[m] for m in range(3)], split3(data))
        c = [q[:n, g * LANES:(g + 1) * LANES] for g in range(3)]
        d = [q[n:, g * LANES:(g + 1) * LANES] for g in range(3)]
        r0 = c[0] + d[1]
        r1 = c[1] - d[0]
        r2 = c[2] + flip * pltpu.roll(d[2], 64, 1)
        kx_i = kx_beg + s
        kx = kx_i.astype(F32)
        weight = jnp.where(kx_i < n // 2, jnp.where(kx_i == 0, 1.0, 2.0), jnp.where(kx_i == n // 2, 1.0, 0.0))
        scale = -4.0 * math.pi * GRAV_CONST / (k_unit * k_unit)

        def influence(yz):
            sq = yz + kx * kx
            return jnp.where(sq > 0, scale / jnp.maximum(sq, 1.0), 0.0)
        g_a, g_b = influence(yz_a), influence(yz_b)
        power = g_a * (r0 * r0 + r1 * r1) + g_b * (r2 * r2)
        energy = energy + weight * jnp.sum(power, axis=0, keepdims=True)
        parts = split3(jnp.concatenate([g_a * r0, g_a * r1, g_b * r2], axis=1))
        back = pl.ds(s * yh, yh)
        for r in range(nc):
            if r % 2 == 0:
                lhs = [jnp.concatenate([ei_ref[m, chip ^ r], ei_ref[m, chip ^ (r + 1)]], axis=0) for m in range(3)]
                two = mul6(lhs, parts)
            p = two[(r % 2) * 4 * yp:(r % 2 + 1) * 4 * yp]
            co, si, ck, sk = [[p[u * yp:(u + 1) * yp, g * LANES:(g + 1) * LANES] for g in range(3)] for u in range(4)]
            pot = (co[0] - si[1], co[1] + si[0], co[2] - flip * pltpu.roll(si[2], 64, 1))
            dy = (-(ck[1] + sk[0]), ck[0] - sk[1], -flip * pltpu.roll(ck[2], 64, 1) - sk[2])
            for comp, val in ((0, pot), (1, dy)):
                for g in range(3):
                    lows[r][comp, g, back, :] = val[g][:yh]
                    highs[r][comp, g, back, :] = val[g][yh - 1:ye]
        return energy

    energy = lax.fori_loop(0, plan.groups[grp], slot, e_in_ref[0:1, :])
    e_row = plan.groups[grp] * yh
    for out in highs:
        out[0, 0, e_row:e_row + 1, :] = energy
    e_out_ref[...] = jnp.broadcast_to(energy, e_out_ref.shape)


def y_call(plan, grp, ids, recs, my, ei, energy):
    shape = jax.ShapeDtypeStruct((2, 3, plan.half_rows[grp], LANES), F32)
    nc = plan.n_chip
    outs = pl.pallas_call(
        functools.partial(y_kernel, plan, grp),
        out_shape=(shape,) * (2 * nc) + (jax.ShapeDtypeStruct((8, LANES), F32),),
        in_specs=[SMEM_SPEC] + [VMEM_SPEC] * (nc + 3), out_specs=(VMEM_SPEC,) * (2 * nc + 1),
        scratch_shapes=[pltpu.VMEM((3, plan.n_chip * plan.y_pad, LANES), F32)],
        cost_estimate=cost(12 * plan.groups[grp] * 384 * (384 * 224 + 896 * 192)),
        compiler_params=pltpu.CompilerParams(vmem_limit_bytes=24 << 20), name="dft_y",
    )(ids, *recs, my, ei, energy)
    return outs[:nc], outs[nc:2 * nc], outs[-1]


I_BATCH = 5


def zi_kernel(plan, grp, with_energy, ids_ref, *refs):
    nc = plan.n_chip
    recs, wi_ref, own_ref, send_ref, buf_ref, e_ref = refs[:nc], *refs[nc:]
    step = pl.program_id(0)
    core, chip = ids_ref[0], ids_ref[1]
    kp, sl, ye = plan.k_rows[grp], plan.groups[grp], plan.y_half

    @pl.when(step == 0)
    def _():
        buf_ref[...] = jnp.zeros(buf_ref.shape, F32)

    for comp in range(2):
        for b in range(I_BATCH):
            for r, rec in enumerate(recs):
                for g in range(3):
                    buf_ref[g, pl.ds((comp * I_BATCH + b) * kp + (chip ^ r) * sl, sl), :] = (
                        rec[comp, g, pl.ds(step * I_BATCH + b, sl, stride=ye), :])
    half_rows = I_BATCH * kp
    parts = split3(jnp.concatenate([buf_ref[g] for g in range(3)], axis=1))
    pot = [p[:half_rows] for p in parts]
    for half, out in ((core, own_ref), (1 - core, send_ref)):
        plain = mul6(parts, [wi_ref[m, half, :, :2 * LANES] for m in range(3)])
        along = mul6(pot, [wi_ref[m, half, :, 2 * LANES:] for m in range(3)])
        for b in range(I_BATCH):
            for ri in range(2):
                ln = slice(ri * LANES, (ri + 1) * LANES)
                out[0, ri, b] = plain[b * kp:(b + 1) * kp, ln]
                out[1, ri, b] = plain[half_rows + b * kp:half_rows + (b + 1) * kp, ln]
                out[2, ri, b] = along[b * kp:(b + 1) * kp, ln]

    if with_energy:
        @pl.when(step == 0)
        def _():
            e_row = sl * ye
            for r, rec in enumerate(recs):
                e_ref[pl.ds(chip ^ r, 1), :] = rec[0, 0, e_row:e_row + 1, :]
            total = e_ref[0:1, :]
            for t in range(1, nc):
                total = total + e_ref[t:t + 1, :]
            own_ref[0, 0, 0, nc * sl:nc * sl + 1, :] = total
            send_ref[0, 0, 0, nc * sl:nc * sl + 1, :] = total


def zi_call(plan, grp, with_energy, ids, recs, wi):
    kp = plan.k_rows[grp]
    shape = jax.ShapeDtypeStruct((3, 2, plan.y_half, kp, LANES), F32)
    spec = pl.BlockSpec((3, 2, I_BATCH, kp, LANES), lambda i: (0, 0, i, 0, 0))
    return pl.pallas_call(
        functools.partial(zi_kernel, plan, grp, with_energy), grid=(plan.y_half // I_BATCH,), out_shape=(shape, shape),
        in_specs=[SMEM_SPEC] + [pl.BlockSpec(r.shape, lambda i: (0,) * 4) for r in recs]
        + [pl.BlockSpec(wi.shape, lambda i: (0,) * 4)],
        out_specs=(spec, spec),
        scratch_shapes=[pltpu.VMEM((3, 2 * I_BATCH * kp, LANES), F32), pltpu.VMEM((8, LANES), F32)],
        cost_estimate=cost(12 * 25 * kp * 384 * 512 * 3),
        compiler_params=pltpu.CompilerParams(vmem_limit_bytes=32 << 20), name="idft_z",
    )(ids, *recs, wi)


def field_kernel(plan, n_xt, half, e_norm, ids_ref, table_ref, num_ref, slot_ref, mi_ref, *refs):
    n_grp = len(plan.groups)
    sides = (refs[:n_grp], refs[n_grp:2 * n_grp])
    out_ref, energy_ref, fhm_ref, flo_ref, lhs_ref = refs[2 * n_grp:]
    core = ids_ref[0]
    n_y = plan.y_half
    for m in range(3):
        for kind in range(2):
            lhs_ref[m, kind] = jnp.concatenate([mi_ref[m, core, kind], mi_ref[m, 1 - core, kind]], axis=1)

    def column(c, y):
        return jnp.concatenate([ref[c, ri, y] for side in sides for ri in range(2) for ref in side], axis=0)

    def put(res, spots):
        hi, mid, lo = split3(res)
        for pos, (y, c) in enumerate(spots):
            ln = slice(pos * LANES, (pos + 1) * LANES)
            fhm_ref[y, c, :, :LANES] = hi[:, ln]
            fhm_ref[y, c, :, LANES:] = mid[:, ln]
            flo_ref[y, c] = lo[:, ln]

    def planes(step, carry):
        y0 = 2 * step
        y1 = jnp.minimum(y0 + 1, n_y - 1)
        data = jnp.concatenate([column(0, y0), column(0, y1)], axis=1)
        put(mul6([lhs_ref[m, 0] for m in range(3)], split3(data)), ((y0, 0), (y1, 0)))
        for y in (y0, y1):
            data = jnp.concatenate([column(1, y), column(2, y)], axis=1)
            put(mul6([lhs_ref[m, 1] for m in range(3)], split3(data)), ((y, 1), (y, 2)))
        return carry
    lax.fori_loop(0, (n_y + 1) // 2, planes, 0)
    e_row = plan.groups[-1] * plan.n_chip
    lanes = sides[0][-1][0, 0, 0, e_row:e_row + 1, :] + sides[1][-1][0, 0, 0, e_row:e_row + 1, :]
    energy_ref[...] = jnp.broadcast_to(jnp.sum(lanes, axis=1, keepdims=True) * e_norm, energy_ref.shape)
    interp_kernel(n_xt, half * (n_y - 1), n_y, num_ref[half], num_ref[half + 1], table_ref, slot_ref,
                  fhm_ref, flo_ref, out_ref)


def field_call(plan, half, ids, table, num, slots, own, rec, mi, n_xt, e_norm):
    return pl.pallas_call(
        functools.partial(field_kernel, plan, n_xt, half, e_norm),
        out_shape=(jax.ShapeDtypeStruct((SLOT_ROWS, LANES), F32), jax.ShapeDtypeStruct((8, LANES), F32)),
        in_specs=[SMEM_SPEC, SMEM_SPEC, SMEM_SPEC] + [VMEM_SPEC] * (2 + 2 * len(own)), out_specs=(VMEM_SPEC, VMEM_SPEC),
        scratch_shapes=[pltpu.VMEM((plan.y_half, 3, plan.x_pad, 2 * LANES), BF16),
                        pltpu.VMEM((plan.y_half, 3, plan.x_pad, LANES), BF16),
                        pltpu.VMEM((3, 2, plan.x_pad, 4 * plan.k_pad), BF16)],
        compiler_params=pltpu.CompilerParams(vmem_limit_bytes=36 << 20), name="idft_x_interp",
    )(ids, table, num, slots, mi, *own, *rec)


def solution(mesh):
    n_cols = mesh.shape["col"]
    n_cx = mesh.shape["row"] // 2
    fine = jax.sharding.Mesh(mesh.devices.reshape(mesh.shape["rep"], n_cols, n_cx, 2), ("rep", "col", "cx", "core"))
    slot_axes = ("rep", "col", "cx", "core")
    chip_axes = ("col", "cx")
    turn = [(a * 2 + b, b * 2 + a) for a in range(n_cols) for b in range(2) if a != b]
    other_core = [(0, 1), (1, 0)]

    def device_body(part_mass, cell_idx, cic_wts, live_mask, gas_block):
        grid_size, y_blk, z_blk = gas_block.shape
        per_dev = part_mass.shape[0]
        n_chip = n_cx * n_cols
        n_slots = per_dev * n_chip * 2
        plan = Plan(grid_size, n_chip, y_blk, z_blk)
        tab = plan.tables()
        core = lax.axis_index("core").astype(jnp.int32)
        chip = (lax.axis_index("cx") * n_cols + lax.axis_index("col")).astype(jnp.int32)
        n_xt = grid_size // X_TILE
        n_blk = y_blk * n_xt

        keep = (core == lax.axis_index("col")).astype(jnp.int32)

        def swap(arr):
            return lax.ppermute(arr, ("col", "core"), turn)

        raw = slot_arrays(part_mass, cell_idx, cic_wts, live_mask, y_blk)
        raw = swap(raw) + raw * keep.astype(F32)
        gas = jnp.pad(jnp.transpose(gas_block, (1, 0, 2)), ((0, plan.y_even - y_blk), (0, 0), (0, 0)))
        raw, gas = lax.optimization_barrier((raw, gas))
        gas_far = swap(gas)
        table, num = pair_table(raw[0].reshape(-1), n_blk, n_xt)
        slots = sort_call(raw)
        rho = deposit_call(table, num, slots, plan.y_even, grid_size, n_xt)
        ids = jnp.stack([core, chip, keep])
        own, send = x_call(plan, ids, rho, gas, gas_far, tab["mx"])

        def exchange(parts):
            out = [parts[0]]
            for r in range(1, n_chip):
                flip = (r >> 1) | ((r & 1) << 1)
                out.append(lax.ppermute(parts[r], chip_axes, [(t, t ^ flip) for t in range(n_chip)]))
            return out

        grps = range(len(plan.groups))

        def chain(token, outs):
            return lax.optimization_barrier((token, tuple(outs)))

        rec = [lax.ppermute(s, "core", other_core) for s in send]
        at_y = []
        for g in grps:
            ids, out = chain(ids, z_call(plan, g, ids, own[g], rec[g], tab["wz"]))
            at_y.append(exchange(out))
        high, low, part = [], [], jnp.zeros((8, LANES), F32)
        for g in grps:
            high_g, low_g, part = y_call(plan, g, ids, at_y[g], tab["my"], tab["ei"], part)
            low.append(low_g)
            if g < len(plan.groups) - 1:
                ids, high_g = chain(ids, high_g)
            else:
                ids, (high_g, low) = chain(ids, (high_g, tuple(low)))
            high.append(exchange(high_g))
        low = [exchange(out) for out in low]
        e_norm = 0.5 / (grid_size ** 3 * n_slots)
        forces = []
        for half, at_z in ((1, high), (0, low)):
            own, send = [], []
            for g in grps:
                with_energy = half == 1 and g == len(plan.groups) - 1
                ids, (own_g, send_g) = chain(ids, zi_call(plan, g, with_energy, ids, at_z[g], tab["wi"]))
                own.append(own_g)
                send.append(lax.ppermute(send_g, "core", other_core))
            ids, out = chain(ids, field_call(plan, half, ids, table, num, slots, own, send, tab["mi"], n_xt, e_norm))
            forces.append(out[0])
            energy = out[1] if half == 1 else energy
        back = unsort_call(slots, *forces)
        home = swap(back) + back * keep.astype(F32)
        return home.reshape(3, per_dev).T, energy[0, 0:1]

    return jax.shard_map(
        device_body, mesh=fine,
        in_specs=(P(slot_axes), P(slot_axes, None), P(slot_axes, None, None), P(slot_axes), P("rep", ("cx", "core"), "col")),
        out_specs=(P(slot_axes, None), P("rep")), check_vma=False)
```

```python
import functools
import math
import numpy as np
import jax
import jax.numpy as jnp
from jax import lax
from jax.sharding import PartitionSpec as P
from jax.experimental import pallas as pl
from jax.experimental.pallas import tpu as pltpu

MATMUL_PREC = lax.Precision.HIGHEST
GRAV_CONST = 1.0
F32 = jnp.float32
BF16 = jnp.bfloat16
LANES = 128
X_TILE = 96
X_ROWS = 112
Y_SHIFT = 15
X_SHIFT = 7
VMEM_BIG = 60 * 1024 * 1024


def split3(val):
    hi = val.astype(BF16)
    rest = val - hi.astype(F32)
    mid = rest.astype(BF16)
    lo = (rest - mid.astype(F32)).astype(BF16)
    return hi, mid, lo


def bitonic(bufs):
    sub = lax.broadcasted_iota(jnp.int32, (8, LANES), 0)
    lane = lax.broadcasted_iota(jnp.int32, (8, LANES), 1)
    base = lane * 128 + sub

    def bit(rank, pos):
        return lax.shift_right_logical(rank, jnp.full_like(rank, pos)) & 1

    def vreg_stage(k, j):
        step = 1 << (j - 3)
        for v in range(16):
            if v & step:
                continue
            low, high = pl.ds(8 * v, 8), pl.ds(8 * (v + step), 8)
            sgn = 1.0 - 2.0 * bit(base + 8 * v, k).astype(F32)
            a = [b[low, :] for b in bufs]
            c = [b[high, :] for b in bufs]
            swap = a[0] * sgn > c[0] * sgn
            for b, p, q in zip(bufs, a, c):
                b[low, :] = jnp.where(swap, q, p)
                b[high, :] = jnp.where(swap, p, q)

    def roll_stage(k, j, dist, axis):
        size = (8, LANES)[axis]
        upper = bit(base, j)
        keep_low = upper == 0
        for v in range(16):
            rows = pl.ds(8 * v, 8)
            sgn = 1.0 - 2.0 * (bit(base + 8 * v, k) ^ upper).astype(F32)
            own = [b[rows, :] for b in bufs]
            other = [jnp.where(keep_low, pltpu.roll(o, size - dist, axis), pltpu.roll(o, dist, axis)) for o in own]
            take = other[0] * sgn < own[0] * sgn
            for b, o, p in zip(bufs, own, other):
                b[rows, :] = jnp.where(take, p, o)

    def stage(k, j):
        if j >= 3:
            vreg_stage(k, j)
        else:
            roll_stage(k, j, 1 << j, 0)

    for k in range(1, 8):
        for j in range(k - 1, -1, -1):
            stage(k, j)

    def phase(k, carry):
        def lane_stage(step, c):
            j = k - 1 - step
            roll_stage(k, j, jnp.left_shift(1, j - 7), 1)
            return c
        lax.fori_loop(0, k - 7, lane_stage, 0)
        for j in range(6, -1, -1):
            stage(k, j)
        return carry
    lax.fori_loop(8, 15, phase, 0)


CHUNKS = 128
UNROLL = 8
SLOT_ROWS = 8 * (CHUNKS + 1)


def sort_kernel(in_ref, out_ref, *bufs):
    for n in range(5):
        bufs[n][...] = in_ref[n]
    row = lax.broadcasted_iota(jnp.int32, (CHUNKS, LANES), 0)
    col = lax.broadcasted_iota(jnp.int32, (CHUNKS, LANES), 1)
    bufs[5][...] = (row * LANES + col).astype(F32)
    bitonic(bufs)
    zero = jnp.zeros((CHUNKS, LANES), F32)
    for n in range(8):
        out_ref[pl.ds(n, CHUNKS, stride=8), :] = bufs[n][...].T if n < 6 else zero
    out_ref[8 * CHUNKS:, :] = jnp.zeros((8, LANES), F32)


def unsort_kernel(slot_ref, low_ref, high_ref, out_ref, *bufs):
    bufs[0][...] = slot_ref[pl.ds(5, CHUNKS, stride=8), :]
    for n in range(3):
        rows = pl.ds(n, CHUNKS, stride=8)
        bufs[n + 1][...] = low_ref[rows, :] + high_ref[rows, :]
    bitonic(bufs)
    for n in range(3):
        out_ref[n] = bufs[n + 1][...].T


def pair_table(key, n_blk, n_xt):
    b_ids = jnp.arange(n_blk + 1)
    bounds = ((b_ids // n_xt) << Y_SHIFT) | (((b_ids % n_xt) * X_TILE) << X_SHIFT)
    starts = jnp.sum((key[None, :] < bounds[:, None].astype(F32)).astype(jnp.int32), axis=1)
    first, last = starts[:-1], starts[1:]
    count = (last - first + LANES - 1) // LANES
    ids = jnp.arange(n_blk)
    ends = jnp.sum(jnp.where(ids[None, :] <= ids[:, None], count[None, :], 0), axis=1)
    t_ids = jnp.arange(n_blk + CHUNKS + 2 * UNROLL)
    blk = jnp.sum((ends[None, :] <= t_ids[:, None]).astype(jnp.int32), axis=1)
    hot = ids[None, :] == blk[:, None]
    beg = jnp.sum(jnp.where(hot, (first - LANES * (ends - count))[None, :], 0), axis=1) + LANES * t_ids
    size = jnp.minimum(jnp.sum(jnp.where(hot, last[None, :], 0), axis=1) - beg, LANES)
    live = t_ids < ends[-1]
    marks = (t_ids * (n_blk // 2) - 1)[:, None]
    split = jnp.sum(jnp.where(ids[None, :] == marks, ends[None, :], 0), axis=1)
    table = jnp.stack([jnp.where(live, blk, 0), jnp.where(live, beg, 0), jnp.where(live, size, 0), split])
    return table.astype(jnp.int32)


def read_window(t, table_ref, slot_ref, n_xt):
    blk = table_ref[0, t]
    beg = table_ref[1, t]
    size = table_ref[2, t]
    y_pl = blk // n_xt
    x_beg = pl.multiple_of((blk % n_xt) * X_TILE, 16)
    row = pl.multiple_of((beg >> 7) * 8, 8)
    off = beg & 127
    back = (LANES - off) & 127
    lane = lax.broadcasted_iota(jnp.int32, (8, LANES), 1)
    win = jnp.where(lane < LANES - off, pltpu.roll(slot_ref[pl.ds(row, 8), :], back, 1),
                    pltpu.roll(slot_ref[pl.ds(row + 8, 8), :], back, 1))
    code = win[0:1].astype(jnp.int32)
    x_c = (code >> X_SHIFT) & 255
    vals = [win[n:n + 1] for n in range(1, 5)]
    return row, off, size, lane, y_pl, x_beg, x_c - x_beg, code & 127, vals


def spread_rows(row):
    return jnp.broadcast_to(row, (16, LANES)).astype(BF16)


def deposit_kernel(n_xt, grid_size, table_ref, slot_ref, rho_ref):
    n_planes = rho_ref.shape[0]

    def clear(y, c):
        rho_ref[y] = jnp.zeros(rho_ref.shape[1:], F32)
        return c
    lax.fori_loop(0, n_planes, clear, 0)
    row_x = lax.broadcasted_iota(jnp.int32, (X_ROWS, LANES), 0)
    row_z = lax.broadcasted_iota(jnp.int32, (LANES, LANES), 0)

    def one(t):
        row, off, size, lane, y_pl, x_beg, x_l, z_c, (q, wx, wy, wz) = read_window(t, table_ref, slot_ref, n_xt)
        q = jnp.where(lane[0:1] < size, q, 0.0)
        pick_x = jnp.concatenate([(row_x == x_l).astype(F32), (row_x == x_l + 1).astype(F32)], axis=1).astype(BF16)
        pick_z = [(row_z == z_c + c).astype(F32).astype(BF16).reshape(8, 16, LANES) for c in range(2)]
        cols = [[], [], []]
        for w_y in (1.0 - wy, wy):
            pieces = [[], [], []]
            for w_x in (1.0 - wx, wx):
                base = q * w_x * w_y
                lower, upper = split3(base * (1.0 - wz)), split3(base * wz)
                for m in range(3):
                    low = spread_rows(lower[m].astype(F32))[None]
                    high = spread_rows(upper[m].astype(F32))[None]
                    pieces[m].append((pick_z[0] * low + pick_z[1] * high).reshape(LANES, LANES))
            for m in range(3):
                cols[m].append(jnp.concatenate(pieces[m], axis=1))
        res = None
        for m in (2, 1, 0):
            part = jnp.concatenate(cols[m], axis=0)
            term = lax.dot_general(pick_x, part, (((1,), (1,)), ((), ())), preferred_element_type=F32)
            res = term if res is None else res + term
        for b in range(2):
            rho_ref[y_pl + b, pl.ds(x_beg, X_ROWS), :] += res[:, b * LANES:(b + 1) * LANES]

    def body(t, c):
        for u in range(UNROLL):
            one(UNROLL * t + u)
        return c
    lax.fori_loop(0, (table_ref[3, 2] + UNROLL - 1) // UNROLL, body, 0)

    def wrap(y, c):
        rho_ref[y, 0:8, :] += rho_ref[y, grid_size:grid_size + 8, :]
        return c
    lax.fori_loop(0, n_planes, wrap, 0)


def interp_kernel(n_xt, y_beg, n_y, t_beg, t_end, table_ref, slot_ref, fhm_ref, flo_ref, out_ref):
    row_x = lax.broadcasted_iota(jnp.int32, (X_ROWS, LANES), 0)
    row_z = lax.broadcasted_iota(jnp.int32, (LANES, LANES), 0)
    out_ref[...] = jnp.zeros(out_ref.shape, F32)

    def one(t):
        row, off, size, lane, y_pl, x_beg, x_l, z_c, (q, wx, wy, wz) = read_window(t, table_ref, slot_ref, n_xt)
        size = jnp.where(t < t_end, size, 0)
        y_pl = jnp.clip(y_pl - y_beg, 0, n_y - 2)
        pick_z = jnp.concatenate([(row_z == z_c).astype(F32), (row_z == z_c + 1).astype(F32)], axis=1).astype(BF16)
        pick_2 = jnp.concatenate([pick_z, pick_z], axis=0)
        on_x = jnp.where(row_x == x_l, 1.0 - wx, jnp.where(row_x == x_l + 1, wx, 0.0))
        rows = pl.ds(x_beg, X_ROWS)
        wt = [on_x * (1.0 - wy), on_x * wy]
        grads = []
        for comp in range(3):
            top = jnp.concatenate([fhm_ref[y_pl + b, comp, rows, :] for b in range(2)], axis=0)
            low = jnp.concatenate([flo_ref[y_pl + b, comp, rows, :] for b in range(2)], axis=0)
            got = jnp.dot(low, pick_z, preferred_element_type=F32) + jnp.dot(top, pick_2, preferred_element_type=F32)
            got = got[:, :LANES] * (1.0 - wz) + got[:, LANES:] * wz
            acc = got[:X_ROWS] * wt[0] + got[X_ROWS:] * wt[1]
            grads.append(-q * jnp.sum(acc, axis=0, keepdims=True))
        full = pltpu.roll(jnp.concatenate(grads + [jnp.zeros((5, LANES), F32)], axis=0), off, 1)
        here, after = pl.ds(row, 8), pl.ds(row + 8, 8)
        out_ref[here, :] = jnp.where((lane >= off) & (lane - off < size), full, out_ref[here, :])
        out_ref[after, :] = jnp.where((lane < off) & (lane + LANES - off < size), full, out_ref[after, :])

    def body(t, c):
        for u in range(UNROLL):
            one(t_beg + UNROLL * t + u)
        return c
    lax.fori_loop(0, (t_end - t_beg + UNROLL - 1) // UNROLL, body, 0)


SMEM_SPEC = pl.BlockSpec(memory_space=pltpu.SMEM)
VMEM_SPEC = pl.BlockSpec(memory_space=pltpu.VMEM)


def sort_call(raw):
    return pl.pallas_call(
        sort_kernel, out_shape=jax.ShapeDtypeStruct((SLOT_ROWS, LANES), F32), in_specs=[VMEM_SPEC], out_specs=VMEM_SPEC,
        scratch_shapes=[pltpu.VMEM((CHUNKS, LANES), F32)] * 6, name="slot_sort",
    )(raw)


def unsort_call(slots, low, high):
    return pl.pallas_call(
        unsort_kernel, out_shape=jax.ShapeDtypeStruct((3, CHUNKS, LANES), F32),
        in_specs=[VMEM_SPEC] * 3, out_specs=VMEM_SPEC,
        scratch_shapes=[pltpu.VMEM((CHUNKS, LANES), F32)] * 4, name="slot_unsort",
    )(slots, low, high)


def deposit_call(table, slots, y_ext, grid_size, n_xt):
    return pl.pallas_call(
        functools.partial(deposit_kernel, n_xt, grid_size),
        out_shape=jax.ShapeDtypeStruct((y_ext, grid_size + 16, LANES), F32),
        in_specs=[SMEM_SPEC, VMEM_SPEC], out_specs=VMEM_SPEC,
        compiler_params=pltpu.CompilerParams(vmem_limit_bytes=24 << 20), name="deposit",
    )(table, slots)


def slot_arrays(part_mass, cell_idx, cic_wts, live_mask, y_blk):
    charge = part_mass * live_mask.astype(F32)
    code = (cell_idx[:, 1] << Y_SHIFT) | (cell_idx[:, 0] << X_SHIFT) | cell_idx[:, 2]
    code = jnp.where(live_mask > 0, code, y_blk << Y_SHIFT).astype(F32)
    upper = cic_wts[:, :, 1]
    return jnp.stack([code, charge, upper[:, 0], upper[:, 1], upper[:, 2]]).reshape(5, CHUNKS, LANES)


def mul6(a, b):
    res = None
    for m, n in ((2, 0), (0, 2), (1, 1), (1, 0), (0, 1), (0, 0)):
        term = jnp.dot(a[m], b[n], preferred_element_type=F32)
        res = term if res is None else res + term
    return res


def table3(mat):
    mat = mat.astype(np.float32)
    hi = mat.astype(BF16)
    mid = (mat - hi.astype(np.float32)).astype(BF16)
    lo = (mat - hi.astype(np.float32) - mid.astype(np.float32)).astype(BF16)
    return np.stack([hi, mid, lo])


GROUP_SLOTS = (6, 7)


class Plan:
    def __init__(self, n, n_chip, y_blk, z_blk):
        self.n, self.n_chip, self.y_blk, self.z_blk = n, n_chip, y_blk, z_blk
        self.y_ext = y_blk + 1
        self.z_ext = z_blk + 1
        self.y_pad = -(-self.y_ext // 8) * 8
        self.half_k = n // 2 + 1
        self.slots = -(-self.half_k // (2 * n_chip))
        self.per_core = self.slots * n_chip
        left, self.groups = self.slots, []
        for size in GROUP_SLOTS:
            self.groups.append(size)
            left -= size
        assert left == 0
        self.k_rows = [-(-size * n_chip // 8) * 8 for size in self.groups]
        self.k_beg = [sum(self.k_rows[:g]) for g in range(len(self.groups))]
        self.s_beg = [sum(self.groups[:g]) for g in range(len(self.groups))]
        self.k_pad = sum(self.k_rows)
        self.rows = [-(-(size * self.y_ext + 1) // 8) * 8 for size in self.groups]
        self.y_half = y_blk // 2 + 1
        self.half_rows = [-(-(size * self.y_half + 1) // 8) * 8 for size in self.groups]
        self.y_even = self.y_ext + self.y_ext % 2
        self.x_pad = n + 16

    def row_slots(self):
        ids = -np.ones(self.k_pad, np.int64)
        for g, size in enumerate(self.groups):
            for t in range(self.n_chip):
                r0 = self.k_beg[g] + t * size
                ids[r0:r0 + size] = t * self.slots + self.s_beg[g] + np.arange(size)
        return ids

    def angle(self, k, r):
        return 2.0 * np.pi / self.n * ((k[:, None] * r[None, :]) % self.n)

    def lane_order(self):
        kz = np.concatenate([np.arange(128), np.arange(128), np.arange(128, self.n), np.arange(128, self.n)])
        im = np.concatenate([np.zeros(128), np.ones(128), np.zeros(self.n - 128), np.ones(self.n - 128)]) > 0
        return kz, im

    def deriv(self, k):
        sgn = np.where(k < self.n // 2, k, k - self.n)
        return np.where(k == self.n // 2, 0, sgn) * (2.0 * np.pi / self.n)

    def tables(self):
        n = self.n
        out = {}
        mx = np.zeros((2, 2, self.k_pad, n))
        mi = np.zeros((2, 2, self.x_pad, 2, self.k_pad))
        ids = self.row_slots()
        for h in range(2):
            kx = np.where(ids >= 0, h * self.per_core + ids, n)
            ok = (kx < self.half_k)[:, None]
            th = self.angle(kx, np.arange(n))
            mx[h, 0] = np.where(ok, np.cos(th), 0.0)
            mx[h, 1] = np.where(ok, -np.sin(th), 0.0)
            th = self.angle(kx, np.arange(self.x_pad))
            wt = np.where(kx < self.half_k, np.where((kx == 0) | (kx == n // 2), 1.0, 2.0), 0.0) / float(n) ** 3
            kd = np.where(kx < n // 2, kx, 0) * (2.0 * np.pi / n) * wt
            mi[h, 0, :, 0] = (-kd[:, None] * np.sin(th)).T
            mi[h, 0, :, 1] = (-kd[:, None] * np.cos(th)).T
            mi[h, 1, :, 0] = (wt[:, None] * np.cos(th)).T
            mi[h, 1, :, 1] = (-wt[:, None] * np.sin(th)).T
        out["mx"] = table3(mx.reshape(2, 2 * self.k_pad, n))
        out["mi"] = table3(mi.reshape(2, 2, self.x_pad, 2 * self.k_pad))
        kz, im = self.lane_order()
        wz = np.zeros((2, 2, LANES, 2 * n))
        wi = np.zeros((2, 2 * n, 4, LANES))
        kd = self.deriv(kz)[:, None]
        for h in range(2):
            z = (h * self.z_blk + np.arange(self.z_ext)) % n
            c, s = np.cos(self.angle(kz, z)), np.sin(self.angle(kz, z))
            wz[h, 0, :self.z_ext] = np.where(im[:, None], -s, c).T
            wz[h, 1, :self.z_ext] = np.where(im[:, None], c, s).T
            re_w, im_w = np.where(im[:, None], -s, c), np.where(im[:, None], c, s)
            wi[h, :, 0, :self.z_ext] = re_w
            wi[h, :, 1, :self.z_ext] = im_w
            wi[h, :, 2, :self.z_ext] = -kd * im_w
            wi[h, :, 3, :self.z_ext] = kd * re_w
        out["wz"] = table3(wz)
        out["wi"] = table3(wi.reshape(2, 2 * n, 4 * LANES))
        ky = np.arange(n)
        my = np.zeros((2, n, self.n_chip, self.y_pad))
        ei = np.zeros((self.n_chip, 4, self.y_pad, n))
        for i in range(self.n_chip):
            y = (i * self.y_blk + np.arange(self.y_ext)) % n
            th = self.angle(ky, y)
            my[0, :, i, :self.y_ext] = np.cos(th)
            my[1, :, i, :self.y_ext] = np.sin(th)
            ei[i, 0, :self.y_ext] = np.cos(th).T
            ei[i, 1, :self.y_ext] = np.sin(th).T
            ei[i, 2, :self.y_ext] = (self.deriv(ky)[:, None] * np.cos(th)).T
            ei[i, 3, :self.y_ext] = (self.deriv(ky)[:, None] * np.sin(th)).T
        out["my"] = table3(my.reshape(2 * n, self.n_chip * self.y_pad))
        out["ei"] = table3(ei.reshape(self.n_chip, 4 * self.y_pad, n))
        return out


def cost(flops):
    return pl.CostEstimate(flops=int(flops), bytes_accessed=1 << 20, transcendentals=0)


X_BATCH = 10


def x_kernel(plan, ids_ref, rho_ref, gas_ref, far_ref, mx_ref, *rest):
    lhs_ref, tmp_ref = rest[-2:]
    core = ids_ref[0]
    n, kp = plan.n, plan.k_pad

    @pl.when(pl.program_id(0) == 0)
    def _():
        tmp_ref[...] = jnp.zeros(tmp_ref.shape, F32)
        for m in range(3):
            lhs_ref[m] = jnp.concatenate([mx_ref[m, core], mx_ref[m, 1 - core]], axis=0)

    keep = ids_ref[2].astype(F32)
    y_left = plan.y_blk - X_BATCH * pl.program_id(0)
    for y in range(X_BATCH):
        @pl.when(y < y_left)
        def _():
            tmp_ref[y, :, :plan.z_blk] = gas_ref[y] * keep + far_ref[y]

        @pl.when(y >= y_left)
        def _():
            tmp_ref[y] = jnp.zeros(tmp_ref.shape[1:], F32)
    n_grp = len(plan.groups)
    lhs = [lhs_ref[m] for m in range(3)]
    for pair in range(X_BATCH // 2):
        ys = (2 * pair, 2 * pair + 1)
        data = jnp.concatenate([rho_ref[y, :n, :] + tmp_ref[y] for y in ys], axis=1)
        res = mul6(lhs, split3(data))
        for h in range(2):
            for g in range(n_grp):
                out = rest[h * n_grp + g]
                for pos, y in enumerate(ys):
                    for ri in range(2):
                        r0 = (2 * h + ri) * kp + plan.k_beg[g]
                        out[ri, y] = res[r0:r0 + plan.k_rows[g], pos * LANES:(pos + 1) * LANES]


def x_call(plan, ids, rho, gas, far, mx):
    steps = plan.y_even // X_BATCH
    shapes = tuple(jax.ShapeDtypeStruct((2, plan.y_even, k, LANES), F32) for k in plan.k_rows)
    out_specs = tuple(pl.BlockSpec((2, X_BATCH, k, LANES), lambda i: (0, i, 0, 0)) for k in plan.k_rows)
    gas_spec = pl.BlockSpec((X_BATCH, plan.n, plan.z_blk), lambda i: (i, 0, 0))
    outs = pl.pallas_call(
        functools.partial(x_kernel, plan), grid=(steps,), out_shape=shapes + shapes,
        in_specs=[SMEM_SPEC, pl.BlockSpec((X_BATCH, plan.x_pad, LANES), lambda i: (i, 0, 0)),
                  gas_spec, gas_spec,
                  pl.BlockSpec(mx.shape, lambda i: (0, 0, 0, 0))],
        out_specs=out_specs + out_specs,
        scratch_shapes=[pltpu.VMEM((3, 4 * plan.k_pad, plan.n), BF16), pltpu.VMEM((X_BATCH, plan.n, LANES), F32)],
        compiler_params=pltpu.CompilerParams(vmem_limit_bytes=32 << 20), name="dft_x",
    )(ids, rho, gas, far, mx)
    return outs[:len(shapes)], outs[len(shapes):]


Z_BATCH = 10


def z_kernel(plan, grp, ids_ref, own_ref, rec_ref, wz_ref, *rest):
    outs, tmp_ref = rest[:-1], rest[-1]
    step = pl.program_id(0)
    core, chip = ids_ref[0], ids_ref[1]
    kp, sl, ye, rows = plan.k_rows[grp], plan.groups[grp], plan.y_ext, plan.rows[grp]

    @pl.when(step == 0)
    def _():
        for out in outs:
            for g in range(3):
                out[g, rows - 8:rows, :] = jnp.zeros((8, LANES), F32)

    flat = (Z_BATCH * kp, LANES)
    data = jnp.concatenate([own_ref[0].reshape(flat), rec_ref[0].reshape(flat),
                            own_ref[1].reshape(flat), rec_ref[1].reshape(flat)], axis=1)
    wts = [jnp.concatenate([wz_ref[m, core, 0], wz_ref[m, 1 - core, 0], wz_ref[m, core, 1], wz_ref[m, 1 - core, 1]], axis=0)
           for m in range(3)]
    res = mul6(split3(data), wts)
    for g in range(3):
        tmp_ref[g] = res[:, g * LANES:(g + 1) * LANES]
    for b in range(Z_BATCH):
        y = step * Z_BATCH + b

        @pl.when(y < ye)
        def _():
            for r, out in enumerate(outs):
                for g in range(3):
                    out[g, pl.ds(y, sl, stride=ye), :] = tmp_ref[g, pl.ds(b * kp + (chip ^ r) * sl, sl), :]


def z_call(plan, grp, ids, own, rec, wz):
    kp = plan.k_rows[grp]
    blk = pl.BlockSpec((2, Z_BATCH, kp, LANES), lambda i: (0, i, 0, 0))
    shape = (3, plan.rows[grp], LANES)
    return pl.pallas_call(
        functools.partial(z_kernel, plan, grp), grid=(plan.y_even // Z_BATCH,),
        out_shape=(jax.ShapeDtypeStruct(shape, F32),) * plan.n_chip,
        in_specs=[SMEM_SPEC, blk, blk, pl.BlockSpec(wz.shape, lambda i: (0,) * 5)],
        out_specs=(pl.BlockSpec(shape, lambda i: (0, 0, 0)),) * plan.n_chip,
        scratch_shapes=[pltpu.VMEM((3, Z_BATCH * kp, LANES), F32)],
        cost_estimate=cost(12 * 50 * kp * 512 * 384),
        compiler_params=pltpu.CompilerParams(vmem_limit_bytes=24 << 20), name="dft_z",
    )(ids, own, rec, wz)


def signed(ids, n):
    return jnp.where(ids < n // 2, ids, ids - n).astype(F32)


def y_kernel(plan, grp, ids_ref, *refs):
    nc = plan.n_chip
    recs, (my_ref, ei_ref, e_in_ref) = refs[:nc], refs[nc:nc + 3]
    highs, lows, e_out_ref, buf_ref = refs[nc + 3:2 * nc + 3], refs[2 * nc + 3:3 * nc + 3], refs[-2], refs[-1]
    n, ye, yp, yh, n_rows = plan.n, plan.y_ext, plan.y_pad, plan.y_half, plan.half_rows[grp]
    core, chip = ids_ref[0], ids_ref[1]
    kx_beg = core * plan.per_core + chip * plan.slots + plan.s_beg[grp]
    k_unit = 2.0 * math.pi / n
    buf_ref[...] = jnp.zeros(buf_ref.shape, F32)
    for out in highs + lows:
        for c in range(2):
            for g in range(3):
                out[c, g, n_rows - 8:n_rows, :] = jnp.zeros((8, LANES), F32)
    lane = lax.broadcasted_iota(jnp.int32, (n, LANES), 1)
    ky = signed(lax.broadcasted_iota(jnp.int32, (n, LANES), 0), n)
    kz_a = signed(lane, n)
    kz_b = signed(128 + (lane & 63), n)
    yz_a, yz_b = ky * ky + kz_a * kz_a, ky * ky + kz_b * kz_b
    flip = jnp.where(lax.broadcasted_iota(jnp.int32, (1, LANES), 1) < 64, 1.0, -1.0)

    def slots(ss, energy):
        data = []
        for pos, s in enumerate(ss):
            rows = pl.ds(s * ye, ye)
            for r, rec in enumerate(recs):
                for g in range(3):
                    buf_ref[3 * pos + g, pl.ds(pl.multiple_of((chip ^ r) * yp, 8), ye), :] = rec[g, rows, :]
            data += [buf_ref[3 * pos + g] for g in range(3)]
        q = mul6([my_ref[m] for m in range(3)], split3(jnp.concatenate(data, axis=1)))
        data = []
        for pos, s in enumerate(ss):
            c = [q[:n, g * LANES:(g + 1) * LANES] for g in range(3 * pos, 3 * pos + 3)]
            d = [q[n:, g * LANES:(g + 1) * LANES] for g in range(3 * pos, 3 * pos + 3)]
            r0 = c[0] + d[1]
            r1 = c[1] - d[0]
            r2 = c[2] + flip * pltpu.roll(d[2], 64, 1)
            kx_i = kx_beg + s
            kx = kx_i.astype(F32)
            weight = jnp.where(kx_i < n // 2, jnp.where(kx_i == 0, 1.0, 2.0), jnp.where(kx_i == n // 2, 1.0, 0.0))
            scale = -4.0 * math.pi * GRAV_CONST / (k_unit * k_unit)

            def influence(yz):
                sq = yz + kx * kx
                return jnp.where(sq > 0, scale / jnp.maximum(sq, 1.0), 0.0)
            g_a, g_b = influence(yz_a), influence(yz_b)
            power = g_a * (r0 * r0 + r1 * r1) + g_b * (r2 * r2)
            energy = energy + weight * jnp.sum(power, axis=0, keepdims=True)
            data += [g_a * r0, g_a * r1, g_b * r2]
        parts = split3(jnp.concatenate(data, axis=1))
        for r in range(nc):
            p = mul6([ei_ref[m, chip ^ r] for m in range(3)], parts)
            for pos, s in enumerate(ss):
                back = pl.ds(s * yh, yh)
                co, si, ck, sk = [[p[u * yp:(u + 1) * yp, g * LANES:(g + 1) * LANES] for g in range(3 * pos, 3 * pos + 3)]
                                  for u in range(4)]
                pot = (co[0] - si[1], co[1] + si[0], co[2] - flip * pltpu.roll(si[2], 64, 1))
                dy = (-(ck[1] + sk[0]), ck[0] - sk[1], -flip * pltpu.roll(ck[2], 64, 1) - sk[2])
                for comp, val in ((0, pot), (1, dy)):
                    for g in range(3):
                        lows[r][comp, g, back, :] = val[g][:yh]
                        highs[r][comp, g, back, :] = val[g][yh - 1:ye]
        return energy

    n_slot = plan.groups[grp]
    energy = lax.fori_loop(0, n_slot // 2, lambda i, e: slots((2 * i, 2 * i + 1), e), e_in_ref[0:1, :])
    if n_slot % 2:
        energy = slots((n_slot - 1,), energy)
    e_row = plan.groups[grp] * yh
    for out in highs:
        out[0, 0, e_row:e_row + 1, :] = energy
    e_out_ref[...] = jnp.broadcast_to(energy, e_out_ref.shape)


def y_call(plan, grp, ids, recs, my, ei, energy):
    shape = jax.ShapeDtypeStruct((2, 3, plan.half_rows[grp], LANES), F32)
    nc = plan.n_chip
    outs = pl.pallas_call(
        functools.partial(y_kernel, plan, grp),
        out_shape=(shape,) * (2 * nc) + (jax.ShapeDtypeStruct((8, LANES), F32),),
        in_specs=[SMEM_SPEC] + [VMEM_SPEC] * (nc + 3), out_specs=(VMEM_SPEC,) * (2 * nc + 1),
        scratch_shapes=[pltpu.VMEM((6, plan.n_chip * plan.y_pad, LANES), F32)],
        cost_estimate=cost(12 * plan.groups[grp] * 384 * (384 * 224 + 896 * 192)),
        compiler_params=pltpu.CompilerParams(vmem_limit_bytes=24 << 20), name="dft_y",
    )(ids, *recs, my, ei, energy)
    return outs[:nc], outs[nc:2 * nc], outs[-1]


I_BATCH = 5


def zi_kernel(plan, grp, with_energy, ids_ref, *refs):
    nc = plan.n_chip
    recs, wi_ref, own_ref, send_ref, buf_ref, e_ref = refs[:nc], *refs[nc:]
    step = pl.program_id(0)
    core, chip = ids_ref[0], ids_ref[1]
    kp, sl, ye = plan.k_rows[grp], plan.groups[grp], plan.y_half

    @pl.when(step == 0)
    def _():
        buf_ref[...] = jnp.zeros(buf_ref.shape, F32)

    for comp in range(2):
        for b in range(I_BATCH):
            for r, rec in enumerate(recs):
                for g in range(3):
                    buf_ref[g, pl.ds((comp * I_BATCH + b) * kp + (chip ^ r) * sl, sl), :] = (
                        rec[comp, g, pl.ds(step * I_BATCH + b, sl, stride=ye), :])
    half_rows = I_BATCH * kp
    parts = split3(jnp.concatenate([buf_ref[g] for g in range(3)], axis=1))
    pot = [p[:half_rows] for p in parts]
    for half, out in ((core, own_ref), (1 - core, send_ref)):
        plain = mul6(parts, [wi_ref[m, half, :, :2 * LANES] for m in range(3)])
        along = mul6(pot, [wi_ref[m, half, :, 2 * LANES:] for m in range(3)])
        for b in range(I_BATCH):
            for ri in range(2):
                ln = slice(ri * LANES, (ri + 1) * LANES)
                out[0, ri, b] = plain[b * kp:(b + 1) * kp, ln]
                out[1, ri, b] = plain[half_rows + b * kp:half_rows + (b + 1) * kp, ln]
                out[2, ri, b] = along[b * kp:(b + 1) * kp, ln]

    if with_energy:
        @pl.when(step == 0)
        def _():
            e_row = sl * ye
            for r, rec in enumerate(recs):
                e_ref[pl.ds(chip ^ r, 1), :] = rec[0, 0, e_row:e_row + 1, :]
            total = e_ref[0:1, :]
            for t in range(1, nc):
                total = total + e_ref[t:t + 1, :]
            own_ref[0, 0, 0, nc * sl:nc * sl + 1, :] = total
            send_ref[0, 0, 0, nc * sl:nc * sl + 1, :] = total


def zi_call(plan, grp, with_energy, ids, recs, wi):
    kp = plan.k_rows[grp]
    shape = jax.ShapeDtypeStruct((3, 2, plan.y_half, kp, LANES), F32)
    spec = pl.BlockSpec((3, 2, I_BATCH, kp, LANES), lambda i: (0, 0, i, 0, 0))
    return pl.pallas_call(
        functools.partial(zi_kernel, plan, grp, with_energy), grid=(plan.y_half // I_BATCH,), out_shape=(shape, shape),
        in_specs=[SMEM_SPEC] + [pl.BlockSpec(r.shape, lambda i: (0,) * 4) for r in recs]
        + [pl.BlockSpec(wi.shape, lambda i: (0,) * 4)],
        out_specs=(spec, spec),
        scratch_shapes=[pltpu.VMEM((3, 2 * I_BATCH * kp, LANES), F32), pltpu.VMEM((8, LANES), F32)],
        cost_estimate=cost(12 * 25 * kp * 384 * 512 * 3),
        compiler_params=pltpu.CompilerParams(vmem_limit_bytes=32 << 20), name="idft_z",
    )(ids, *recs, wi)


def field_kernel(plan, n_xt, half, e_norm, ids_ref, table_ref, slot_ref, mi_ref, *refs):
    n_grp = len(plan.groups)
    sides = (refs[:n_grp], refs[n_grp:2 * n_grp])
    out_ref, energy_ref, fhm_ref, flo_ref, lhs_ref = refs[2 * n_grp:]
    core = ids_ref[0]
    n_y = plan.y_half
    for m in range(3):
        for kind in range(2):
            lhs_ref[m, kind] = jnp.concatenate([mi_ref[m, core, kind], mi_ref[m, 1 - core, kind]], axis=1)

    def column(c, y):
        return jnp.concatenate([ref[c, ri, y] for side in sides for ri in range(2) for ref in side], axis=0)

    def put(res, spots):
        hi, mid, lo = split3(res)
        for pos, (y, c) in enumerate(spots):
            ln = slice(pos * LANES, (pos + 1) * LANES)
            fhm_ref[y, c, :, :LANES] = hi[:, ln]
            fhm_ref[y, c, :, LANES:] = mid[:, ln]
            flo_ref[y, c] = lo[:, ln]

    def planes(step, carry):
        y0 = 2 * step
        y1 = jnp.minimum(y0 + 1, n_y - 1)
        data = jnp.concatenate([column(0, y0), column(0, y1)], axis=1)
        put(mul6([lhs_ref[m, 0] for m in range(3)], split3(data)), ((y0, 0), (y1, 0)))
        for y in (y0, y1):
            data = jnp.concatenate([column(1, y), column(2, y)], axis=1)
            put(mul6([lhs_ref[m, 1] for m in range(3)], split3(data)), ((y, 1), (y, 2)))
        return carry
    lax.fori_loop(0, (n_y + 1) // 2, planes, 0)
    e_row = plan.groups[-1] * plan.n_chip
    lanes = sides[0][-1][0, 0, 0, e_row:e_row + 1, :] + sides[1][-1][0, 0, 0, e_row:e_row + 1, :]
    energy_ref[...] = jnp.broadcast_to(jnp.sum(lanes, axis=1, keepdims=True) * e_norm, energy_ref.shape)
    interp_kernel(n_xt, half * (n_y - 1), n_y, table_ref[3, half], table_ref[3, half + 1], table_ref, slot_ref,
                  fhm_ref, flo_ref, out_ref)


def field_call(plan, half, ids, table, slots, own, rec, mi, n_xt, e_norm):
    return pl.pallas_call(
        functools.partial(field_kernel, plan, n_xt, half, e_norm),
        out_shape=(jax.ShapeDtypeStruct((SLOT_ROWS, LANES), F32), jax.ShapeDtypeStruct((8, LANES), F32)),
        in_specs=[SMEM_SPEC, SMEM_SPEC] + [VMEM_SPEC] * (2 + 2 * len(own)), out_specs=(VMEM_SPEC, VMEM_SPEC),
        scratch_shapes=[pltpu.VMEM((plan.y_half, 3, plan.x_pad, 2 * LANES), BF16),
                        pltpu.VMEM((plan.y_half, 3, plan.x_pad, LANES), BF16),
                        pltpu.VMEM((3, 2, plan.x_pad, 4 * plan.k_pad), BF16)],
        compiler_params=pltpu.CompilerParams(vmem_limit_bytes=36 << 20), name="idft_x_interp",
    )(ids, table, slots, mi, *own, *rec)


def solution(mesh):
    n_cols = mesh.shape["col"]
    n_cx = mesh.shape["row"] // 2
    fine = jax.sharding.Mesh(mesh.devices.reshape(mesh.shape["rep"], n_cols, n_cx, 2), ("rep", "col", "cx", "core"))
    slot_axes = ("rep", "col", "cx", "core")
    chip_axes = ("col", "cx")
    turn = [(a * 2 + b, b * 2 + a) for a in range(n_cols) for b in range(2) if a != b]
    other_core = [(0, 1), (1, 0)]

    def device_body(part_mass, cell_idx, cic_wts, live_mask, gas_block):
        grid_size, y_blk, z_blk = gas_block.shape
        per_dev = part_mass.shape[0]
        n_chip = n_cx * n_cols
        n_slots = per_dev * n_chip * 2
        plan = Plan(grid_size, n_chip, y_blk, z_blk)
        tab = plan.tables()
        core = lax.axis_index("core").astype(jnp.int32)
        chip = (lax.axis_index("cx") * n_cols + lax.axis_index("col")).astype(jnp.int32)
        n_xt = grid_size // X_TILE
        n_blk = y_blk * n_xt

        keep = (core == lax.axis_index("col")).astype(jnp.int32)

        def swap(arr):
            return lax.ppermute(arr, ("col", "core"), turn)

        raw = slot_arrays(part_mass, cell_idx, cic_wts, live_mask, y_blk)
        raw = swap(raw) + raw * keep.astype(F32)
        gas = jnp.transpose(gas_block, (1, 0, 2))
        raw, gas = lax.optimization_barrier((raw, gas))
        gas_far = swap(gas)
        table = pair_table(raw[0].reshape(-1), n_blk, n_xt)
        slots = sort_call(raw)
        rho = deposit_call(table, slots, plan.y_even, grid_size, n_xt)
        ids = jnp.stack([core, chip, keep])
        own, send = x_call(plan, ids, rho, gas, gas_far, tab["mx"])

        def exchange(parts):
            out = [parts[0]]
            for r in range(1, n_chip):
                flip = (r >> 1) | ((r & 1) << 1)
                out.append(lax.ppermute(parts[r], chip_axes, [(t, t ^ flip) for t in range(n_chip)]))
            return out

        grps = range(len(plan.groups))

        def chain(token, outs):
            return lax.optimization_barrier((token, tuple(outs)))

        rec = [lax.ppermute(s, "core", other_core) for s in send]
        at_y = []
        for g in grps:
            ids, out = chain(ids, z_call(plan, g, ids, own[g], rec[g], tab["wz"]))
            at_y.append(exchange(out))
        high, low, part = [], [], jnp.zeros((8, LANES), F32)
        for g in grps:
            high_g, low_g, part = y_call(plan, g, ids, at_y[g], tab["my"], tab["ei"], part)
            low.append(low_g)
            if g < len(plan.groups) - 1:
                ids, high_g = chain(ids, high_g)
            else:
                ids, (high_g, low) = chain(ids, (high_g, tuple(low)))
            high.append(exchange(high_g))
        low = [exchange(out) for out in low]
        e_norm = 0.5 / (grid_size ** 3 * n_slots)
        forces = []
        for half, at_z in ((1, high), (0, low)):
            own, send = [], []
            for g in grps:
                with_energy = half == 1 and g == len(plan.groups) - 1
                ids, (own_g, send_g) = chain(ids, zi_call(plan, g, with_energy, ids, at_z[g], tab["wi"]))
                own.append(own_g)
                send.append(lax.ppermute(send_g, "core", other_core))
            ids, out = chain(ids, field_call(plan, half, ids, table, slots, own, send, tab["mi"], n_xt, e_norm))
            forces.append(out[0])
            energy = out[1] if half == 1 else energy
        back = unsort_call(slots, *forces)
        home = swap(back) + back * keep.astype(F32)
        return home.reshape(3, per_dev).T, energy[0, 0:1]

    return jax.shard_map(
        device_body, mesh=fine,
        in_specs=(P(slot_axes), P(slot_axes, None), P(slot_axes, None, None), P(slot_axes), P("rep", ("cx", "core"), "col")),
        out_specs=(P(slot_axes, None), P("rep")), check_vma=False)
```
